8 devices in a mesh: data: 1 (over z), col: 2 (over y), row: 4 (over x, core).
Axes of the slice: x: 2, y: 2, z: 1, core: 2. Of those that a mesh axis runs over, the one named last changes fastest.
Arguments:
- image: bfloat16 [256, 128, 3], P(('data', 'row'), 'col')
- w_enc1a: bfloat16 [3, 3, 3, 192], replicated
- b_enc1a: float32 [192], replicated
- w_enc1b: bfloat16 [3, 3, 192, 192], replicated
- b_enc1b: float32 [192], replicated
- w_enc2a: bfloat16 [3, 3, 192, 384], replicated
- b_enc2a: float32 [384], replicated
- w_enc2b: bfloat16 [3, 3, 384, 384], replicated
- b_enc2b: float32 [384], replicated
- w_mid_a: bfloat16 [3, 3, 384, 768], replicated
- b_mid_a: float32 [768], replicated
- w_mid_b: bfloat16 [3, 3, 768, 768], replicated
- b_mid_b: float32 [768], replicated
- w_up2: bfloat16 [2, 2, 768, 384], replicated
- w_dec2a: bfloat16 [3, 3, 768, 384], replicated
- b_dec2a: float32 [384], replicated
- w_dec2b: bfloat16 [3, 3, 384, 384], replicated
- b_dec2b: float32 [384], replicated
- w_up1: bfloat16 [2, 2, 384, 192], replicated
- w_dec1a: bfloat16 [3, 3, 384, 192], replicated
- b_dec1a: float32 [192], replicated
- w_dec1b: bfloat16 [3, 3, 192, 192], replicated
- b_dec1b: float32 [192], replicated
- w_head: bfloat16 [192, 6], replicated
- b_head: float32 [6], replicated
Outputs:
- output: float32 [256, 128, 6], P(('data', 'row'), 'col')
All inputs are finite; a program needn't handle non-finite values.
Results may differ from the reference program's by a relative error of at most 0.0168.
Values are sent between devices in bfloat16 or wider.
A program may use at most 1 GiB of HBM per device.

```python
import jax
import jax.numpy as jnp
from jax import lax

IN_CH = 3
BASE_CH = 192
OUT_CH = 6
IMG_ROWS = 256
IMG_COLS = 128


def weight_specs():
    ch_one = BASE_CH
    ch_two = 2 * BASE_CH
    ch_four = 4 * BASE_CH
    bias_gain = 0.0625
    return [
        ("w_enc1a", (3, 3, IN_CH, ch_one), 9 * IN_CH, 2.0, jnp.bfloat16),
        ("b_enc1a", (ch_one,), 1, bias_gain, jnp.float32),
        ("w_enc1b", (3, 3, ch_one, ch_one), 9 * ch_one, 2.0, jnp.bfloat16),
        ("b_enc1b", (ch_one,), 1, bias_gain, jnp.float32),
        ("w_enc2a", (3, 3, ch_one, ch_two), 9 * ch_one, 2.0, jnp.bfloat16),
        ("b_enc2a", (ch_two,), 1, bias_gain, jnp.float32),
        ("w_enc2b", (3, 3, ch_two, ch_two), 9 * ch_two, 2.0, jnp.bfloat16),
        ("b_enc2b", (ch_two,), 1, bias_gain, jnp.float32),
        ("w_mid_a", (3, 3, ch_two, ch_four), 9 * ch_two, 2.0, jnp.bfloat16),
        ("b_mid_a", (ch_four,), 1, bias_gain, jnp.float32),
        ("w_mid_b", (3, 3, ch_four, ch_four), 9 * ch_four, 2.0, jnp.bfloat16),
        ("b_mid_b", (ch_four,), 1, bias_gain, jnp.float32),
        ("w_up2", (2, 2, ch_four, ch_two), ch_four, 1.0, jnp.bfloat16),
        ("w_dec2a", (3, 3, ch_four, ch_two), 9 * ch_four, 2.0, jnp.bfloat16),
        ("b_dec2a", (ch_two,), 1, bias_gain, jnp.float32),
        ("w_dec2b", (3, 3, ch_two, ch_two), 9 * ch_two, 2.0, jnp.bfloat16),
        ("b_dec2b", (ch_two,), 1, bias_gain, jnp.float32),
        ("w_up1", (2, 2, ch_two, ch_one), ch_two, 1.0, jnp.bfloat16),
        ("w_dec1a", (3, 3, ch_two, ch_one), 9 * ch_two, 2.0, jnp.bfloat16),
        ("b_dec1a", (ch_one,), 1, bias_gain, jnp.float32),
        ("w_dec1b", (3, 3, ch_one, ch_one), 9 * ch_one, 2.0, jnp.bfloat16),
        ("b_dec1b", (ch_one,), 1, bias_gain, jnp.float32),
        ("w_head", (ch_one, OUT_CH), ch_one, 1.0, jnp.bfloat16),
        ("b_head", (OUT_CH,), 1, bias_gain, jnp.float32),
    ]


def setup_inputs(seed: int = 0, part: int = 0) -> dict:
    root = jax.random.key(seed)
    image_key = jax.random.fold_in(jax.random.fold_in(root, 1000), part)
    pixels = jax.random.normal(image_key, (IMG_ROWS, IMG_COLS, IN_CH), jnp.float32)
    result = {"image": pixels.astype(jnp.bfloat16)}
    for index, spec in enumerate(weight_specs()):
        name, shape, fan_in, gain, dtype = spec
        values = jax.random.normal(jax.random.fold_in(root, index), shape, jnp.float32)
        result[name] = (values * (gain / fan_in) ** 0.5).astype(dtype)
    return result


def conv_relu(hidden, weight, bias):
    conv_out = lax.conv_general_dilated(hidden.astype(jnp.float32)[None], weight.astype(jnp.float32), (1, 1), "SAME", dimension_numbers=("NHWC", "HWIO", "NHWC"))[0]
    return jax.nn.relu(conv_out + bias).astype(jnp.bfloat16)


def double_conv(hidden, w_first, b_first, w_second, b_second):
    return conv_relu(conv_relu(hidden, w_first, b_first), w_second, b_second)


def max_pool(hidden):
    height, width, channels = hidden.shape
    return hidden.reshape(height // 2, 2, width // 2, 2, channels).max(axis=(1, 3))


def up_conv(hidden, weight):
    height = hidden.shape[0]
    width = hidden.shape[1]
    summed = jnp.einsum("ijc,abco->iajbo", hidden.astype(jnp.float32), weight.astype(jnp.float32))
    return summed.astype(jnp.bfloat16).reshape(2 * height, 2 * width, weight.shape[3])


def reference(image, w_enc1a, b_enc1a, w_enc1b, b_enc1b, w_enc2a, b_enc2a, w_enc2b, b_enc2b, w_mid_a, b_mid_a, w_mid_b, b_mid_b, w_up2, w_dec2a, b_dec2a, w_dec2b, b_dec2b, w_up1, w_dec1a, b_dec1a, w_dec1b, b_dec1b, w_head, b_head):
    skip_one = double_conv(image, w_enc1a, b_enc1a, w_enc1b, b_enc1b)
    skip_two = double_conv(max_pool(skip_one), w_enc2a, b_enc2a, w_enc2b, b_enc2b)
    middle = double_conv(max_pool(skip_two), w_mid_a, b_mid_a, w_mid_b, b_mid_b)
    hidden = double_conv(jnp.concatenate([up_conv(middle, w_up2), skip_two], axis=2), w_dec2a, b_dec2a, w_dec2b, b_dec2b)
    hidden = double_conv(jnp.concatenate([up_conv(hidden, w_up1), skip_one], axis=2), w_dec1a, b_dec1a, w_dec1b, b_dec1b)
    flat = hidden.reshape(-1, hidden.shape[2])
    head_out = jnp.dot(flat, w_head, preferred_element_type=jnp.float32) + b_head
    return head_out.reshape(hidden.shape[0], hidden.shape[1], w_head.shape[1])
```

```python
import jax
import jax.numpy as jnp
from jax import lax
from jax.sharding import PartitionSpec as P

CONV_DIMS = ("NHWC", "HWIO", "NHWC")


def solution(mesh):
    row_count = mesh.shape["row"]
    col_count = mesh.shape["col"]
    grid_size = row_count * col_count
    grid_axes = ("col", "row")
    row_next = [(source, source + 1) for source in range(row_count - 1)]
    row_prev = [(source + 1, source) for source in range(row_count - 1)]
    col_next = [(source, source + 1) for source in range(col_count - 1)]
    col_prev = [(source + 1, source) for source in range(col_count - 1)]
    tile_spec = P(("data", "row"), "col", None)

    def with_halo(tile):
        from_above = lax.ppermute(tile[-1:], "row", row_next)
        from_below = lax.ppermute(tile[:1], "row", row_prev)
        tall_tile = jnp.concatenate([from_above, tile, from_below], axis=0)
        from_left = lax.ppermute(tall_tile[:, -1:], "col", col_next)
        from_right = lax.ppermute(tall_tile[:, :1], "col", col_prev)
        return jnp.concatenate([from_left, tall_tile, from_right], axis=1)

    def conv_relu(hidden, weight, bias, padding):
        conv_out = lax.conv_general_dilated(hidden[None], weight, (1, 1), padding, dimension_numbers=CONV_DIMS, preferred_element_type=jnp.float32)[0]
        return jax.nn.relu(conv_out + bias).astype(jnp.bfloat16)

    def double_tile(tile, w_first, b_first, w_second, b_second):
        first = conv_relu(with_halo(tile), w_first, b_first, "VALID")
        return conv_relu(with_halo(first), w_second, b_second, "VALID")

    def max_pool(tile):
        height, width, channels = tile.shape
        return tile.reshape(height // 2, 2, width // 2, 2, channels).max(axis=(1, 3))

    def up_conv(tile, weight):
        height = tile.shape[0]
        width = tile.shape[1]
        summed = jnp.einsum("ijc,abco->iajbo", tile, weight, preferred_element_type=jnp.float32)
        return summed.astype(jnp.bfloat16).reshape(2 * height, 2 * width, weight.shape[3])

    def device_body(image_tile, *params):
        (w_enc1a, b_enc1a, w_enc1b, b_enc1b, w_enc2a, b_enc2a, w_enc2b, b_enc2b,
         w_mid_a, b_mid_a, w_mid_b, b_mid_b, w_up2, w_dec2a, b_dec2a, w_dec2b, b_dec2b,
         w_up1, w_dec1a, b_dec1a, w_dec1b, b_dec1b, w_head, b_head) = params
        skip_one = double_tile(image_tile, w_enc1a, b_enc1a, w_enc1b, b_enc1b)
        skip_two = double_tile(max_pool(skip_one), w_enc2a, b_enc2a, w_enc2b, b_enc2b)
        mid_tile = double_tile(max_pool(skip_two), w_mid_a, b_mid_a, w_mid_b, b_mid_b)
        hidden = double_tile(jnp.concatenate([up_conv(mid_tile, w_up2), skip_two], axis=2), w_dec2a, b_dec2a, w_dec2b, b_dec2b)
        hidden = double_tile(jnp.concatenate([up_conv(hidden, w_up1), skip_one], axis=2), w_dec1a, b_dec1a, w_dec1b, b_dec1b)
        return jnp.einsum("hwc,co->hwo", hidden, w_head, preferred_element_type=jnp.float32) + b_head

    def program(image, *params):
        mapped = jax.shard_map(device_body, mesh=mesh, in_specs=(tile_spec,) + tuple([P()] * len(params)), out_specs=tile_spec, check_vma=False)
        return mapped(image, *params)

    return program
```

```python
import functools

import jax
import jax.numpy as jnp
import numpy as np
from jax import lax
from jax.experimental import pallas as pl
from jax.experimental.pallas import tpu as pltpu
from jax.sharding import PartitionSpec as P

MESH = pl.DeviceIdType.MESH
F32 = jnp.float32
BF16 = jnp.bfloat16
ROWS = 18
SIDE = 16
PIX = SIDE * SIDE
EXCHANGE_FACTOR = (2, 2, 1, 1, 2, 2, 4, 4)
EXCHANGE_LANES = (256, 384, 384, 768, 768, 384, 384, 256)


def kernel(row_count, x8, w8, we1b, we2a, we2b, wma, wmb, wu2, wd2a, wd2b, wu1, wd1a, wd1b, wh,
           be1a, be1b, be2a, be2b, bma, bmb, bd2a, bd2b, bd1a, bd1b, bh, y,
           vw8, ve1b, ve2a, ve2b, vma, vmb, vu2, vd2a, vd2b, vu1, vd1a, vd1b,
           h1, cat1, d1a, p1, e2a, cat2, d2, p2, ma, mid,
           sc0, sc1, sc2, sc3, sc4, sc5, sc6, sc7, rc0, rc1, rc2, rc3, rc4, rc5, rc6, rc7,
           w_sem, send_sem, recv_sem):
    row = lax.axis_index("row")
    col = lax.axis_index("col")
    data = lax.axis_index("data")
    last = row_count - 1
    has_up = row > 0
    has_down = row < last
    up = (data, col, row - 1)
    down = (data, col, row + 1)
    side = (data, 1 - col, row)
    side_up = (data, 1 - col, row - 1)
    side_down = (data, 1 - col, row + 1)
    edge = (1 - col) * (SIDE - 1)
    send_cols = (sc0, sc1, sc2, sc3, sc4, sc5, sc6, sc7)
    recv_cols = (rc0, rc1, rc2, rc3, rc4, rc5, rc6, rc7)

    loads = (
        (w8, vw8), (we1b, ve1b), (we2a, ve2a.at[:, :, 64:256, :]), (we2b, ve2b), (wma, vma), (wmb, vmb),
        (wu2, vu2), (wd2a, vd2a), (wd2b, vd2b), (wu1, vu1), (wd1a, vd1a), (wd1b, vd1b.at[:, :, 0:192, :]),
    )
    copies = [pltpu.make_async_copy(src, dst, w_sem.at[k]) for k, (src, dst) in enumerate(loads)]
    for k in range(4):
        copies[k].start()

    def zero_halo(buf, factor):
        shape = buf.shape[1:2] + buf.shape[3:]
        buf[0, :, ROWS - 1] = jnp.zeros(shape, BF16)
        buf[factor - 1, :, 0] = jnp.zeros(shape, BF16)

    for buf, factor in ((h1, 4), (cat1, 4), (p1, 2), (e2a, 2), (cat2, 2), (p2, 1), (ma, 1)):
        zero_halo(buf, factor)

    def zero_plane(t, carry):
        d1a[t // 6, lax.rem(t, 6)] = jnp.zeros(d1a.shape[2:], BF16)
        return carry

    lax.fori_loop(0, 24, zero_plane, 0)
    for buf, factor in zip(recv_cols, EXCHANGE_FACTOR):
        buf[factor:factor + 2] = jnp.zeros((2,) + buf.shape[1:], BF16)
    ve2a[:, :, 0:64, :] = jnp.zeros((3, 3, 64, 384), BF16)
    vd1b[:, :, 192:256, :] = jnp.zeros((3, 3, 64, 192), BF16)

    barrier = pltpu.get_barrier_semaphore()
    pl.semaphore_signal(barrier, inc=1, device_id=side, device_id_type=MESH)

    @pl.when(has_up)
    def _():
        pl.semaphore_signal(barrier, inc=1, device_id=up, device_id_type=MESH)
        pl.semaphore_signal(barrier, inc=1, device_id=side_up, device_id_type=MESH)

    @pl.when(has_down)
    def _():
        pl.semaphore_signal(barrier, inc=1, device_id=down, device_id_type=MESH)
        pl.semaphore_signal(barrier, inc=1, device_id=side_down, device_id_type=MESH)

    for k in range(4, len(copies)):
        copies[k].start()

    def relu_bias(acc, bias):
        return jnp.maximum(acc + bias[...], 0.0)

    copies[0].wait()
    ext = ROWS * SIDE
    pos = lax.broadcasted_iota(jnp.int32, (ext, 256), 0)
    pos_row = pos // SIDE
    pos_col = lax.rem(pos, SIDE)
    off_rows = ((pos_row == 0) & (row == 0)) | ((pos_row == ROWS - 1) & (row == last))
    off_left = off_rows | ((pos_col == 0) & (col == 0))
    off_right = off_rows | ((pos_col == SIDE - 1) & (col == 1))

    def first_conv(a, carry):
        for b in range(6):
            acc = jnp.dot(x8[...], vw8[a * 6 + b], preferred_element_type=F32)
            off = off_left if b == 0 else off_right if b == 5 else off_rows
            out = jnp.where(off, 0.0, relu_bias(acc, be1a)).astype(BF16)
            h1[a, b] = out.reshape(ROWS, SIDE, 256)
        return carry

    lax.fori_loop(0, 4, first_conv, 0)

    def taps(buf, factor, a):
        rows = []
        for b in range(factor):
            parts = []
            for dy in range(3):
                shifted = a + (dy - 1) + factor
                plane = lax.rem(shifted, factor)
                start = shifted // factor
                for dx in range(3):
                    piece = buf[plane, b + dx, pl.ds(start, SIDE)]
                    parts.append(piece.reshape(PIX, piece.shape[-1]))
            rows.append(jnp.concatenate(parts, axis=1))
        return rows[0] if factor == 1 else jnp.concatenate(rows, axis=0)

    def conv(buf, factor, a, weight, bias, transposed=False):
        lhs = taps(buf, factor, a)
        if transposed:
            acc = None
            width = weight.shape[-1]
            for t in range(9):
                part = lax.dot_general(lhs[:, t * width:(t + 1) * width], weight[t // 3, t % 3],
                                       (((1,), (1,)), ((), ())), preferred_element_type=F32)
                acc = part if acc is None else acc + part
        else:
            flat = weight[...].reshape(lhs.shape[1], weight.shape[-1])
            acc = jnp.dot(lhs, flat, preferred_element_type=F32)
        return relu_bias(acc, bias).astype(BF16)

    def store_row(buf, factor, a, value, lane, width):
        for b in range(factor):
            buf[a, b + 1, 1:ROWS - 1, :, lane:lane + width] = value[b * PIX:(b + 1) * PIX].reshape(SIDE, SIDE, width)

    def conv_layer(src, dst, factor, weight, bias, lane, transposed=False):
        width = bias.shape[-1]

        def body(a, carry):
            store_row(dst, factor, a, conv(src, factor, a, weight, bias, transposed), lane, width)
            return carry

        if factor == 1:
            body(0, 0)
        else:
            lax.fori_loop(0, factor, body, 0)

    def pool(src, dst, factor, lane, width):
        for a in range(factor):
            for b in range(factor):
                best = None
                for p in range(2):
                    for q in range(2):
                        piece = src[2 * a + p, 2 * b + q + 1, 1:ROWS - 1, :, lane:lane + width]
                        best = piece if best is None else jnp.maximum(best, piece)
                dst[a, b + 1, 1:ROWS - 1] = best

    def messages(index, buf):
        factor = EXCHANGE_FACTOR[index]
        cols, got = send_cols[index], recv_cols[index]

        def remote(src, dst, k, device):
            return pltpu.make_async_remote_copy(
                src_ref=src, dst_ref=dst, send_sem=send_sem.at[index, k], recv_sem=recv_sem.at[index, k],
                device_id=device, device_id_type=MESH)

        to_side = remote(cols, got.at[pl.ds(0, factor)], 0, side)
        to_up = remote(buf.at[0, :, 1], buf.at[0, :, ROWS - 1], 1, up)
        to_down = remote(buf.at[factor - 1, :, ROWS - 2], buf.at[factor - 1, :, 0], 2, down)
        to_side_up = remote(cols.at[0], got.at[factor + 1], 3, side_up)
        to_side_down = remote(cols.at[factor - 1], got.at[factor], 4, side_down)
        return to_side, to_up, to_down, to_side_up, to_side_down

    def exchange(index, buf):
        factor = EXCHANGE_FACTOR[index]
        lanes = EXCHANGE_LANES[index]
        cols, got = send_cols[index], recv_cols[index]
        at = lax.broadcasted_iota(jnp.int32, (PIX, lanes), 0)
        at_col = lax.rem(at, SIDE)

        def shifted_planes(a, carry):
            left = buf[a, factor, 1:ROWS - 1].reshape(PIX, lanes).astype(F32)
            left = jnp.where(at_col == 0, 0.0, pltpu.roll(left, 1, 0))
            buf[a, 0, 1:ROWS - 1] = left.astype(BF16).reshape(SIDE, SIDE, lanes)
            right = buf[a, 1, 1:ROWS - 1].reshape(PIX, lanes).astype(F32)
            right = jnp.where(at_col == SIDE - 1, 0.0, pltpu.roll(right, PIX - 1, 0))
            buf[a, factor + 1, 1:ROWS - 1] = right.astype(BF16).reshape(SIDE, SIDE, lanes)
            return carry

        lax.fori_loop(0, factor, shifted_planes, 0)
        pick_row = lax.broadcasted_iota(jnp.int32, (SIDE, PIX), 0)
        pick_at = lax.broadcasted_iota(jnp.int32, (SIDE, PIX), 1)
        pick = (pick_at == pick_row * SIDE + edge).astype(F32).astype(BF16)
        for a in range(factor):
            plane = buf[a, 1 + (factor - 1) * (1 - col), 1:ROWS - 1].reshape(PIX, lanes)
            cols[a] = jnp.dot(pick, plane, preferred_element_type=F32).astype(BF16)
        to_side, to_up, to_down, to_side_up, to_side_down = messages(index, buf)
        to_side.start()

        @pl.when(has_up)
        def _():
            to_up.start()
            to_side_up.start()

        @pl.when(has_down)
        def _():
            to_down.start()
            to_side_down.start()

        to_side.wait()

        @pl.when(has_up)
        def _():
            to_up.wait_send()
            to_side_up.wait_send()
            to_down.wait_recv()
            to_side_down.wait_recv()

        @pl.when(has_down)
        def _():
            to_down.wait_send()
            to_side_down.wait_send()
            to_up.wait_recv()
            to_side_up.wait_recv()

        place_at = lax.broadcasted_iota(jnp.int32, (ROWS * SIDE, 3 * SIDE), 0)
        place_from = lax.broadcasted_iota(jnp.int32, (ROWS * SIDE, 3 * SIDE), 1)
        place = (lax.rem(place_at, SIDE) == edge) & (place_at // SIDE + SIDE - 1 == place_from)
        place = place.astype(F32).astype(BF16)
        fix = (factor + 1) * (1 - col)

        def insert(a, carry):
            halo = jnp.concatenate([got[factor], got[a], got[factor + 1]], axis=0)
            put = jnp.dot(place, halo, preferred_element_type=F32)
            plane = buf[a, fix].reshape(ROWS * SIDE, lanes).astype(F32)
            buf[a, fix] = (plane + put).astype(BF16).reshape(ROWS, SIDE, lanes)
            return carry

        lax.fori_loop(0, factor, insert, 0)

    copies[1].wait()
    conv_layer(h1, cat1, 4, ve1b, be1b, 128)
    pool(cat1, p1, 2, 128, 256)

    total = jnp.where(has_up, 2, 0) + jnp.where(has_down, 2, 0) + 1
    pl.semaphore_wait(barrier, total)
    exchange(0, p1)
    copies[2].wait()
    conv_layer(p1, e2a, 2, ve2a, be2a, 0)
    exchange(1, e2a)
    copies[3].wait()
    conv_layer(e2a, cat2, 2, ve2b, be2b, 384)
    pool(cat2, p2, 1, 384, 384)
    exchange(2, p2)
    copies[4].wait()
    conv_layer(p2, ma, 1, vma, bma, 0)
    exchange(3, ma)
    copies[5].wait()
    mid[...] = conv(ma, 1, 0, vmb, bmb)
    copies[6].wait()
    for p in range(2):
        for q in range(2):
            out = jnp.dot(mid[...], vu2[p, q], preferred_element_type=F32).astype(BF16)
            cat2[p, q + 1, 1:ROWS - 1, :, 0:384] = out.reshape(SIDE, SIDE, 384)
    exchange(4, cat2)
    copies[7].wait()
    conv_layer(cat2, e2a, 2, vd2a, bd2a, 0)
    exchange(5, e2a)
    copies[8].wait()

    def dec2b(a, carry):
        d2[pl.ds(2 * a * PIX, 2 * PIX)] = conv(e2a, 2, a, vd2b, bd2b)
        return carry

    lax.fori_loop(0, 2, dec2b, 0)
    copies[9].wait()

    def up1(t, carry):
        a = t // 2
        p = lax.rem(t, 2)
        lhs = d2[pl.ds(2 * a * PIX, 2 * PIX)]
        for q in range(2):
            out = lax.dot_general(lhs, vu1[p, q], (((1,), (1,)), ((), ())), preferred_element_type=F32).astype(BF16)
            for b in range(2):
                cat1[t, 2 * b + q + 1, 1:ROWS - 1, :, 0:192] = out[b * PIX:(b + 1) * PIX].reshape(SIDE, SIDE, 192)
        return carry

    lax.fori_loop(0, 4, up1, 0)
    exchange(6, cat1)
    copies[10].wait()
    conv_layer(cat1, d1a, 4, vd1a, bd1a, 0, transposed=True)
    exchange(7, d1a)
    copies[11].wait()

    def dec1b(a, carry):
        out = conv(d1a, 4, a, vd1b, bd1b)
        for b in range(4):
            head = lax.dot_general(wh[...], out[b * PIX:(b + 1) * PIX], (((1,), (1,)), ((), ())), preferred_element_type=F32)
            y[a, b] = head + bh[...]
        return carry

    lax.fori_loop(0, 4, dec1b, 0)


def solution(mesh):
    row_count = mesh.shape["row"]
    col_count = mesh.shape["col"]
    row_next = [(source, source + 1) for source in range(row_count - 1)]
    row_prev = [(source + 1, source) for source in range(row_count - 1)]
    col_next = [(source, source + 1) for source in range(col_count - 1)]
    col_prev = [(source + 1, source) for source in range(col_count - 1)]
    tile_spec = P(("data", "row"), "col", None)

    def with_halo(tile, depth):
        from_above = lax.ppermute(tile[-depth:], "row", row_next)
        from_below = lax.ppermute(tile[:depth], "row", row_prev)
        tall_tile = jnp.concatenate([from_above, tile, from_below], axis=0)
        from_left = lax.ppermute(tall_tile[:, -depth:], "col", col_next)
        from_right = lax.ppermute(tall_tile[:, :depth], "col", col_prev)
        return jnp.concatenate([from_left, tall_tile, from_right], axis=1)

    def patches(image_tile):
        haloed = with_halo(image_tile, 2)
        padded = jnp.pad(haloed, ((3, 5), (0, 0), (0, 0)))
        select = np.zeros((68, 8, 16), np.float32)
        for px in range(8):
            for j in range(16):
                select[4 * j + px, px, j] = 1.0
        picked = jnp.einsum("rwc,wpj->rpjc", padded, jnp.asarray(select, BF16), preferred_element_type=F32).astype(BF16)
        blocks = picked.reshape(19, 4, 8, 16, 3)
        rows = jnp.concatenate([blocks[:18], blocks[1:, :2]], axis=1)
        return rows.transpose(0, 3, 1, 2, 4).reshape(288, 144)

    def first_weights(w_enc1a):
        planes = []
        for a in range(4):
            for b in range(6):
                planes.append(jnp.pad(w_enc1a, ((a, 3 - a), (b, 5 - b), (0, 0), (0, 64))))
        return jnp.stack(planes).reshape(24, 144, 256)

    def device_body(image_tile, *params):
        (w_enc1a, b_enc1a, w_enc1b, b_enc1b, w_enc2a, b_enc2a, w_enc2b, b_enc2b,
         w_mid_a, b_mid_a, w_mid_b, b_mid_b, w_up2, w_dec2a, b_dec2a, w_dec2b, b_dec2b,
         w_up1, w_dec1a, b_dec1a, w_dec1b, b_dec1b, w_head, b_head) = params
        anywhere = pl.BlockSpec(memory_space=pl.ANY)
        vmem = pl.BlockSpec(memory_space=pltpu.VMEM)
        operands = [
            patches(image_tile), first_weights(w_enc1a),
            jnp.pad(w_enc1b, ((0, 0), (0, 0), (0, 64), (64, 0))), w_enc2a, w_enc2b, w_mid_a, w_mid_b,
            w_up2, w_dec2a, w_dec2b, jnp.swapaxes(w_up1, 2, 3), jnp.swapaxes(w_dec1a, 2, 3), w_dec1b, w_head.T,
            jnp.pad(b_enc1a, (0, 64))[None], jnp.pad(b_enc1b, (64, 0))[None], b_enc2a[None], b_enc2b[None],
            b_mid_a[None], b_mid_b[None], b_dec2a[None], b_dec2b[None], b_dec1a[None], b_dec1b[None], b_head[:, None],
        ]
        specs = [vmem] + [anywhere] * 12 + [vmem] * 12
        level = lambda factor, lanes: pltpu.VMEM((factor, factor + 2, ROWS, SIDE, lanes), BF16)
        scratch = [
            pltpu.VMEM((24, 144, 256), BF16), pltpu.VMEM((3, 3, 256, 256), BF16), pltpu.VMEM((3, 3, 256, 384), BF16),
            pltpu.VMEM((3, 3, 384, 384), BF16), pltpu.VMEM((3, 3, 384, 768), BF16), pltpu.VMEM((3, 3, 768, 768), BF16),
            pltpu.VMEM((2, 2, 768, 384), BF16), pltpu.VMEM((3, 3, 768, 384), BF16), pltpu.VMEM((3, 3, 384, 384), BF16),
            pltpu.VMEM((2, 2, 192, 384), BF16), pltpu.VMEM((3, 3, 192, 384), BF16), pltpu.VMEM((3, 3, 256, 192), BF16),
            level(4, 256), level(4, 384), level(4, 256), level(2, 256), level(2, 384), level(2, 768),
            pltpu.VMEM((4 * PIX, 384), BF16), level(1, 384), level(1, 768), pltpu.VMEM((PIX, 768), BF16),
        ]
        scratch += [pltpu.VMEM((f, SIDE, c), BF16) for f, c in zip(EXCHANGE_FACTOR, EXCHANGE_LANES)]
        scratch += [pltpu.VMEM((f + 2, SIDE, c), BF16) for f, c in zip(EXCHANGE_FACTOR, EXCHANGE_LANES)]
        scratch += [pltpu.SemaphoreType.DMA((12,)), pltpu.SemaphoreType.DMA((8, 5)), pltpu.SemaphoreType.DMA((8, 5))]
        out = pl.pallas_call(
            functools.partial(kernel, row_count),
            name="unet",
            out_shape=jax.ShapeDtypeStruct((4, 4, 6, PIX), F32),
            in_specs=specs,
            out_specs=vmem,
            scratch_shapes=scratch,
            compiler_params=pltpu.CompilerParams(collective_id=0, has_side_effects=True, vmem_limit_bytes=67043328),
        )(*operands)
        grid = out.reshape(4, 4, 6, 16, 16).transpose(3, 0, 4, 1, 2)
        return grid.reshape(64, 64, 6)

    def program(image, *params):
        mapped = jax.shard_map(device_body, mesh=mesh, in_specs=(tile_spec,) + tuple([P()] * len(params)), out_specs=tile_spec, check_vma=False)
        return mapped(image, *params)

    return program
```

```python
import functools

import jax
import jax.numpy as jnp
from jax import lax
from jax.experimental import pallas as pl
from jax.experimental.pallas import tpu as pltpu
from jax.sharding import PartitionSpec as P

MESH = pl.DeviceIdType.MESH
F32 = jnp.float32
BF16 = jnp.bfloat16
ROWS = 18
SIDE = 16
PIX = SIDE * SIDE
EXCHANGE_FACTOR = (2, 2, 1, 1, 2, 2, 4, 4, 1)
EXCHANGE_LANES = (256, 384, 384, 768, 768, 384, 384, 256, 128)
PATCH = 192


def kernel(row_count, x, we1a, we1b, we2a, we2b, wma, wmb, wu2, wd2a, wd2b, wu1, wd1a, wd1b, wh,
           be1a, be1b, be2a, be2b, bma, bmb, bd2a, bd2b, bd1a, bd1b, bh, y,
           vw8, re1b, ve1b, ve2a, ve2b, vma, vmb, vu2, vd2a, vd2b, vu1, vd1a, vd1b,
           h1, cat1, d1a, p1, e2a, cat2, d2, p2, ma, mid, x1, x8, wf, be1, weave,
           sc0, sc1, sc2, sc3, sc4, sc5, sc6, sc7, sc8, rc0, rc1, rc2, rc3, rc4, rc5, rc6, rc7, rc8,
           w_sem, send_sem, recv_sem):
    row = lax.axis_index("row")
    col = lax.axis_index("col")
    data = lax.axis_index("data")
    last = row_count - 1
    has_up = row > 0
    has_down = row < last
    up = (data, col, row - 1)
    down = (data, col, row + 1)
    side = (data, 1 - col, row)
    side_up = (data, 1 - col, row - 1)
    side_down = (data, 1 - col, row + 1)
    edge = (1 - col) * (SIDE - 1)
    send_cols = (sc0, sc1, sc2, sc3, sc4, sc5, sc6, sc7, sc8)
    recv_cols = (rc0, rc1, rc2, rc3, rc4, rc5, rc6, rc7, rc8)

    loads = (
        (we1b, re1b), (we2a, ve2a.at[:, :, 64:256, :]), (we2b, ve2b), (wma, vma), (wmb, vmb),
        (wu2, vu2), (wd2a, vd2a), (wd2b, vd2b), (wu1, vu1), (wd1a, vd1a), (wd1b, vd1b.at[:, :, 0:192, :]),
    )
    copies = [pltpu.make_async_copy(src, dst, w_sem.at[k]) for k, (src, dst) in enumerate(loads)]
    for k in range(3):
        copies[k].start()

    def zero_halo(buf, factor):
        shape = buf.shape[1:2] + buf.shape[3:]
        buf[0, :, ROWS - 1] = jnp.zeros(shape, BF16)
        buf[factor - 1, :, 0] = jnp.zeros(shape, BF16)

    for buf, factor in ((h1, 4), (cat1, 4), (p1, 2), (e2a, 2), (cat2, 2), (p2, 1), (ma, 1), (x1, 1)):
        zero_halo(buf, factor)

    def zero_plane(t, carry):
        d1a[t // 6, lax.rem(t, 6)] = jnp.zeros(d1a.shape[2:], BF16)
        return carry

    lax.fori_loop(0, 24, zero_plane, 0)
    for buf, factor in zip(recv_cols, EXCHANGE_FACTOR):
        buf[factor:factor + 2] = jnp.zeros((2,) + buf.shape[1:], BF16)
    ve2a[:, :, 0:64, :] = jnp.zeros((3, 3, 64, 384), BF16)
    vd1b[:, :, 192:256, :] = jnp.zeros((3, 3, 64, 192), BF16)

    barrier = pltpu.get_barrier_semaphore()
    pl.semaphore_signal(barrier, inc=1, device_id=side, device_id_type=MESH)

    @pl.when(has_up)
    def _():
        pl.semaphore_signal(barrier, inc=1, device_id=up, device_id_type=MESH)
        pl.semaphore_signal(barrier, inc=1, device_id=side_up, device_id_type=MESH)

    @pl.when(has_down)
    def _():
        pl.semaphore_signal(barrier, inc=1, device_id=down, device_id_type=MESH)
        pl.semaphore_signal(barrier, inc=1, device_id=side_down, device_id_type=MESH)

    for k in range(3, len(copies)):
        copies[k].start()

    def relu_bias(acc, bias):
        return jnp.maximum(acc + bias[...].reshape(1, bias.shape[-1]), 0.0)

    def iota(shape, dim):
        return lax.broadcasted_iota(jnp.int32, shape, dim)

    def ones_at(mask):
        return mask.astype(F32).astype(BF16)

    at, to = iota((64, 64), 0), iota((64, 64), 1)
    split_cols = ones_at(at == lax.rem(to, 16) * 4 + to // 16)
    at, to = iota((PIX, 64), 0), iota((PIX, 64), 1)
    own_col = lax.rem(at, 16) == lax.rem(to, 16)
    image = None
    for ch in range(3):
        cols = jnp.dot(x[ch], split_cols, preferred_element_type=F32).astype(BF16)
        for a in range(4):
            spread = ones_at(to == (at // 16) * 4 + a)
            lines = jnp.where(own_col, jnp.dot(spread, cols, preferred_element_type=F32), 0.0).astype(BF16)
            fold = ones_at(iota((64, 128), 1) == iota((64, 128), 0) // 16 + (ch * 16 + a * 4))
            part = jnp.dot(lines, fold, preferred_element_type=F32)
            image = part if image is None else image + part
    x1[0, 1, 1:ROWS - 1] = image.astype(BF16).reshape(SIDE, SIDE, 128)

    def first_weights():
        wf[...] = jnp.zeros(wf.shape, F32)
        for t in range(9):
            wf[4 * t:4 * t + 3, 0:192] = we1a[t // 3, t % 3].astype(F32)
        k, m = iota((PATCH, 40), 0), iota((PATCH, 40), 1)
        base = (k // 32) * 12 + (lax.rem(k, 32) // 4) * 4 + lax.rem(k, 4)
        row_ok = k // 32
        col_ok = lax.rem(k, 32) // 4

        def body(t, carry):
            a, b = t // 6, lax.rem(t, 6)
            good = (row_ok >= a) & (row_ok <= a + 2) & (col_ok >= b) & (col_ok <= b + 2)
            place = ones_at(good & (m == base - a * 12 - b * 4))
            vw8[t] = jnp.dot(place, wf[...].astype(BF16), preferred_element_type=F32).astype(BF16)
            return carry

        lax.fori_loop(0, 24, body, 0)
        be1[0:1, 0:192] = be1a[...].reshape(1, 192)
        be1[0:1, 192:256] = jnp.zeros((1, 64), F32)
        be1[1:2, :] = jnp.concatenate([jnp.zeros((1, 64), F32), be1b[...].reshape(1, 192)], axis=1)
        n, m = iota((PIX, PIX), 0), iota((PIX, PIX), 1)
        weave[...] = ones_at(m == lax.rem(n, 4) * 64 + (n // 64) * 16 + lax.rem(n, 64) // 4)
        copies[0].wait()

        def shift(t, carry):
            a, b = t // 3, lax.rem(t, 3)
            value = re1b[a, b].astype(F32)
            ve1b[a, b, 0:192] = jnp.concatenate([jnp.zeros((192, 64), F32), value], axis=1).astype(BF16)
            ve1b[a, b, 192:256] = jnp.zeros((64, 256), BF16)
            return carry

        lax.fori_loop(0, 9, shift, 0)

    def patch_matrix():
        blocks = []
        for dx in range(3):
            plane = x1[0, dx].reshape(ROWS * SIDE, 128)
            pad = jnp.zeros((SIDE, 128), BF16)
            blocks.append((jnp.concatenate([pad, plane[:-SIDE]], axis=0), plane, jnp.concatenate([plane[SIDE:], pad], axis=0)))
        total = None
        lane, k = iota((128, PATCH), 0), iota((128, PATCH), 1)
        ch, a, b = lane // 16, lax.rem(lane, 16) // 4, lax.rem(lane, 4)
        for dy in range(3):
            for dx in range(3):
                py, px = a + (4 * dy - 3), b + (4 * dx - 2)
                good = (ch < 3) & (py >= 0) & (py < 6) & (px >= 0) & (px < 8)
                place = ones_at(good & (k == py * 32 + px * 4 + ch))
                part = jnp.dot(blocks[dx][dy], place, preferred_element_type=F32)
                total = part if total is None else total + part
        x8[...] = total.astype(BF16)

    def first_layer():
        ext = ROWS * SIDE
        pos = iota((ext, 256), 0)
        pos_row = pos // SIDE
        pos_col = lax.rem(pos, SIDE)
        off_rows = ((pos_row == 0) & (row == 0)) | ((pos_row == ROWS - 1) & (row == last))
        off_left = off_rows | ((pos_col == 0) & (col == 0))
        off_right = off_rows | ((pos_col == SIDE - 1) & (col == 1))

        def body(a, carry):
            for b in range(6):
                acc = jnp.dot(x8[...], vw8[a * 6 + b], preferred_element_type=F32)
                off = off_left if b == 0 else off_right if b == 5 else off_rows
                out = jnp.where(off, 0.0, jnp.maximum(acc + be1[0:1, :], 0.0)).astype(BF16)
                h1[a, b] = out.reshape(ROWS, SIDE, 256)
            return carry

        lax.fori_loop(0, 4, body, 0)

    def taps(buf, factor, a):
        rows = []
        for b in range(factor):
            parts = []
            for dy in range(3):
                shifted = a + (dy - 1) + factor
                plane = lax.rem(shifted, factor)
                start = shifted // factor
                for dx in range(3):
                    piece = buf[plane, b + dx, pl.ds(start, SIDE)]
                    parts.append(piece.reshape(PIX, piece.shape[-1]))
            rows.append(jnp.concatenate(parts, axis=1))
        return rows[0] if factor == 1 else jnp.concatenate(rows, axis=0)

    def conv(buf, factor, a, weight, bias, transposed=False):
        lhs = taps(buf, factor, a)
        if transposed:
            acc = None
            width = weight.shape[-1]
            for t in range(9):
                part = lax.dot_general(lhs[:, t * width:(t + 1) * width], weight[t // 3, t % 3],
                                       (((1,), (1,)), ((), ())), preferred_element_type=F32)
                acc = part if acc is None else acc + part
        else:
            flat = weight[...].reshape(lhs.shape[1], weight.shape[-1])
            acc = jnp.dot(lhs, flat, preferred_element_type=F32)
        return relu_bias(acc, bias).astype(BF16)

    def store_row(buf, factor, a, value, lane, width):
        for b in range(factor):
            buf[a, b + 1, 1:ROWS - 1, :, lane:lane + width] = value[b * PIX:(b + 1) * PIX].reshape(SIDE, SIDE, width)

    def conv_layer(src, dst, factor, weight, bias, lane, transposed=False):
        width = bias.shape[-1]

        def body(a, carry):
            store_row(dst, factor, a, conv(src, factor, a, weight, bias, transposed), lane, width)
            return carry

        if factor == 1:
            body(0, 0)
        else:
            lax.fori_loop(0, factor, body, 0)

    def pool(src, dst, factor, lane, width):
        for a in range(factor):
            for b in range(factor):
                best = None
                for p in range(2):
                    for q in range(2):
                        piece = src[2 * a + p, 2 * b + q + 1, 1:ROWS - 1, :, lane:lane + width]
                        best = piece if best is None else jnp.maximum(best, piece)
                dst[a, b + 1, 1:ROWS - 1] = best

    def messages(index, buf):
        factor = EXCHANGE_FACTOR[index]
        cols, got = send_cols[index], recv_cols[index]

        def remote(src, dst, k, device):
            return pltpu.make_async_remote_copy(
                src_ref=src, dst_ref=dst, send_sem=send_sem.at[index, k], recv_sem=recv_sem.at[index, k],
                device_id=device, device_id_type=MESH)

        to_side = remote(cols, got.at[pl.ds(0, factor)], 0, side)
        to_up = remote(buf.at[0, :, 1], buf.at[0, :, ROWS - 1], 1, up)
        to_down = remote(buf.at[factor - 1, :, ROWS - 2], buf.at[factor - 1, :, 0], 2, down)
        to_side_up = remote(cols.at[0], got.at[factor + 1], 3, side_up)
        to_side_down = remote(cols.at[factor - 1], got.at[factor], 4, side_down)
        return to_side, to_up, to_down, to_side_up, to_side_down

    def exchange(index, buf, meanwhile=None):
        factor = EXCHANGE_FACTOR[index]
        lanes = EXCHANGE_LANES[index]
        cols, got = send_cols[index], recv_cols[index]
        at = lax.broadcasted_iota(jnp.int32, (PIX, lanes), 0)
        at_col = lax.rem(at, SIDE)

        def shifted_planes(a, carry):
            left = buf[a, factor, 1:ROWS - 1].reshape(PIX, lanes).astype(F32)
            left = jnp.where(at_col == 0, 0.0, pltpu.roll(left, 1, 0))
            buf[a, 0, 1:ROWS - 1] = left.astype(BF16).reshape(SIDE, SIDE, lanes)
            right = buf[a, 1, 1:ROWS - 1].reshape(PIX, lanes).astype(F32)
            right = jnp.where(at_col == SIDE - 1, 0.0, pltpu.roll(right, PIX - 1, 0))
            buf[a, factor + 1, 1:ROWS - 1] = right.astype(BF16).reshape(SIDE, SIDE, lanes)
            return carry

        lax.fori_loop(0, factor, shifted_planes, 0)
        pick_row = lax.broadcasted_iota(jnp.int32, (SIDE, PIX), 0)
        pick_at = lax.broadcasted_iota(jnp.int32, (SIDE, PIX), 1)
        pick = (pick_at == pick_row * SIDE + edge).astype(F32).astype(BF16)
        for a in range(factor):
            plane = buf[a, 1 + (factor - 1) * (1 - col), 1:ROWS - 1].reshape(PIX, lanes)
            cols[a] = jnp.dot(pick, plane, preferred_element_type=F32).astype(BF16)
        to_side, to_up, to_down, to_side_up, to_side_down = messages(index, buf)
        if index == 8:
            total = jnp.where(has_up, 2, 0) + jnp.where(has_down, 2, 0) + 1
            pl.semaphore_wait(barrier, total)
        to_side.start()

        @pl.when(has_up)
        def _():
            to_up.start()
            to_side_up.start()

        @pl.when(has_down)
        def _():
            to_down.start()
            to_side_down.start()

        if meanwhile is not None:
            meanwhile()
        to_side.wait()

        @pl.when(has_up)
        def _():
            to_up.wait_send()
            to_side_up.wait_send()
            to_down.wait_recv()
            to_side_down.wait_recv()

        @pl.when(has_down)
        def _():
            to_down.wait_send()
            to_side_down.wait_send()
            to_up.wait_recv()
            to_side_up.wait_recv()

        place_at = lax.broadcasted_iota(jnp.int32, (ROWS * SIDE, 3 * SIDE), 0)
        place_from = lax.broadcasted_iota(jnp.int32, (ROWS * SIDE, 3 * SIDE), 1)
        place = (lax.rem(place_at, SIDE) == edge) & (place_at // SIDE + SIDE - 1 == place_from)
        place = place.astype(F32).astype(BF16)
        fix = (factor + 1) * (1 - col)

        def insert(a, carry):
            halo = jnp.concatenate([got[factor], got[a], got[factor + 1]], axis=0)
            put = jnp.dot(place, halo, preferred_element_type=F32)
            plane = buf[a, fix].reshape(ROWS * SIDE, lanes).astype(F32)
            buf[a, fix] = (plane + put).astype(BF16).reshape(ROWS, SIDE, lanes)
            return carry

        lax.fori_loop(0, factor, insert, 0)

    exchange(8, x1, first_weights)
    patch_matrix()
    first_layer()
    conv_layer(h1, cat1, 4, ve1b, be1.at[1:2], 128)
    pool(cat1, p1, 2, 128, 256)
    exchange(0, p1)
    copies[1].wait()
    conv_layer(p1, e2a, 2, ve2a, be2a, 0)
    exchange(1, e2a)
    copies[2].wait()
    conv_layer(e2a, cat2, 2, ve2b, be2b, 384)
    pool(cat2, p2, 1, 384, 384)
    exchange(2, p2)
    copies[3].wait()
    conv_layer(p2, ma, 1, vma, bma, 0)
    exchange(3, ma)
    copies[4].wait()
    mid[...] = conv(ma, 1, 0, vmb, bmb)
    copies[5].wait()
    for p in range(2):
        for q in range(2):
            out = jnp.dot(mid[...], vu2[p, q], preferred_element_type=F32).astype(BF16)
            cat2[p, q + 1, 1:ROWS - 1, :, 0:384] = out.reshape(SIDE, SIDE, 384)
    exchange(4, cat2)
    copies[6].wait()
    conv_layer(cat2, e2a, 2, vd2a, bd2a, 0)
    exchange(5, e2a)
    copies[7].wait()

    def dec2b(a, carry):
        d2[pl.ds(2 * a * PIX, 2 * PIX)] = conv(e2a, 2, a, vd2b, bd2b)
        return carry

    lax.fori_loop(0, 2, dec2b, 0)
    copies[8].wait()

    def up1(t, carry):
        a = t // 2
        p = lax.rem(t, 2)
        lhs = d2[pl.ds(2 * a * PIX, 2 * PIX)]
        for q in range(2):
            out = lax.dot_general(lhs, vu1[p, q], (((1,), (1,)), ((), ())), preferred_element_type=F32).astype(BF16)
            for b in range(2):
                cat1[t, 2 * b + q + 1, 1:ROWS - 1, :, 0:192] = out[b * PIX:(b + 1) * PIX].reshape(SIDE, SIDE, 192)
        return carry

    lax.fori_loop(0, 4, up1, 0)
    exchange(6, cat1)
    copies[9].wait()
    conv_layer(cat1, d1a, 4, vd1a, bd1a, 0, transposed=True)
    exchange(7, d1a)
    copies[10].wait()

    head_bias = jnp.zeros((6, 64), F32)
    for c in range(6):
        head_bias = jnp.where(iota((6, 64), 0) == c, bh[c], head_bias)

    def dec1b(a, carry):
        out = conv(d1a, 4, a, vd1b, bd1b)
        for g in range(4):
            picked = jnp.concatenate([out[b * PIX + g * 64:b * PIX + g * 64 + 64] for b in range(4)], axis=0)
            lines = jnp.dot(weave[...], picked, preferred_element_type=F32).astype(BF16)
            head = lax.dot_general(wh[...], lines, (((1,), (1,)), ((), ())), preferred_element_type=F32)
            for i in range(4):
                y[4 * (4 * g + i) + a] = head[:, i * 64:i * 64 + 64] + head_bias
        return carry

    lax.fori_loop(0, 4, dec1b, 0)


def solution(mesh):
    row_count = mesh.shape["row"]
    tile_spec = P(("data", "row"), "col", None)

    def device_body(image_tile, *params):
        (w_enc1a, b_enc1a, w_enc1b, b_enc1b, w_enc2a, b_enc2a, w_enc2b, b_enc2b,
         w_mid_a, b_mid_a, w_mid_b, b_mid_b, w_up2, w_dec2a, b_dec2a, w_dec2b, b_dec2b,
         w_up1, w_dec1a, b_dec1a, w_dec1b, b_dec1b, w_head, b_head) = params
        anywhere = pl.BlockSpec(memory_space=pl.ANY)
        vmem = pl.BlockSpec(memory_space=pltpu.VMEM)
        operands = [
            jnp.transpose(image_tile, (2, 0, 1)), w_enc1a, w_enc1b, w_enc2a, w_enc2b, w_mid_a, w_mid_b,
            w_up2, w_dec2a, w_dec2b, jnp.swapaxes(w_up1, 2, 3), jnp.swapaxes(w_dec1a, 2, 3), w_dec1b, w_head.T,
            b_enc1a, b_enc1b, b_enc2a, b_enc2b, b_mid_a, b_mid_b, b_dec2a, b_dec2b, b_dec1a, b_dec1b, b_head,
        ]
        specs = [vmem] * 2 + [anywhere] * 11 + [vmem] * 11 + [pl.BlockSpec(memory_space=pltpu.SMEM)]
        level = lambda factor, lanes: pltpu.VMEM((factor, factor + 2, ROWS, SIDE, lanes), BF16)
        scratch = [
            pltpu.VMEM((24, PATCH, 256), BF16), pltpu.VMEM((3, 3, 192, 192), BF16), pltpu.VMEM((3, 3, 256, 256), BF16), pltpu.VMEM((3, 3, 256, 384), BF16),
            pltpu.VMEM((3, 3, 384, 384), BF16), pltpu.VMEM((3, 3, 384, 768), BF16), pltpu.VMEM((3, 3, 768, 768), BF16),
            pltpu.VMEM((2, 2, 768, 384), BF16), pltpu.VMEM((3, 3, 768, 384), BF16), pltpu.VMEM((3, 3, 384, 384), BF16),
            pltpu.VMEM((2, 2, 192, 384), BF16), pltpu.VMEM((3, 3, 192, 384), BF16), pltpu.VMEM((3, 3, 256, 192), BF16),
            level(4, 256), level(4, 384), level(4, 256), level(2, 256), level(2, 384), level(2, 768),
            pltpu.VMEM((4 * PIX, 384), BF16), level(1, 384), level(1, 768), pltpu.VMEM((PIX, 768), BF16),
            level(1, 128), pltpu.VMEM((ROWS * SIDE, PATCH), BF16), pltpu.VMEM((40, 256), F32), pltpu.VMEM((2, 256), F32),
            pltpu.VMEM((PIX, PIX), BF16),
        ]
        scratch += [pltpu.VMEM((f, SIDE, c), BF16) for f, c in zip(EXCHANGE_FACTOR, EXCHANGE_LANES)]
        scratch += [pltpu.VMEM((f + 2, SIDE, c), BF16) for f, c in zip(EXCHANGE_FACTOR, EXCHANGE_LANES)]
        scratch += [pltpu.SemaphoreType.DMA((11,)), pltpu.SemaphoreType.DMA((9, 5)), pltpu.SemaphoreType.DMA((9, 5))]
        out = pl.pallas_call(
            functools.partial(kernel, row_count),
            name="unet",
            out_shape=jax.ShapeDtypeStruct((64, 6, 64), F32),
            in_specs=specs,
            out_specs=vmem,
            scratch_shapes=scratch,
            compiler_params=pltpu.CompilerParams(collective_id=0, has_side_effects=True, vmem_limit_bytes=67043328),
        )(*operands)
        return jnp.transpose(out, (0, 2, 1))

    def program(image, *params):
        mapped = jax.shard_map(device_body, mesh=mesh, in_specs=(tile_spec,) + tuple([P()] * len(params)), out_specs=tile_spec, check_vma=False)
        return mapped(image, *params)

    return program
```

```python
import functools

import jax
import jax.numpy as jnp
from jax import lax
from jax.experimental import pallas as pl
from jax.experimental.pallas import tpu as pltpu
from jax.sharding import PartitionSpec as P

MESH = pl.DeviceIdType.MESH
F32 = jnp.float32
BF16 = jnp.bfloat16
ROWS = 18
SIDE = 16
PIX = SIDE * SIDE
EXT = ROWS * SIDE
C1 = 192
C1P = 256
C2 = 384
C3 = 768
HALF = 64
LANE = 128
PATCH = 192
TAPROWS = 40
BY_ROWS = (((1,), (1,)), ((), ()))
POOL1, ENC2A, POOL2, MIDA, UP2, DEC2A, CAT1, DEC1A, IMAGE, SKIP2 = range(10)
EXCHANGE = ((2, C1P), (2, C2), (1, C2), (1, C3), (2, C2), (2, C2), (4, C2), (4, C1P), (1, LANE), (2, C2))
MESSAGES = 5
LOADS = 19


def iota(shape, dim):
    return lax.broadcasted_iota(jnp.int32, shape, dim)


def grid_iota(*shape):
    return iota(shape, 0), iota(shape, 1)


def ones_at(mask):
    return mask.astype(F32).astype(BF16)


def dot(lhs, rhs):
    return jnp.dot(lhs, rhs, preferred_element_type=F32)


def dot_rows(lhs, rhs):
    return lax.dot_general(lhs, rhs, BY_ROWS, preferred_element_type=F32)


def biased_relu(acc, bias):
    return jnp.maximum(acc + bias[...].reshape(1, bias.shape[-1]), 0.0).astype(BF16)


def kernel(row_count, x, we1a, we1b, we2a, we2b, wma, wmb, wu2, wd2a, wd2b, wu1, wd1a, wd1b, wh,
           be1a, be1b, be2a, be2b, bma, bmb, bd2a, bd2b, bd1a, bd1b, bh, y, *scratch):
    (vw8, re1b, ve1b, ve2a, ve2b, vma, vmb, vu2, vd2a, vu1, vd1a, vd1b,
     h1, cat1, d1a, p1, e2a, cat2, d2, p2, ma, mid, x1, x8, wf, bpad, weave, part) = scratch[:-2 * len(EXCHANGE) - 3]
    send_cols = scratch[-2 * len(EXCHANGE) - 3:-len(EXCHANGE) - 3]
    recv_cols = scratch[-len(EXCHANGE) - 3:-3]
    w_sem, send_sem, recv_sem = scratch[-3:]
    row, col, data = lax.axis_index("row"), lax.axis_index("col"), lax.axis_index("data")
    last = row_count - 1
    has_up, has_down = row > 0, row < last
    up, down = (data, col, row - 1), (data, col, row + 1)
    side, side_up, side_down = (data, 1 - col, row), (data, 1 - col, row - 1), (data, 1 - col, row + 1)
    edge = (1 - col) * (SIDE - 1)

    loads = [(we1b, re1b), (we2a, ve2a.at[:, :, HALF:, :]), (we2b, ve2b), (wma, vma), (wmb, vmb),
             (wu2, vu2), (wd2a, vd2a), (wu1, vu1)]
    loads += [(wd1a.at[t // 3, t % 3], vd1a.at[:C1, pl.ds(t * C2, C2)]) for t in range(9)]
    loads += [(wd1b, vd1b.at[:, :, :C1, :]), (wd2b, ve2b)]
    copies = [pltpu.make_async_copy(src, dst, w_sem.at[k]) for k, (src, dst) in enumerate(loads)]
    for copy in copies[:3]:
        copy.start()
    for buf, factor in ((h1, 4), (cat1, 4), (d1a, 4), (p1, 2), (e2a, 2), (cat2, 2), (p2, 1), (ma, 1), (x1, 1)):
        blank = jnp.zeros(buf.shape[1:2] + buf.shape[3:], BF16)
        buf[0, :, ROWS - 1] = blank
        buf[factor - 1, :, 0] = blank
    for buf, (factor, _) in zip(recv_cols, EXCHANGE):
        buf[factor:] = jnp.zeros((2,) + buf.shape[1:], BF16)

    barrier = pltpu.get_barrier_semaphore()

    def arrive(device):
        pl.semaphore_signal(barrier, inc=1, device_id=device, device_id_type=MESH)

    arrive(side)

    @pl.when(has_up)
    def _():
        arrive(up)
        arrive(side_up)

    @pl.when(has_down)
    def _():
        arrive(down)
        arrive(side_down)

    for copy in copies[3:-1]:
        copy.start()

    def messages(index, buf, lane):
        factor, width = EXCHANGE[index]
        cols, got = send_cols[index], recv_cols[index]
        own = pl.ds(1, factor)
        lanes = pl.ds(lane, width)

        def remote(k, src, dst, device):
            return pltpu.make_async_remote_copy(
                src_ref=src, dst_ref=dst, send_sem=send_sem.at[index, k], recv_sem=recv_sem.at[index, k],
                device_id=device, device_id_type=MESH)

        routes = (
            (cols, got.at[pl.ds(0, factor)], side),
            (buf.at[0, own, 1, :, lanes], buf.at[0, own, ROWS - 1, :, lanes], up),
            (buf.at[factor - 1, own, ROWS - 2, :, lanes], buf.at[factor - 1, own, 0, :, lanes], down),
            (cols.at[0], got.at[factor + 1], side_up),
            (cols.at[factor - 1], got.at[factor], side_down),
        )
        return [remote(k, *route) for k, route in enumerate(routes)]

    def shift(value, right):
        value = value.astype(F32)
        count = value.shape[0]
        at = lax.rem(iota(value.shape, 0), SIDE)
        if right:
            return jnp.where(at == SIDE - 1, 0.0, pltpu.roll(value, count - 1, 0))
        return jnp.where(at == 0, 0.0, pltpu.roll(value, 1, 0))

    def start(index, buf, lane=0):
        factor, width = EXCHANGE[index]
        lanes = pl.ds(lane, width)
        to_side, to_up, to_down, to_side_up, to_side_down = messages(index, buf, lane)
        if index == IMAGE:
            pl.semaphore_wait(barrier, 2 * has_up.astype(jnp.int32) + 2 * has_down.astype(jnp.int32) + 1)

        @pl.when(has_up)
        def _():
            to_up.start()

        @pl.when(has_down)
        def _():
            to_down.start()

        pick_row, pick_at = grid_iota(SIDE, PIX)
        pick = ones_at(pick_at == pick_row * SIDE + edge)
        cols = send_cols[index]
        for a in range(factor):
            plane = buf[a, 1 + (factor - 1) * (1 - col), 1:ROWS - 1, :, lanes].reshape(PIX, width)
            cols[a] = dot(pick, plane).astype(BF16)
        to_side.start()

        @pl.when(has_up)
        def _():
            to_side_up.start()

        @pl.when(has_down)
        def _():
            to_side_down.start()

        def shifted(a):
            for source, target in ((factor, 0), (1, factor + 1)):
                value = shift(buf[a, source, 1:ROWS - 1, :, lanes].reshape(PIX, width), target > 0)
                buf[a, target, 1:ROWS - 1, :, lanes] = value.astype(BF16).reshape(SIDE, SIDE, width)

        if factor == 1:
            shifted(0)
        else:
            pl.loop(0, factor)(shifted)

    def finish(index, buf, lane=0):
        factor, width = EXCHANGE[index]
        lanes = pl.ds(lane, width)
        got = recv_cols[index]
        to_side, to_up, to_down, to_side_up, to_side_down = messages(index, buf, lane)
        to_side.wait()

        @pl.when(has_up)
        def _():
            to_up.wait_send()
            to_side_up.wait_send()
            to_down.wait_recv()
            to_side_down.wait_recv()

        @pl.when(has_down)
        def _():
            to_down.wait_send()
            to_side_down.wait_send()
            to_up.wait_recv()
            to_side_up.wait_recv()

        at, source = grid_iota(EXT, 3 * SIDE)
        place = ones_at((lax.rem(at, SIDE) == edge) & (at // SIDE + SIDE - 1 == source))
        fix = (factor + 1) * (1 - col)
        for a in range(factor):
            put = dot(place, jnp.concatenate([got[factor], got[a], got[factor + 1]], axis=0))
            plane = buf[a, fix, 1:ROWS - 1, :, lanes].reshape(PIX, width).astype(F32) + put[SIDE:EXT - SIDE]
            buf[a, fix, 1:ROWS - 1, :, lanes] = plane.astype(BF16).reshape(SIDE, SIDE, width)
            ends = ([(0, put[:SIDE])] if a == factor - 1 else []) + ([(ROWS - 1, put[EXT - SIDE:])] if a == 0 else [])
            for line, corner in ends:
                left = shift(buf[a, factor, line, :, lanes], False) + jnp.where(col == 1, corner, 0.0)
                right = shift(buf[a, 1, line, :, lanes], True) + jnp.where(col == 0, corner, 0.0)
                buf[a, 0, line, :, lanes] = left.astype(BF16)
                buf[a, factor + 1, line, :, lanes] = right.astype(BF16)

    ALL = [(dy, dx) for dy in range(3) for dx in range(3)]

    def gather(buf, factor, a, bs, taps, lane=0, width=None):
        lanes = pl.ds(lane, buf.shape[-1] if width is None else width)
        rows = []
        for b in bs:
            parts = []
            for dy, dx in taps:
                shifted = a + (dy - 1 + factor)
                piece = buf[lax.rem(shifted, factor), b + dx, pl.ds(shifted // factor, SIDE), :, lanes]
                parts.append(piece.reshape(PIX, piece.shape[-1]))
            rows.append(jnp.concatenate(parts, axis=1))
        return jnp.concatenate(rows, axis=0)

    def conv(buf, factor, a, bs, weight):
        return dot(gather(buf, factor, a, bs, ALL), weight[...].reshape(9 * buf.shape[-1], weight.shape[-1]))

    def put_planes(buf, a, bs, value, lane=0):
        width = value.shape[-1]
        for k, b in enumerate(bs):
            plane = value[k * PIX:(k + 1) * PIX].reshape(SIDE, SIDE, width)
            buf[a, b + 1, 1:ROWS - 1, :, lane:lane + width] = plane

    def pool(src, dst, factor, lane, width):
        for a in range(factor):
            for b in range(factor):
                quad = [src[2 * a + p, 2 * b + q + 1, 1:ROWS - 1, :, lane:lane + width] for p in range(2) for q in range(2)]
                dst[a, b + 1, 1:ROWS - 1] = functools.reduce(jnp.maximum, quad)

    LEVEL2 = [(a, b) for a in range(2) for b in range(2)]

    def near(a, b):
        return [(dy, dx) for dy, dx in ALL if dy != 2 * a and dx != 2 * b]

    def weights_of(weight, taps):
        return jnp.concatenate([weight[dy, dx] for dy, dx in taps], axis=0)

    def conv_level2(index, src, weight, bias, put):
        start(index, src)
        for a, b in LEVEL2:
            taps = near(a, b)
            part[2 * a + b] = dot(gather(src, 2, a, (b,), taps), weights_of(weight, taps))
        finish(index, src)
        for a, b in LEVEL2:
            taps = [tap for tap in ALL if tap not in near(a, b)]
            acc = part[2 * a + b] + dot(gather(src, 2, a, (b,), taps), weights_of(weight, taps))
            put(a, b, biased_relu(acc, bias))

    at, to = grid_iota(HALF, HALF)
    split_cols = ones_at(at == lax.rem(to, SIDE) * 4 + to // SIDE)
    at, to = grid_iota(PIX, HALF)
    own_col = lax.rem(at, SIDE) == lax.rem(to, SIDE)
    fold_at, fold_to = grid_iota(HALF, LANE)
    image = []
    for ch in range(3):
        cols = dot(x[ch], split_cols).astype(BF16)
        for a in range(4):
            spread = ones_at(to == (at // SIDE) * 4 + a)
            lines = jnp.where(own_col, dot(spread, cols), 0.0).astype(BF16)
            image.append(dot(lines, ones_at(fold_to == fold_at // SIDE + (ch * SIDE + a * 4))))
    x1[0, 1, 1:ROWS - 1] = sum(image[1:], image[0]).astype(BF16).reshape(SIDE, SIDE, LANE)
    start(IMAGE, x1)

    wf[...] = jnp.zeros(wf.shape, F32)
    for t in range(9):
        wf[pl.ds(4 * t, 3), :C1] = we1a[t // 3, t % 3].astype(F32)
    k, m = grid_iota(PATCH, TAPROWS)
    py, px = k // 32, lax.rem(k, 32) // 4
    base = py * 12 + px * 4 + lax.rem(k, 4)

    @pl.loop(0, 4)
    def _(a):
        for b in range(6):
            good = (py >= a) & (py <= a + 2) & (px >= b) & (px <= b + 2)
            place = ones_at(good & (m == base - a * 12 - b * 4))
            vw8[a * 6 + b] = dot(place, wf[...].astype(BF16)).astype(BF16)

    pad = jnp.zeros((1, HALF), F32)
    bpad[0:1, :] = jnp.concatenate([be1a[...].reshape(1, C1), pad], axis=1)
    bpad[1:2, :] = jnp.concatenate([pad, be1b[...].reshape(1, C1)], axis=1)
    bpad[2:3, :] = jnp.concatenate([bd1a[...].reshape(1, C1), pad], axis=1)
    n, m = grid_iota(PIX, PIX)
    weave[...] = ones_at(m == lax.rem(n, 4) * HALF + (n // HALF) * SIDE + lax.rem(n, HALF) // 4)
    ve2a[:, :, :HALF, :] = jnp.zeros((3, 3, HALF, C2), BF16)
    vd1b[:, :, C1:, :] = jnp.zeros((3, 3, HALF, C1), BF16)
    vd1a[C1:, :] = jnp.zeros((HALF, vd1a.shape[1]), BF16)
    copies[0].wait()

    @pl.loop(0, 3)
    def _(dy):
        for dx in range(3):
            value = jnp.concatenate([jnp.zeros((C1, HALF), F32), re1b[dy, dx].astype(F32)], axis=1)
            ve1b[dy, dx, :C1] = value.astype(BF16)
            ve1b[dy, dx, C1:] = jnp.zeros((HALF, C1P), BF16)

    finish(IMAGE, x1)

    blank = jnp.zeros((SIDE, LANE), BF16)
    lane, k = grid_iota(LANE, PATCH)
    ch, a, b = lane // SIDE, lax.rem(lane, SIDE) // 4, lax.rem(lane, 4)
    patches = []
    for dx in range(3):
        plane = x1[0, dx].reshape(EXT, LANE)
        blocks = (jnp.concatenate([blank, plane[:-SIDE]], axis=0), plane, jnp.concatenate([plane[SIDE:], blank], axis=0))
        for dy, block in enumerate(blocks):
            py, px = a + (4 * dy - 3), b + (4 * dx - 2)
            good = (ch < 3) & (py >= 0) & (py < 6) & (px >= 0) & (px < 8)
            patches.append(dot(block, ones_at(good & (k == py * 32 + px * 4 + ch))))
    x8[...] = sum(patches[1:], patches[0]).astype(BF16)

    pos = iota((EXT, C1P), 0)
    pos_row, pos_col = pos // SIDE, lax.rem(pos, SIDE)
    off_rows = ((pos_row == 0) & (row == 0)) | ((pos_row == ROWS - 1) & (row == last))
    off = {0: off_rows | ((pos_col == 0) & (col == 0)), 5: off_rows | ((pos_col == SIDE - 1) & (col == 1))}

    @pl.loop(0, 4)
    def _(a):
        for b in range(6):
            acc = dot(x8[...], vw8[a * 6 + b])
            out = jnp.where(off.get(b, off_rows), 0.0, jnp.maximum(acc + bpad[0:1, :], 0.0))
            h1[a, b] = out.astype(BF16).reshape(ROWS, SIDE, C1P)

    @pl.loop(0, 4)
    def _(a):
        put_planes(cat1, a, range(4), biased_relu(conv(h1, 4, a, range(4), ve1b), bpad.at[1:2]), LANE)

    pool(cat1, p1, 2, LANE, C1P)

    copies[1].wait()
    conv_level2(POOL1, p1, ve2a, be2a, lambda a, b, value: put_planes(e2a, a, (b,), value))
    copies[2].wait()
    conv_level2(ENC2A, e2a, ve2b, be2b, lambda a, b, value: put_planes(cat2, a, (b,), value, C2))
    copies[-1].start()
    pool(cat2, p2, 1, C2, C2)

    start(POOL2, p2)
    start(SKIP2, cat2, C2)
    copies[3].wait()
    finish(POOL2, p2)
    put_planes(ma, 0, (0,), biased_relu(conv(p2, 1, 0, (0,), vma), bma))
    start(MIDA, ma)
    copies[6].wait()
    finish(SKIP2, cat2, C2)

    def half_dec2a(a, lane):
        flat = jnp.concatenate([vd2a[dy, dx, lane:lane + C2] for dy, dx in ALL], axis=0)
        return dot(gather(cat2, 2, a, range(2), ALL, lane, C2), flat)

    part[:2] = half_dec2a(0, C2).reshape(2, PIX, C2)
    copies[4].wait()
    finish(MIDA, ma)
    mid[...] = biased_relu(conv(ma, 1, 0, (0,), vmb), bmb)
    copies[5].wait()
    for p, q in LEVEL2:
        put_planes(cat2, p, (q,), dot(mid[...], vu2[p, q]).astype(BF16))
    start(UP2, cat2)
    part[2:] = half_dec2a(1, C2).reshape(2, PIX, C2)
    finish(UP2, cat2)

    @pl.loop(0, 2)
    def _(a):
        put_planes(e2a, a, range(2), biased_relu(part[pl.ds(2 * a, 2)].reshape(2 * PIX, C2) + half_dec2a(a, 0), bd2a))

    copies[-1].wait()

    def put_d2(a, b, value):
        d2[pl.ds((2 * a + b) * PIX, PIX)] = value

    conv_level2(DEC2A, e2a, ve2b, bd2b, put_d2)
    copies[7].wait()

    @pl.loop(0, 4)
    def _(t):
        p = lax.rem(t, 2)
        lhs = d2[pl.ds((t - p) * PIX, 2 * PIX)]
        for q in range(2):
            put_planes(cat1, t, (q, q + 2), dot_rows(lhs, vu1[p, q]).astype(BF16))

    for copy in copies[8:17]:
        copy.wait()

    def level1(index, src, layer):
        start(index, src)
        pl.loop(1, 3)(lambda a: layer(a, (1, 2)))
        finish(index, src)
        pl.loop(1, 3)(lambda a: layer(a, (0, 3)))
        pl.loop(0, 2)(lambda t: layer(3 * t, range(4)))

    def dec1a(a, bs):
        put_planes(d1a, a, bs, biased_relu(dot_rows(gather(cat1, 4, a, bs, ALL), vd1a[...]), bpad.at[2:3]))

    level1(CAT1, cat1, dec1a)
    copies[17].wait()
    head_bias = jnp.zeros((6, HALF), F32)
    for c in range(6):
        head_bias = jnp.where(iota(head_bias.shape, 0) == c, bh[c], head_bias)

    def dec1b(a, bs):
        put_planes(h1, a, bs, biased_relu(conv(d1a, 4, a, bs, vd1b), bd1b))
        if 0 not in bs:
            return
        for g in range(4):
            lines = pl.ds(4 * g + 1, 4)
            picked = jnp.concatenate([h1[a, b + 1, lines, :, :C1].reshape(HALF, C1) for b in range(4)], axis=0)
            head = dot_rows(wh[...], dot(weave[...], picked).astype(BF16))
            for i in range(4):
                y[4 * (4 * g + i) + a] = head[:, i * HALF:(i + 1) * HALF] + head_bias

    level1(DEC1A, d1a, dec1b)


def solution(mesh):
    tile_spec = P(("data", "row"), "col", None)

    def device_body(image_tile, *params):
        (w_enc1a, b_enc1a, w_enc1b, b_enc1b, w_enc2a, b_enc2a, w_enc2b, b_enc2b,
         w_mid_a, b_mid_a, w_mid_b, b_mid_b, w_up2, w_dec2a, b_dec2a, w_dec2b, b_dec2b,
         w_up1, w_dec1a, b_dec1a, w_dec1b, b_dec1b, w_head, b_head) = params
        anywhere = pl.BlockSpec(memory_space=pl.ANY)
        vmem = pl.BlockSpec(memory_space=pltpu.VMEM)
        operands = [
            jnp.transpose(image_tile, (2, 0, 1)), w_enc1a, w_enc1b, w_enc2a, w_enc2b, w_mid_a, w_mid_b,
            w_up2, w_dec2a, w_dec2b, jnp.swapaxes(w_up1, 2, 3), jnp.swapaxes(w_dec1a, 2, 3), w_dec1b, w_head.T,
            b_enc1a, b_enc1b, b_enc2a, b_enc2b, b_mid_a, b_mid_b, b_dec2a, b_dec2b, b_dec1a, b_dec1b, b_head,
        ]
        specs = [vmem] * 2 + [anywhere] * 11 + [vmem] * 11 + [pl.BlockSpec(memory_space=pltpu.SMEM)]

        def kept(*shape, dtype=BF16):
            return pltpu.VMEM(shape, dtype)

        def level(factor, lanes):
            return kept(factor, factor + 2, ROWS, SIDE, lanes)

        scratch = [
            kept(24, PATCH, C1P), kept(3, 3, C1, C1), kept(3, 3, C1P, C1P), kept(3, 3, C1P, C2), kept(3, 3, C2, C2),
            kept(3, 3, C2, C3), kept(3, 3, C3, C3), kept(2, 2, C3, C2), kept(3, 3, C3, C2),
            kept(2, 2, C1, C2), kept(C1P, 9 * C2), kept(3, 3, C1P, C1),
            level(4, C1P), level(4, C2), level(4, C1P), level(2, C1P), level(2, C2), level(2, C3),
            kept(4 * PIX, C2), level(1, C2), level(1, C3), kept(PIX, C3), level(1, LANE), kept(EXT, PATCH),
            kept(TAPROWS, C1P, dtype=F32), kept(3, C1P, dtype=F32), kept(PIX, PIX),
            kept(4, PIX, C2, dtype=F32),
        ]
        scratch += [kept(factor, SIDE, width) for factor, width in EXCHANGE]
        scratch += [kept(factor + 2, SIDE, width) for factor, width in EXCHANGE]
        links = pltpu.SemaphoreType.DMA((len(EXCHANGE), MESSAGES))
        scratch += [pltpu.SemaphoreType.DMA((LOADS,)), links, links]
        out = pl.pallas_call(
            functools.partial(kernel, mesh.shape["row"]),
            name="unet",
            out_shape=jax.ShapeDtypeStruct((HALF, 6, HALF), F32),
            in_specs=specs,
            out_specs=vmem,
            scratch_shapes=scratch,
            compiler_params=pltpu.CompilerParams(collective_id=0, has_side_effects=True, vmem_limit_bytes=67043328),
        )(*operands)
        return jnp.transpose(out, (0, 2, 1))

    def program(image, *params):
        mapped = jax.shard_map(device_body, mesh=mesh, in_specs=(tile_spec,) + tuple([P()] * len(params)), out_specs=tile_spec, check_vma=False)
        return mapped(image, *params)

    return program
```

```python
import functools

import jax
import jax.numpy as jnp
from jax import lax
from jax.experimental import pallas as pl
from jax.experimental.pallas import tpu as pltpu
from jax.sharding import PartitionSpec as P

MESH = pl.DeviceIdType.MESH
F32 = jnp.float32
BF16 = jnp.bfloat16
ROWS = 18
SIDE = 16
PIX = SIDE * SIDE
EXT = ROWS * SIDE
C1 = 192
C1P = 256
C2 = 384
C3 = 768
HALF = 64
LANE = 128
PATCH = 192
TAPROWS = 40
BY_ROWS = (((1,), (1,)), ((), ()))
POOL1, ENC2A, POOL2, MIDA, UP2, DEC2A, CAT1, DEC1A, IMAGE, SKIP2 = range(10)
EXCHANGE = ((2, C1P), (2, C2), (1, C2), (1, C3), (2, C2), (2, C2), (4, C2), (4, C1P), (1, LANE), (2, C2))
MESSAGES = 5
LOADS = 19


def iota(shape, dim):
    return lax.broadcasted_iota(jnp.int32, shape, dim)


def grid_iota(*shape):
    return iota(shape, 0), iota(shape, 1)


def ones_at(mask):
    return mask.astype(F32).astype(BF16)


def dot(lhs, rhs):
    return jnp.dot(lhs, rhs, preferred_element_type=F32)


def dot_rows(lhs, rhs):
    return lax.dot_general(lhs, rhs, BY_ROWS, preferred_element_type=F32)


def biased_relu(acc, bias):
    return jnp.maximum(acc + bias[...].reshape(1, bias.shape[-1]), 0.0).astype(BF16)


def kernel(row_count, x, we1a, we1b, we2a, we2b, wma, wmb, wu2, wd2a, wd2b, wu1, wd1a, wd1b, wh,
           be1a, be1b, be2a, be2b, bma, bmb, bd2a, bd2b, bd1a, bd1b, bh, y, *scratch):
    (vw8, re1b, ve1b, ve2a, ve2b, vma, vmb, vu2, vd2a, vu1, vd1a, vd1b,
     h1, cat1, d1a, p1, e2a, cat2, d2, p2, ma, mid, x1, x8, wf, bpad, weave, part) = scratch[:-2 * len(EXCHANGE) - 3]
    send_cols = scratch[-2 * len(EXCHANGE) - 3:-len(EXCHANGE) - 3]
    recv_cols = scratch[-len(EXCHANGE) - 3:-3]
    w_sem, send_sem, recv_sem = scratch[-3:]
    row, col, data = lax.axis_index("row"), lax.axis_index("col"), lax.axis_index("data")
    last = row_count - 1
    has_up, has_down = row > 0, row < last
    up, down = (data, col, row - 1), (data, col, row + 1)
    side, side_up, side_down = (data, 1 - col, row), (data, 1 - col, row - 1), (data, 1 - col, row + 1)
    edge = (1 - col) * (SIDE - 1)

    loads = [(we1b, re1b), (we2a, ve2a.at[:, :, HALF:, :]), (we2b, ve2b), (wma, vma), (wmb, vmb),
             (wu2, vu2), (wd2a, vd2a), (wu1, vu1)]
    loads += [(wd1a.at[t // 3, t % 3], vd1a.at[:C1, pl.ds(t * C2, C2)]) for t in range(9)]
    loads += [(wd1b, vd1b.at[:, :, :C1, :]), (wd2b, ve2b)]
    copies = [pltpu.make_async_copy(src, dst, w_sem.at[k]) for k, (src, dst) in enumerate(loads)]
    for copy in copies[:3]:
        copy.start()
    for buf, factor in ((h1, 4), (cat1, 4), (d1a, 4), (p1, 2), (e2a, 2), (cat2, 2), (p2, 1), (ma, 1), (x1, 1)):
        blank = jnp.zeros(buf.shape[1:2] + buf.shape[3:], BF16)
        buf[0, :, ROWS - 1] = blank
        buf[factor - 1, :, 0] = blank
    for buf, (factor, _) in zip(recv_cols, EXCHANGE):
        buf[factor:] = jnp.zeros((2,) + buf.shape[1:], BF16)

    barrier = pltpu.get_barrier_semaphore()

    def arrive(device):
        pl.semaphore_signal(barrier, inc=1, device_id=device, device_id_type=MESH)

    arrive(side)

    @pl.when(has_up)
    def _():
        arrive(up)
        arrive(side_up)

    @pl.when(has_down)
    def _():
        arrive(down)
        arrive(side_down)

    for copy in copies[3:-1]:
        copy.start()

    def messages(index, buf, lane):
        factor, width = EXCHANGE[index]
        cols, got = send_cols[index], recv_cols[index]
        own = pl.ds(1, factor)
        lanes = pl.ds(lane, width)

        def remote(k, src, dst, device):
            return pltpu.make_async_remote_copy(
                src_ref=src, dst_ref=dst, send_sem=send_sem.at[index, k], recv_sem=recv_sem.at[index, k],
                device_id=device, device_id_type=MESH)

        routes = (
            (cols, got.at[pl.ds(0, factor)], side),
            (buf.at[0, own, 1, :, lanes], buf.at[0, own, ROWS - 1, :, lanes], up),
            (buf.at[factor - 1, own, ROWS - 2, :, lanes], buf.at[factor - 1, own, 0, :, lanes], down),
            (cols.at[0], got.at[factor + 1], side_up),
            (cols.at[factor - 1], got.at[factor], side_down),
        )
        return [remote(k, *route) for k, route in enumerate(routes)]

    def shift(value, right):
        value = value.astype(F32)
        count = value.shape[0]
        at = lax.rem(iota(value.shape, 0), SIDE)
        if right:
            return jnp.where(at == SIDE - 1, 0.0, pltpu.roll(value, count - 1, 0))
        return jnp.where(at == 0, 0.0, pltpu.roll(value, 1, 0))

    def start(index, buf, lane=0):
        factor, width = EXCHANGE[index]
        lanes = pl.ds(lane, width)
        to_side, to_up, to_down, to_side_up, to_side_down = messages(index, buf, lane)
        if index == IMAGE:
            pl.semaphore_wait(barrier, 2 * has_up.astype(jnp.int32) + 2 * has_down.astype(jnp.int32) + 1)

        @pl.when(has_up)
        def _():
            to_up.start()

        @pl.when(has_down)
        def _():
            to_down.start()

        pick_row, pick_at = grid_iota(SIDE, PIX)
        pick = ones_at(pick_at == pick_row * SIDE + edge)
        cols = send_cols[index]
        for a in range(factor):
            plane = buf[a, 1 + (factor - 1) * (1 - col), 1:ROWS - 1, :, lanes].reshape(PIX, width)
            cols[a] = dot(pick, plane).astype(BF16)
        to_side.start()

        @pl.when(has_up)
        def _():
            to_side_up.start()

        @pl.when(has_down)
        def _():
            to_side_down.start()

        def shifted(a):
            for source, target in ((factor, 0), (1, factor + 1)):
                value = shift(buf[a, source, 1:ROWS - 1, :, lanes].reshape(PIX, width), target > 0)
                buf[a, target, 1:ROWS - 1, :, lanes] = value.astype(BF16).reshape(SIDE, SIDE, width)

        if factor == 1:
            shifted(0)
        else:
            pl.loop(0, factor)(shifted)

    def finish(index, buf, lane=0):
        factor, width = EXCHANGE[index]
        lanes = pl.ds(lane, width)
        got = recv_cols[index]
        to_side, to_up, to_down, to_side_up, to_side_down = messages(index, buf, lane)
        to_side.wait()

        @pl.when(has_up)
        def _():
            to_up.wait_send()
            to_side_up.wait_send()
            to_down.wait_recv()
            to_side_down.wait_recv()

        @pl.when(has_down)
        def _():
            to_down.wait_send()
            to_side_down.wait_send()
            to_up.wait_recv()
            to_side_up.wait_recv()

        at, source = grid_iota(EXT, 3 * SIDE)
        place = ones_at((lax.rem(at, SIDE) == edge) & (at // SIDE + SIDE - 1 == source))
        fix = (factor + 1) * (1 - col)
        for a in range(factor):
            put = dot(place, jnp.concatenate([got[factor], got[a], got[factor + 1]], axis=0))
            plane = buf[a, fix, 1:ROWS - 1, :, lanes].reshape(PIX, width).astype(F32) + put[SIDE:EXT - SIDE]
            buf[a, fix, 1:ROWS - 1, :, lanes] = plane.astype(BF16).reshape(SIDE, SIDE, width)
            ends = ([(0, put[:SIDE])] if a == factor - 1 else []) + ([(ROWS - 1, put[EXT - SIDE:])] if a == 0 else [])
            for line, corner in ends:
                left = shift(buf[a, factor, line, :, lanes], False) + jnp.where(col == 1, corner, 0.0)
                right = shift(buf[a, 1, line, :, lanes], True) + jnp.where(col == 0, corner, 0.0)
                buf[a, 0, line, :, lanes] = left.astype(BF16)
                buf[a, factor + 1, line, :, lanes] = right.astype(BF16)

    ALL = [(dy, dx) for dy in range(3) for dx in range(3)]

    def gather(buf, factor, a, bs, taps, lane=0, width=None):
        lanes = pl.ds(lane, buf.shape[-1] if width is None else width)
        rows = []
        for b in bs:
            parts = []
            for dy, dx in taps:
                shifted = a + (dy - 1 + factor)
                piece = buf[lax.rem(shifted, factor), b + dx, pl.ds(shifted // factor, SIDE), :, lanes]
                parts.append(piece.reshape(PIX, piece.shape[-1]))
            rows.append(jnp.concatenate(parts, axis=1))
        return jnp.concatenate(rows, axis=0)

    def conv(buf, factor, a, bs, weight):
        return dot(gather(buf, factor, a, bs, ALL), weight[...].reshape(9 * buf.shape[-1], weight.shape[-1]))

    def put_planes(buf, a, bs, value, lane=0):
        width = value.shape[-1]
        for k, b in enumerate(bs):
            plane = value[k * PIX:(k + 1) * PIX].reshape(SIDE, SIDE, width)
            buf[a, b + 1, 1:ROWS - 1, :, lane:lane + width] = plane

    def pool(src, dst, factor, lane, width):
        for a in range(factor):
            for b in range(factor):
                quad = [src[2 * a + p, 2 * b + q + 1, 1:ROWS - 1, :, lane:lane + width] for p in range(2) for q in range(2)]
                dst[a, b + 1, 1:ROWS - 1] = functools.reduce(jnp.maximum, quad)

    LEVEL2 = [(a, b) for a in range(2) for b in range(2)]

    def plane_of(buf, a, b, line, lane, width):
        return buf[a, b, pl.ds(line, SIDE), :, pl.ds(lane, width)].reshape(PIX, width)

    def near(a, b, buf, weight, lane, width):
        lhs = [plane_of(buf, k, l + 1, 1, lane, width) for k, l in LEVEL2]
        rhs = [weight[k - a + 1, l - b + 1, lane:lane + width] for k, l in LEVEL2]
        return dot(jnp.concatenate(lhs, axis=1), jnp.concatenate(rhs, axis=0))

    def far(a, b, buf, weight, lane, width):
        lhs = [plane_of(buf, 1 - a, b + dx, 2 * a, lane, width) for dx in range(3)]
        lhs += [plane_of(buf, k, 3 * b, 1, lane, width) for k in range(2)]
        rhs = [weight[2 * a, dx, lane:lane + width] for dx in range(3)]
        rhs += [weight[k - a + 1, 2 * b, lane:lane + width] for k in range(2)]
        return dot(jnp.concatenate(lhs, axis=1), jnp.concatenate(rhs, axis=0))

    def over_level2(terms, put, *operands):
        @pl.loop(0, 2)
        def _(a):
            for b in range(2):
                put(a, b, terms(a, b, *operands))

    def keep(a, b, value):
        part[2 * a + b] = value

    def add(a, b, value):
        part[2 * a + b] += value

    def done(bias, put):
        return lambda a, b, value: put(a, b, biased_relu(part[2 * a + b] + value, bias))

    def conv_level2(index, src, weight, bias, put):
        width = src.shape[-1]
        start(index, src)
        over_level2(near, keep, src, weight, 0, width)
        finish(index, src)
        over_level2(far, done(bias, put), src, weight, 0, width)

    at, to = grid_iota(HALF, HALF)
    split_cols = ones_at(at == lax.rem(to, SIDE) * 4 + to // SIDE)
    at, to = grid_iota(PIX, HALF)
    own_col = lax.rem(at, SIDE) == lax.rem(to, SIDE)
    fold_at, fold_to = grid_iota(HALF, LANE)
    image = []
    for ch in range(3):
        cols = dot(x[ch], split_cols).astype(BF16)
        for a in range(4):
            spread = ones_at(to == (at // SIDE) * 4 + a)
            lines = jnp.where(own_col, dot(spread, cols), 0.0).astype(BF16)
            image.append(dot(lines, ones_at(fold_to == fold_at // SIDE + (ch * SIDE + a * 4))))
    x1[0, 1, 1:ROWS - 1] = sum(image[1:], image[0]).astype(BF16).reshape(SIDE, SIDE, LANE)
    start(IMAGE, x1)

    wf[...] = jnp.zeros(wf.shape, F32)
    for t in range(9):
        wf[pl.ds(4 * t, 3), :C1] = we1a[t // 3, t % 3].astype(F32)
    k, m = grid_iota(PATCH, TAPROWS)
    py, px = k // 32, lax.rem(k, 32) // 4
    base = py * 12 + px * 4 + lax.rem(k, 4)

    @pl.loop(0, 4)
    def _(a):
        for b in range(6):
            good = (py >= a) & (py <= a + 2) & (px >= b) & (px <= b + 2)
            place = ones_at(good & (m == base - a * 12 - b * 4))
            vw8[a * 6 + b] = dot(place, wf[...].astype(BF16)).astype(BF16)

    pad = jnp.zeros((1, HALF), F32)
    bpad[0:1, :] = jnp.concatenate([be1a[...].reshape(1, C1), pad], axis=1)
    bpad[1:2, :] = jnp.concatenate([pad, be1b[...].reshape(1, C1)], axis=1)
    bpad[2:3, :] = jnp.concatenate([bd1a[...].reshape(1, C1), pad], axis=1)
    n, m = grid_iota(PIX, PIX)
    weave[...] = ones_at(m == lax.rem(n, 4) * HALF + (n // HALF) * SIDE + lax.rem(n, HALF) // 4)
    ve2a[:, :, :HALF, :] = jnp.zeros((3, 3, HALF, C2), BF16)
    vd1b[:, :, C1:, :] = jnp.zeros((3, 3, HALF, C1), BF16)
    vd1a[C1:, :] = jnp.zeros((HALF, vd1a.shape[1]), BF16)
    copies[0].wait()

    @pl.loop(0, 3)
    def _(dy):
        for dx in range(3):
            value = jnp.concatenate([jnp.zeros((C1, HALF), F32), re1b[dy, dx].astype(F32)], axis=1)
            ve1b[dy, dx, :C1] = value.astype(BF16)
            ve1b[dy, dx, C1:] = jnp.zeros((HALF, C1P), BF16)

    finish(IMAGE, x1)

    blank = jnp.zeros((SIDE, LANE), BF16)
    lane, k = grid_iota(LANE, PATCH)
    ch, a, b = lane // SIDE, lax.rem(lane, SIDE) // 4, lax.rem(lane, 4)
    patches = []
    for dx in range(3):
        plane = x1[0, dx].reshape(EXT, LANE)
        blocks = (jnp.concatenate([blank, plane[:-SIDE]], axis=0), plane, jnp.concatenate([plane[SIDE:], blank], axis=0))
        for dy, block in enumerate(blocks):
            py, px = a + (4 * dy - 3), b + (4 * dx - 2)
            good = (ch < 3) & (py >= 0) & (py < 6) & (px >= 0) & (px < 8)
            patches.append(dot(block, ones_at(good & (k == py * 32 + px * 4 + ch))))
    x8[...] = sum(patches[1:], patches[0]).astype(BF16)

    pos = iota((EXT, C1P), 0)
    pos_row, pos_col = pos // SIDE, lax.rem(pos, SIDE)
    off_rows = ((pos_row == 0) & (row == 0)) | ((pos_row == ROWS - 1) & (row == last))
    off = {0: off_rows | ((pos_col == 0) & (col == 0)), 5: off_rows | ((pos_col == SIDE - 1) & (col == 1))}

    @pl.loop(0, 4)
    def _(a):
        for b in range(6):
            acc = dot(x8[...], vw8[a * 6 + b])
            out = jnp.where(off.get(b, off_rows), 0.0, jnp.maximum(acc + bpad[0:1, :], 0.0))
            h1[a, b] = out.astype(BF16).reshape(ROWS, SIDE, C1P)

    @pl.loop(0, 2)
    def _(t):
        for a in (2 * t, 2 * t + 1):
            put_planes(cat1, a, range(4), biased_relu(conv(h1, 4, a, range(4), ve1b), bpad.at[1:2]), LANE)

    pool(cat1, p1, 2, LANE, C1P)

    copies[1].wait()
    conv_level2(POOL1, p1, ve2a, be2a, lambda a, b, value: put_planes(e2a, a, (b,), value))
    copies[2].wait()
    conv_level2(ENC2A, e2a, ve2b, be2b, lambda a, b, value: put_planes(cat2, a, (b,), value, C2))
    copies[-1].start()
    pool(cat2, p2, 1, C2, C2)

    start(POOL2, p2)
    start(SKIP2, cat2, C2)
    copies[6].wait()
    over_level2(near, keep, cat2, vd2a, C2, C2)
    copies[3].wait()
    finish(POOL2, p2)
    put_planes(ma, 0, (0,), biased_relu(conv(p2, 1, 0, (0,), vma), bma))
    start(MIDA, ma)
    finish(SKIP2, cat2, C2)
    over_level2(far, add, cat2, vd2a, C2, C2)
    copies[4].wait()
    finish(MIDA, ma)
    mid[...] = biased_relu(conv(ma, 1, 0, (0,), vmb), bmb)
    copies[5].wait()
    for p, q in LEVEL2:
        put_planes(cat2, p, (q,), dot(mid[...], vu2[p, q]).astype(BF16))
    start(UP2, cat2)
    over_level2(near, add, cat2, vd2a, 0, C2)
    finish(UP2, cat2)
    over_level2(far, done(bd2a, lambda a, b, value: put_planes(e2a, a, (b,), value)), cat2, vd2a, 0, C2)
    copies[-1].wait()

    def put_d2(a, b, value):
        d2[pl.ds((2 * a + b) * PIX, PIX)] = value

    conv_level2(DEC2A, e2a, ve2b, bd2b, put_d2)
    copies[7].wait()

    @pl.loop(0, 2)
    def _(t):
        lhs = d2[pl.ds(2 * t * PIX, 2 * PIX)]
        for p, q in LEVEL2:
            put_planes(cat1, 2 * t + p, (q, q + 2), dot_rows(lhs, vu1[p, q]).astype(BF16))

    for copy in copies[8:17]:
        copy.wait()

    def level1(index, src, layer):
        start(index, src)
        for a in range(1, 3):
            layer(a, (1, 2))
        finish(index, src)
        for a in range(1, 3):
            layer(a, (0, 3))
        for a in (0, 3):
            layer(a, range(4))

    def dec1a(a, bs):
        put_planes(d1a, a, bs, biased_relu(dot_rows(gather(cat1, 4, a, bs, ALL), vd1a[...]), bpad.at[2:3]))

    level1(CAT1, cat1, dec1a)
    copies[17].wait()
    head_bias = jnp.zeros((6, HALF), F32)
    for c in range(6):
        head_bias = jnp.where(iota(head_bias.shape, 0) == c, bh[c], head_bias)

    def dec1b(a, bs):
        put_planes(h1, a, bs, biased_relu(conv(d1a, 4, a, bs, vd1b), bd1b))
        if 0 not in bs:
            return
        for g in range(4):
            lines = pl.ds(4 * g + 1, 4)
            picked = jnp.concatenate([h1[a, b + 1, lines, :, :C1].reshape(HALF, C1) for b in range(4)], axis=0)
            head = dot_rows(wh[...], dot(weave[...], picked).astype(BF16))
            for i in range(4):
                y[:, 4 * (4 * g + i) + a, :] = head[:, i * HALF:(i + 1) * HALF] + head_bias

    level1(DEC1A, d1a, dec1b)


def solution(mesh):
    tile_spec = P(("data", "row"), "col", None)

    def device_body(image_tile, *params):
        (w_enc1a, b_enc1a, w_enc1b, b_enc1b, w_enc2a, b_enc2a, w_enc2b, b_enc2b,
         w_mid_a, b_mid_a, w_mid_b, b_mid_b, w_up2, w_dec2a, b_dec2a, w_dec2b, b_dec2b,
         w_up1, w_dec1a, b_dec1a, w_dec1b, b_dec1b, w_head, b_head) = params
        anywhere = pl.BlockSpec(memory_space=pl.ANY)
        vmem = pl.BlockSpec(memory_space=pltpu.VMEM)
        operands = [
            jnp.transpose(image_tile, (2, 0, 1)), w_enc1a, w_enc1b, w_enc2a, w_enc2b, w_mid_a, w_mid_b,
            w_up2, w_dec2a, w_dec2b, jnp.swapaxes(w_up1, 2, 3), jnp.swapaxes(w_dec1a, 2, 3), w_dec1b, w_head.T,
            b_enc1a, b_enc1b, b_enc2a, b_enc2b, b_mid_a, b_mid_b, b_dec2a, b_dec2b, b_dec1a, b_dec1b, b_head,
        ]
        specs = [vmem] * 2 + [anywhere] * 11 + [vmem] * 11 + [pl.BlockSpec(memory_space=pltpu.SMEM)]

        def kept(*shape, dtype=BF16):
            return pltpu.VMEM(shape, dtype)

        def level(factor, lanes):
            return kept(factor, factor + 2, ROWS, SIDE, lanes)

        scratch = [
            kept(24, PATCH, C1P), kept(3, 3, C1, C1), kept(3, 3, C1P, C1P), kept(3, 3, C1P, C2), kept(3, 3, C2, C2),
            kept(3, 3, C2, C3), kept(3, 3, C3, C3), kept(2, 2, C3, C2), kept(3, 3, C3, C2),
            kept(2, 2, C1, C2), kept(C1P, 9 * C2), kept(3, 3, C1P, C1),
            level(4, C1P), level(4, C2), level(4, C1P), level(2, C1P), level(2, C2), level(2, C3),
            kept(4 * PIX, C2), level(1, C2), level(1, C3), kept(PIX, C3), level(1, LANE), kept(EXT, PATCH),
            kept(TAPROWS, C1P, dtype=F32), kept(3, C1P, dtype=F32), kept(PIX, PIX),
            kept(4, PIX, C2, dtype=F32),
        ]
        scratch += [kept(factor, SIDE, width) for factor, width in EXCHANGE]
        scratch += [kept(factor + 2, SIDE, width) for factor, width in EXCHANGE]
        links = pltpu.SemaphoreType.DMA((len(EXCHANGE), MESSAGES))
        scratch += [pltpu.SemaphoreType.DMA((LOADS,)), links, links]
        out = pl.pallas_call(
            functools.partial(kernel, mesh.shape["row"]),
            name="unet",
            out_shape=jax.ShapeDtypeStruct((6, HALF, HALF), F32),
            in_specs=specs,
            out_specs=vmem,
            scratch_shapes=scratch,
            compiler_params=pltpu.CompilerParams(collective_id=0, has_side_effects=True, vmem_limit_bytes=67043328),
        )(*operands)
        return jnp.transpose(out, (1, 2, 0))

    def program(image, *params):
        mapped = jax.shard_map(device_body, mesh=mesh, in_specs=(tile_spec,) + tuple([P()] * len(params)), out_specs=tile_spec, check_vma=False)
        return mapped(image, *params)

    return program
```

```python
import functools

import jax
import jax.numpy as jnp
from jax import lax
from jax.experimental import pallas as pl
from jax.experimental.pallas import tpu as pltpu
from jax.sharding import PartitionSpec as P

MESH = pl.DeviceIdType.MESH
F32 = jnp.float32
BF16 = jnp.bfloat16
ROWS = 18
SIDE = 16
PIX = SIDE * SIDE
EXT = ROWS * SIDE
C1 = 192
C1P = 256
C2 = 384
C3 = 768
HALF = 64
LANE = 128
PATCH = 192
TAPROWS = 40
BY_ROWS = (((1,), (1,)), ((), ()))
POOL1, ENC2A, POOL2, MIDA, UP2, DEC2A, CAT1, DEC1A, IMAGE, SKIP2, SKIP1 = range(11)
EXCHANGE = ((2, C1P), (2, C2), (1, C2), (1, C3), (2, C2), (2, C2), (4, C1P), (4, C1P), (1, LANE), (2, C2), (4, C1P))
MESSAGES = 5
LOADS = 19


def iota(shape, dim):
    return lax.broadcasted_iota(jnp.int32, shape, dim)


def grid_iota(*shape):
    return iota(shape, 0), iota(shape, 1)


def ones_at(mask):
    return mask.astype(F32).astype(BF16)


def dot(lhs, rhs):
    return jnp.dot(lhs, rhs, preferred_element_type=F32)


def dot_rows(lhs, rhs):
    return lax.dot_general(lhs, rhs, BY_ROWS, preferred_element_type=F32)


def biased_relu(acc, bias):
    return jnp.maximum(acc + bias[...].reshape(1, bias.shape[-1]), 0.0).astype(BF16)


def kernel(row_count, x, we1a, we1b, we2a, we2b, wma, wmb, wu2, wd2a, wd2b, wu1, wd1a, wd1b, wh,
           be1a, be1b, be2a, be2b, bma, bmb, bd2a, bd2b, bd1a, bd1b, y, *scratch):
    (vw8, re1b, ve1b, ve2a, ve2b, vma, vmb, vu2, vd2a, vu1, vd1a, vd1b,
     h1, cat1, d1a, p1, e2a, cat2, d2, p2, ma, mid, x1, x8, wf, bpad, weave, part, heads) = scratch[:-2 * len(EXCHANGE) - 3]
    send_cols = scratch[-2 * len(EXCHANGE) - 3:-len(EXCHANGE) - 3]
    recv_cols = scratch[-len(EXCHANGE) - 3:-3]
    w_sem, send_sem, recv_sem = scratch[-3:]
    row, col, data = lax.axis_index("row"), lax.axis_index("col"), lax.axis_index("data")
    last = row_count - 1
    has_up, has_down = row > 0, row < last
    up, down = (data, col, row - 1), (data, col, row + 1)
    side, side_up, side_down = (data, 1 - col, row), (data, 1 - col, row - 1), (data, 1 - col, row + 1)
    edge = (1 - col) * (SIDE - 1)

    loads = [(we1b, re1b), (we2a, ve2a.at[:, :, HALF:, :]), (we2b, ve2b), (wma, vma), (wmb, vmb),
             (wu2, vu2), (wd2a, vd2a), (wu1, vu1)]
    loads += [(wd1a.at[t // 3, t % 3], vd1a.at[:C1, pl.ds(t * C2, C2)]) for t in range(9)]
    loads += [(wd1b, vd1b.at[:, :, :C1, :]), (wd2b, ve2b)]
    copies = [pltpu.make_async_copy(src, dst, w_sem.at[k]) for k, (src, dst) in enumerate(loads)]
    for copy in copies[:3]:
        copy.start()
    for buf, factor in ((h1, 4), (cat1, 4), (d1a, 4), (p1, 2), (e2a, 2), (cat2, 2), (p2, 1), (ma, 1), (x1, 1)):
        blank = jnp.zeros(buf.shape[1:2] + buf.shape[3:], BF16)
        buf[0, :, ROWS - 1] = blank
        buf[factor - 1, :, 0] = blank
    for buf, (factor, _) in zip(recv_cols, EXCHANGE):
        buf[factor:] = jnp.zeros((2,) + buf.shape[1:], BF16)

    barrier = pltpu.get_barrier_semaphore()

    def arrive(device):
        pl.semaphore_signal(barrier, inc=1, device_id=device, device_id_type=MESH)

    arrive(side)

    @pl.when(has_up)
    def _():
        arrive(up)
        arrive(side_up)

    @pl.when(has_down)
    def _():
        arrive(down)
        arrive(side_down)

    for copy in copies[3:-1]:
        copy.start()

    def messages(index, buf, lane):
        factor, width = EXCHANGE[index]
        cols, got = send_cols[index], recv_cols[index]
        own = pl.ds(1, factor)
        lanes = pl.ds(lane, width)

        def remote(k, src, dst, device):
            return pltpu.make_async_remote_copy(
                src_ref=src, dst_ref=dst, send_sem=send_sem.at[index, k], recv_sem=recv_sem.at[index, k],
                device_id=device, device_id_type=MESH)

        routes = (
            (cols, got.at[pl.ds(0, factor)], side),
            (buf.at[0, own, 1, :, lanes], buf.at[0, own, ROWS - 1, :, lanes], up),
            (buf.at[factor - 1, own, ROWS - 2, :, lanes], buf.at[factor - 1, own, 0, :, lanes], down),
            (cols.at[0], got.at[factor + 1], side_up),
            (cols.at[factor - 1], got.at[factor], side_down),
        )
        return [remote(k, *route) for k, route in enumerate(routes)]

    def shift(value, right):
        value = value.astype(F32)
        count = value.shape[0]
        at = lax.rem(iota(value.shape, 0), SIDE)
        if right:
            return jnp.where(at == SIDE - 1, 0.0, pltpu.roll(value, count - 1, 0))
        return jnp.where(at == 0, 0.0, pltpu.roll(value, 1, 0))

    def start(index, buf, lane=0):
        factor, width = EXCHANGE[index]
        lanes = pl.ds(lane, width)
        to_side, to_up, to_down, to_side_up, to_side_down = messages(index, buf, lane)
        if index == IMAGE:
            pl.semaphore_wait(barrier, 2 * has_up.astype(jnp.int32) + 2 * has_down.astype(jnp.int32) + 1)

        @pl.when(has_up)
        def _():
            to_up.start()

        @pl.when(has_down)
        def _():
            to_down.start()

        pick_row, pick_at = grid_iota(SIDE, PIX)
        pick = ones_at(pick_at == pick_row * SIDE + edge)
        cols = send_cols[index]
        for a in range(factor):
            plane = buf[a, 1 + (factor - 1) * (1 - col), 1:ROWS - 1, :, lanes].reshape(PIX, width)
            cols[a] = dot(pick, plane).astype(BF16)
        to_side.start()

        @pl.when(has_up)
        def _():
            to_side_up.start()

        @pl.when(has_down)
        def _():
            to_side_down.start()

        def shifted(a):
            for source, target in ((factor, 0), (1, factor + 1)):
                value = shift(buf[a, source, 1:ROWS - 1, :, lanes].reshape(PIX, width), target > 0)
                buf[a, target, 1:ROWS - 1, :, lanes] = value.astype(BF16).reshape(SIDE, SIDE, width)

        if factor == 1:
            shifted(0)
        else:
            pl.loop(0, factor)(shifted)

    def finish(index, buf, lane=0):
        factor, width = EXCHANGE[index]
        lanes = pl.ds(lane, width)
        got = recv_cols[index]
        to_side, to_up, to_down, to_side_up, to_side_down = messages(index, buf, lane)
        to_side.wait()

        @pl.when(has_up)
        def _():
            to_up.wait_send()
            to_side_up.wait_send()
            to_down.wait_recv()
            to_side_down.wait_recv()

        @pl.when(has_down)
        def _():
            to_down.wait_send()
            to_side_down.wait_send()
            to_up.wait_recv()
            to_side_up.wait_recv()

        at, source = grid_iota(EXT, 3 * SIDE)
        place = ones_at((lax.rem(at, SIDE) == edge) & (at // SIDE + SIDE - 1 == source))
        fix = (factor + 1) * (1 - col)
        for a in range(factor):
            put = dot(place, jnp.concatenate([got[factor], got[a], got[factor + 1]], axis=0))
            plane = buf[a, fix, 1:ROWS - 1, :, lanes].reshape(PIX, width).astype(F32) + put[SIDE:EXT - SIDE]
            buf[a, fix, 1:ROWS - 1, :, lanes] = plane.astype(BF16).reshape(SIDE, SIDE, width)
            ends = ([(0, put[:SIDE])] if a == factor - 1 else []) + ([(ROWS - 1, put[EXT - SIDE:])] if a == 0 else [])
            for line, corner in ends:
                left = shift(buf[a, factor, line, :, lanes], False) + jnp.where(col == 1, corner, 0.0)
                right = shift(buf[a, 1, line, :, lanes], True) + jnp.where(col == 0, corner, 0.0)
                buf[a, 0, line, :, lanes] = left.astype(BF16)
                buf[a, factor + 1, line, :, lanes] = right.astype(BF16)

    ALL = [(dy, dx) for dy in range(3) for dx in range(3)]

    def gather(buf, factor, planes):
        rows = []
        for a, b in planes:
            parts = []
            for dy, dx in ALL:
                shifted = a + (dy - 1 + factor)
                piece = buf[lax.rem(shifted, factor), b + dx, pl.ds(shifted // factor, SIDE)]
                parts.append(piece.reshape(PIX, piece.shape[-1]))
            rows.append(jnp.concatenate(parts, axis=1))
        return jnp.concatenate(rows, axis=0)

    def conv(buf, factor, planes, weight):
        return dot(gather(buf, factor, planes), weight[...].reshape(9 * buf.shape[-1], weight.shape[-1]))

    def put_planes(buf, planes, value, lane=0):
        width = value.shape[-1]
        for k, (a, b) in enumerate(planes):
            plane = value[k * PIX:(k + 1) * PIX].reshape(SIDE, SIDE, width)
            buf[a, b + 1, 1:ROWS - 1, :, lane:lane + width] = plane

    def row_of(a):
        return [(a, b) for b in range(4)]

    def pool(src, dst, factor, lane, width):
        for a in range(factor):
            for b in range(factor):
                quad = [src[2 * a + p, 2 * b + q + 1, 1:ROWS - 1, :, lane:lane + width] for p in range(2) for q in range(2)]
                dst[a, b + 1, 1:ROWS - 1] = functools.reduce(jnp.maximum, quad)

    LEVEL2 = [(a, b) for a in range(2) for b in range(2)]

    def plane_of(buf, a, b, line, lane, width):
        return buf[a, b, pl.ds(line, SIDE), :, pl.ds(lane, width)].reshape(PIX, width)

    def near(a, b, buf, weight, lane, width):
        lhs = [plane_of(buf, k, l + 1, 1, lane, width) for k, l in LEVEL2]
        rhs = [weight[k - a + 1, l - b + 1, lane:lane + width] for k, l in LEVEL2]
        return dot(jnp.concatenate(lhs, axis=1), jnp.concatenate(rhs, axis=0))

    def far(a, b, buf, weight, lane, width):
        lhs = [plane_of(buf, 1 - a, b + dx, 2 * a, lane, width) for dx in range(3)]
        lhs += [plane_of(buf, k, 3 * b, 1, lane, width) for k in range(2)]
        rhs = [weight[2 * a, dx, lane:lane + width] for dx in range(3)]
        rhs += [weight[k - a + 1, 2 * b, lane:lane + width] for k in range(2)]
        return dot(jnp.concatenate(lhs, axis=1), jnp.concatenate(rhs, axis=0))

    def over_level2(terms, put, *operands):
        @pl.loop(0, 2)
        def _(a):
            for b in range(2):
                put(a, b, terms(a, b, *operands))

    def keep(a, b, value):
        part[2 * a + b] = value

    def add(a, b, value):
        part[2 * a + b] += value

    def done(bias, put):
        return lambda a, b, value: put(a, b, biased_relu(part[2 * a + b] + value, bias))

    def conv_level2(index, src, weight, bias, put, first=None, then=None):
        width = src.shape[-1]
        start(index, src)
        if first is not None:
            first()
        over_level2(near, keep, src, weight, 0, width)
        if then is not None:
            then()
        finish(index, src)
        over_level2(far, done(bias, put), src, weight, 0, width)

    at, to = grid_iota(HALF, HALF)
    split_cols = ones_at(at == lax.rem(to, SIDE) * 4 + to // SIDE)
    at, to = grid_iota(PIX, HALF)
    own_col = lax.rem(at, SIDE) == lax.rem(to, SIDE)
    fold_at, fold_to = grid_iota(HALF, LANE)
    image = []
    for ch in range(3):
        cols = dot(x[ch], split_cols).astype(BF16)
        for a in range(4):
            spread = ones_at(to == (at // SIDE) * 4 + a)
            lines = jnp.where(own_col, dot(spread, cols), 0.0).astype(BF16)
            image.append(dot(lines, ones_at(fold_to == fold_at // SIDE + (ch * SIDE + a * 4))))
    x1[0, 1, 1:ROWS - 1] = sum(image[1:], image[0]).astype(BF16).reshape(SIDE, SIDE, LANE)
    start(IMAGE, x1)

    wf[...] = jnp.zeros(wf.shape, F32)
    for t in range(9):
        wf[pl.ds(4 * t, 3), :C1] = we1a[t // 3, t % 3].astype(F32)
    k, m = grid_iota(PATCH, TAPROWS)
    py, px = k // 32, lax.rem(k, 32) // 4
    base = py * 12 + px * 4 + lax.rem(k, 4)

    @pl.loop(0, 4)
    def _(a):
        for b in range(6):
            good = (py >= a) & (py <= a + 2) & (px >= b) & (px <= b + 2)
            place = ones_at(good & (m == base - a * 12 - b * 4))
            vw8[a * 6 + b] = dot(place, wf[...].astype(BF16)).astype(BF16)

    pad = jnp.zeros((1, HALF), F32)
    bpad[0:1, :] = jnp.concatenate([be1a[...].reshape(1, C1), pad], axis=1)
    bpad[1:2, :] = jnp.concatenate([pad, be1b[...].reshape(1, C1)], axis=1)
    bpad[2:3, :] = jnp.concatenate([bd1a[...].reshape(1, C1), pad], axis=1)
    copies[0].wait()

    @pl.loop(0, 3)
    def _(dy):
        for dx in range(3):
            value = jnp.concatenate([jnp.zeros((C1, HALF), F32), re1b[dy, dx].astype(F32)], axis=1)
            ve1b[dy, dx, :C1] = value.astype(BF16)
            ve1b[dy, dx, C1:] = jnp.zeros((HALF, C1P), BF16)

    finish(IMAGE, x1)

    blank = jnp.zeros((SIDE, LANE), BF16)
    lane, k = grid_iota(LANE, PATCH)
    ch, a, b = lane // SIDE, lax.rem(lane, SIDE) // 4, lax.rem(lane, 4)
    patches = []
    for dx in range(3):
        plane = x1[0, dx].reshape(EXT, LANE)
        blocks = (jnp.concatenate([blank, plane[:-SIDE]], axis=0), plane, jnp.concatenate([plane[SIDE:], blank], axis=0))
        for dy, block in enumerate(blocks):
            py, px = a + (4 * dy - 3), b + (4 * dx - 2)
            good = (ch < 3) & (py >= 0) & (py < 6) & (px >= 0) & (px < 8)
            patches.append(dot(block, ones_at(good & (k == py * 32 + px * 4 + ch))))
    x8[...] = sum(patches[1:], patches[0]).astype(BF16)

    pos = iota((EXT, C1P), 0)
    pos_row, pos_col = pos // SIDE, lax.rem(pos, SIDE)
    off_rows = ((pos_row == 0) & (row == 0)) | ((pos_row == ROWS - 1) & (row == last))
    off = {0: off_rows | ((pos_col == 0) & (col == 0)), 5: off_rows | ((pos_col == SIDE - 1) & (col == 1))}

    @pl.loop(0, 4)
    def _(a):
        for b in range(6):
            acc = dot(x8[...], vw8[a * 6 + b])
            out = jnp.where(off.get(b, off_rows), 0.0, jnp.maximum(acc + bpad[0:1, :], 0.0))
            h1[a, b] = out.astype(BF16).reshape(ROWS, SIDE, C1P)

    @pl.loop(0, 2)
    def _(t):
        for a in (2 * t, 2 * t + 1):
            put_planes(cat1, row_of(a), biased_relu(conv(h1, 4, row_of(a), ve1b), bpad.at[1:2]), LANE)

    pool(cat1, p1, 2, LANE, C1P)

    ve2a[:, :, :HALF, :] = jnp.zeros((3, 3, HALF, C2), BF16)

    def fill_constants():
        start(SKIP1, cat1, LANE)
        n, m = grid_iota(2 * PIX, 2 * PIX)
        weave[...] = ones_at(m == lax.rem(n, 4) * LANE + (n // HALF) * SIDE + lax.rem(n, HALF) // 4)
        vd1b[:, :, C1:, :] = jnp.zeros((3, 3, HALF, C1), BF16)
        vd1a[C1:, :] = jnp.zeros((HALF, vd1a.shape[1]), BF16)
        heads[...] = jnp.zeros(heads.shape, F32)

    copies[1].wait()
    conv_level2(POOL1, p1, ve2a, be2a, lambda a, b, value: put_planes(e2a, [(a, b)], value), first=fill_constants)
    copies[2].wait()
    conv_level2(ENC2A, e2a, ve2b, be2b, lambda a, b, value: put_planes(cat2, [(a, b)], value, C2),
                then=lambda: finish(SKIP1, cat1, LANE))
    copies[-1].start()
    pool(cat2, p2, 1, C2, C2)

    start(POOL2, p2)
    start(SKIP2, cat2, C2)
    copies[6].wait()
    over_level2(near, keep, cat2, vd2a, C2, C2)
    copies[3].wait()
    finish(POOL2, p2)
    put_planes(ma, [(0, 0)], biased_relu(conv(p2, 1, [(0, 0)], vma), bma))
    start(MIDA, ma)
    finish(SKIP2, cat2, C2)
    over_level2(far, add, cat2, vd2a, C2, C2)
    copies[4].wait()
    finish(MIDA, ma)
    mid[...] = biased_relu(conv(ma, 1, [(0, 0)], vmb), bmb)
    copies[5].wait()
    for p in range(2):
        out = dot(mid[...], jnp.concatenate([vu2[p, 0], vu2[p, 1]], axis=1)).astype(BF16)
        for q in range(2):
            put_planes(cat2, [(p, q)], out[:, q * C2:(q + 1) * C2])
    start(UP2, cat2)
    over_level2(near, add, cat2, vd2a, 0, C2)
    finish(UP2, cat2)
    over_level2(far, done(bd2a, lambda a, b, value: put_planes(e2a, [(a, b)], value)), cat2, vd2a, 0, C2)
    copies[-1].wait()

    def put_d2(a, b, value):
        d2[pl.ds((2 * a + b) * PIX, PIX)] = value

    conv_level2(DEC2A, e2a, ve2b, bd2b, put_d2)
    copies[7].wait()

    @pl.loop(0, 2)
    def _(t):
        lhs = d2[pl.ds(2 * t * PIX, 2 * PIX)]
        for p, q in LEVEL2:
            put_planes(cat1, [(2 * t + p, q), (2 * t + p, q + 2)], dot_rows(lhs, vu1[p, q]).astype(BF16))

    for copy in copies[8:17]:
        copy.wait()

    border = 3 * col

    def level1(index, src, layer):
        start(index, src)
        for a in (1, 2):
            layer([(a, 1), (a, 2), (a, border)])
        finish(index, src)
        layer([(1, 3 - border), (2, 3 - border)])
        for a in (0, 3):
            layer(row_of(a))

    def dec1a(planes):
        put_planes(d1a, planes, biased_relu(dot_rows(gather(cat1, 4, planes), vd1a[...]), bpad.at[2:3]))

    level1(CAT1, cat1, dec1a)
    copies[17].wait()

    def head(a):
        lines = [h1[a, b + 1, pl.ds(8 * h + 1, 8), :, :C1].reshape(LANE, C1) for h in range(2) for b in range(4)]
        heads[a, :6] = dot_rows(wh[...], jnp.concatenate(lines, axis=0))

    def dec1b(planes):
        put_planes(h1, planes, biased_relu(conv(d1a, 4, planes, vd1b), bd1b))

    level1(DEC1A, d1a, dec1b)
    for a in range(4):
        head(a)
    wide = 2 * PIX
    flat = jnp.concatenate([heads[a, :, h * wide:(h + 1) * wide] for a in range(4) for h in range(2)], axis=0)
    high = flat.astype(BF16)
    rest = flat - high.astype(F32)
    middle = rest.astype(BF16)
    low = (rest - middle.astype(F32)).astype(BF16)
    woven = dot_rows(high, weave[...]) + dot_rows(middle, weave[...]) + dot_rows(low, weave[...])
    for a in range(4):
        for h in range(2):
            for i in range(8):
                y[:, 4 * (8 * h + i) + a, :] = woven[(2 * a + h) * 8:(2 * a + h) * 8 + 6, i * HALF:(i + 1) * HALF]


def solution(mesh):
    tile_spec = P(("data", "row"), "col", None)

    def device_body(image_tile, *params):
        (w_enc1a, b_enc1a, w_enc1b, b_enc1b, w_enc2a, b_enc2a, w_enc2b, b_enc2b,
         w_mid_a, b_mid_a, w_mid_b, b_mid_b, w_up2, w_dec2a, b_dec2a, w_dec2b, b_dec2b,
         w_up1, w_dec1a, b_dec1a, w_dec1b, b_dec1b, w_head, b_head) = params
        anywhere = pl.BlockSpec(memory_space=pl.ANY)
        vmem = pl.BlockSpec(memory_space=pltpu.VMEM)
        operands = [
            jnp.transpose(image_tile, (2, 0, 1)), w_enc1a, w_enc1b, w_enc2a, w_enc2b, w_mid_a, w_mid_b,
            w_up2, w_dec2a, w_dec2b, jnp.swapaxes(w_up1, 2, 3), jnp.swapaxes(w_dec1a, 2, 3), w_dec1b, w_head.T,
            b_enc1a, b_enc1b, b_enc2a, b_enc2b, b_mid_a, b_mid_b, b_dec2a, b_dec2b, b_dec1a, b_dec1b,
        ]
        specs = [vmem] * 2 + [anywhere] * 11 + [vmem] * 11

        def kept(*shape, dtype=BF16):
            return pltpu.VMEM(shape, dtype)

        def level(factor, lanes):
            return kept(factor, factor + 2, ROWS, SIDE, lanes)

        scratch = [
            kept(24, PATCH, C1P), kept(3, 3, C1, C1), kept(3, 3, C1P, C1P), kept(3, 3, C1P, C2), kept(3, 3, C2, C2),
            kept(3, 3, C2, C3), kept(3, 3, C3, C3), kept(2, 2, C3, C2), kept(3, 3, C3, C2),
            kept(2, 2, C1, C2), kept(C1P, 9 * C2), kept(3, 3, C1P, C1),
            level(4, C1P), level(4, C2), level(4, C1P), level(2, C1P), level(2, C2), level(2, C3),
            kept(4 * PIX, C2), level(1, C2), level(1, C3), kept(PIX, C3), level(1, LANE), kept(EXT, PATCH),
            kept(TAPROWS, C1P, dtype=F32), kept(3, C1P, dtype=F32), kept(2 * PIX, 2 * PIX),
            kept(4, PIX, C2, dtype=F32), kept(4, 8, 4 * PIX, dtype=F32),
        ]
        scratch += [kept(factor, SIDE, width) for factor, width in EXCHANGE]
        scratch += [kept(factor + 2, SIDE, width) for factor, width in EXCHANGE]
        links = pltpu.SemaphoreType.DMA((len(EXCHANGE), MESSAGES))
        scratch += [pltpu.SemaphoreType.DMA((LOADS,)), links, links]
        out = pl.pallas_call(
            functools.partial(kernel, mesh.shape["row"]),
            name="unet",
            out_shape=jax.ShapeDtypeStruct((6, HALF, HALF), F32),
            in_specs=specs,
            out_specs=vmem,
            scratch_shapes=scratch,
            compiler_params=pltpu.CompilerParams(collective_id=0, has_side_effects=True, vmem_limit_bytes=67043328),
        )(*operands)
        return jnp.transpose(out, (1, 2, 0)) + b_head

    def program(image, *params):
        mapped = jax.shard_map(device_body, mesh=mesh, in_specs=(tile_spec,) + tuple([P()] * len(params)), out_specs=tile_spec, check_vma=False)
        return mapped(image, *params)

    return program
```

```python
import functools

import jax
import jax.numpy as jnp
from jax import lax
from jax.experimental import pallas as pl
from jax.experimental.pallas import tpu as pltpu
from jax.sharding import PartitionSpec as P

MESH = pl.DeviceIdType.MESH
F32 = jnp.float32
BF16 = jnp.bfloat16
ROWS = 18
SIDE = 16
PIX = SIDE * SIDE
EXT = ROWS * SIDE
C1 = 192
C1P = 256
C2 = 384
C3 = 768
HALF = 64
LANE = 128
PATCH = 192
TAPROWS = 40
BY_ROWS = (((1,), (1,)), ((), ()))
POOL1, ENC2A, POOL2, MIDA, UP2, DEC2A, CAT1, DEC1A, IMAGE, SKIP2, SKIP1 = range(11)
EXCHANGE = ((2, C1P), (2, C2), (1, C2), (1, C3), (2, C2), (2, C2), (4, C1P), (4, C1P), (1, LANE), (2, C2), (4, C1P))
MESSAGES = 5
LOADS = 19


def iota(shape, dim):
    return lax.broadcasted_iota(jnp.int32, shape, dim)


def grid_iota(*shape):
    return iota(shape, 0), iota(shape, 1)


def ones_at(mask):
    return mask.astype(F32).astype(BF16)


def dot(lhs, rhs):
    return jnp.dot(lhs, rhs, preferred_element_type=F32)


def dot_rows(lhs, rhs):
    return lax.dot_general(lhs, rhs, BY_ROWS, preferred_element_type=F32)


def biased_relu(acc, bias):
    return jnp.maximum(acc + bias[...].reshape(1, bias.shape[-1]), 0.0).astype(BF16)


def kernel(row_count, x, we1a, we1b, we2a, we2b, wma, wmb, wu2, wd2a, wd2b, wu1, wd1a, wd1b, wh,
           be1a, be1b, be2a, be2b, bma, bmb, bd2a, bd2b, bd1a, bd1b, y, *scratch):
    (vw8, re1b, ve1b, ve2a, ve2b, vma, vmb, vu2, vd2a, vu1, vd1a, vd1b,
     h1, cat1, d1a, p1, e2a, cat2, d2, p2, ma, mid, x1, x8, wf, bpad, weave, part, heads) = scratch[:-2 * len(EXCHANGE) - 3]
    send_cols = scratch[-2 * len(EXCHANGE) - 3:-len(EXCHANGE) - 3]
    recv_cols = scratch[-len(EXCHANGE) - 3:-3]
    w_sem, send_sem, recv_sem = scratch[-3:]
    row, col, data = lax.axis_index("row"), lax.axis_index("col"), lax.axis_index("data")
    last = row_count - 1
    has_up, has_down = row > 0, row < last
    up, down = (data, col, row - 1), (data, col, row + 1)
    side, side_up, side_down = (data, 1 - col, row), (data, 1 - col, row - 1), (data, 1 - col, row + 1)
    edge = (1 - col) * (SIDE - 1)

    barrier = pltpu.get_barrier_semaphore()

    def arrive(device):
        pl.semaphore_signal(barrier, inc=1, device_id=device, device_id_type=MESH)

    arrive(side)

    @pl.when(has_up)
    def _():
        arrive(up)
        arrive(side_up)

    @pl.when(has_down)
    def _():
        arrive(down)
        arrive(side_down)

    loads = [(we1b, re1b), (we2a, ve2a.at[:, :, HALF:, :]), (we2b, ve2b), (wma, vma), (wmb, vmb),
             (wu2, vu2), (wd2a, vd2a), (wu1, vu1)]
    loads += [(wd1a.at[t // 3, t % 3], vd1a.at[:C1, pl.ds(t * C2, C2)]) for t in range(9)]
    loads += [(wd1b, vd1b.at[:, :, :C1, :]), (wd2b, ve2b)]
    copies = [pltpu.make_async_copy(src, dst, w_sem.at[k]) for k, (src, dst) in enumerate(loads)]
    for copy in copies[:3]:
        copy.start()
    for copy in copies[3:-1]:
        copy.start()

    def messages(index, buf, lane):
        factor, width = EXCHANGE[index]
        cols, got = send_cols[index], recv_cols[index]
        own = pl.ds(1, factor)
        lanes = pl.ds(lane, width)

        def remote(k, src, dst, device):
            return pltpu.make_async_remote_copy(
                src_ref=src, dst_ref=dst, send_sem=send_sem.at[index, k], recv_sem=recv_sem.at[index, k],
                device_id=device, device_id_type=MESH)

        routes = (
            (cols, got.at[pl.ds(0, factor)], side),
            (buf.at[0, own, 1, :, lanes], buf.at[0, own, ROWS - 1, :, lanes], up),
            (buf.at[factor - 1, own, ROWS - 2, :, lanes], buf.at[factor - 1, own, 0, :, lanes], down),
            (cols.at[0], got.at[factor + 1], side_up),
            (cols.at[factor - 1], got.at[factor], side_down),
        )
        return [remote(k, *route) for k, route in enumerate(routes)]

    def shift(value, right):
        value = value.astype(F32)
        count = value.shape[0]
        at = lax.rem(iota(value.shape, 0), SIDE)
        if right:
            return jnp.where(at == SIDE - 1, 0.0, pltpu.roll(value, count - 1, 0))
        return jnp.where(at == 0, 0.0, pltpu.roll(value, 1, 0))

    def start(index, buf, lane=0):
        factor, width = EXCHANGE[index]
        lanes = pl.ds(lane, width)
        to_side, to_up, to_down, to_side_up, to_side_down = messages(index, buf, lane)
        if index == IMAGE:
            pl.semaphore_wait(barrier, 2 * has_up.astype(jnp.int32) + 2 * has_down.astype(jnp.int32) + 1)

        @pl.when(has_up)
        def _():
            to_up.start()

        @pl.when(has_down)
        def _():
            to_down.start()

        pick_row, pick_at = grid_iota(SIDE, PIX)
        pick = ones_at(pick_at == pick_row * SIDE + edge)
        cols = send_cols[index]
        for a in range(factor):
            plane = buf[a, 1 + (factor - 1) * (1 - col), 1:ROWS - 1, :, lanes].reshape(PIX, width)
            cols[a] = dot(pick, plane).astype(BF16)
        to_side.start()

        @pl.when(has_up)
        def _():
            to_side_up.start()

        @pl.when(has_down)
        def _():
            to_side_down.start()

        def shifted(a):
            for source, target in ((factor, 0), (1, factor + 1)):
                value = shift(buf[a, source, 1:ROWS - 1, :, lanes].reshape(PIX, width), target > 0)
                buf[a, target, 1:ROWS - 1, :, lanes] = value.astype(BF16).reshape(SIDE, SIDE, width)

        if factor == 1:
            shifted(0)
        else:
            pl.loop(0, factor)(shifted)

    def finish(index, buf, lane=0):
        factor, width = EXCHANGE[index]
        lanes = pl.ds(lane, width)
        got = recv_cols[index]
        to_side, to_up, to_down, to_side_up, to_side_down = messages(index, buf, lane)
        to_side.wait()

        @pl.when(has_up)
        def _():
            to_up.wait_send()
            to_side_up.wait_send()
            to_down.wait_recv()
            to_side_down.wait_recv()

        @pl.when(has_down)
        def _():
            to_down.wait_send()
            to_side_down.wait_send()
            to_up.wait_recv()
            to_side_up.wait_recv()

        at, source = grid_iota(EXT, 3 * SIDE)
        place = ones_at((lax.rem(at, SIDE) == edge) & (at // SIDE + SIDE - 1 == source))
        fix = (factor + 1) * (1 - col)
        for a in range(factor):
            put = dot(place, jnp.concatenate([got[factor], got[a], got[factor + 1]], axis=0))
            plane = buf[a, fix, 1:ROWS - 1, :, lanes].reshape(PIX, width).astype(F32) + put[SIDE:EXT - SIDE]
            buf[a, fix, 1:ROWS - 1, :, lanes] = plane.astype(BF16).reshape(SIDE, SIDE, width)
            ends = ([(0, put[:SIDE])] if a == factor - 1 else []) + ([(ROWS - 1, put[EXT - SIDE:])] if a == 0 else [])
            for line, corner in ends:
                left = shift(buf[a, factor, line, :, lanes], False) + jnp.where(col == 1, corner, 0.0)
                right = shift(buf[a, 1, line, :, lanes], True) + jnp.where(col == 0, corner, 0.0)
                buf[a, 0, line, :, lanes] = left.astype(BF16)
                buf[a, factor + 1, line, :, lanes] = right.astype(BF16)

    ALL = [(dy, dx) for dy in range(3) for dx in range(3)]

    def gather(buf, factor, planes):
        rows = []
        for a, b in planes:
            parts = []
            for dy, dx in ALL:
                shifted = a + (dy - 1 + factor)
                piece = buf[lax.rem(shifted, factor), b + dx, pl.ds(shifted // factor, SIDE)]
                parts.append(piece.reshape(PIX, piece.shape[-1]))
            rows.append(jnp.concatenate(parts, axis=1))
        return jnp.concatenate(rows, axis=0)

    def conv(buf, factor, planes, weight):
        return dot(gather(buf, factor, planes), weight[...].reshape(9 * buf.shape[-1], weight.shape[-1]))

    def put_planes(buf, planes, value, lane=0):
        width = value.shape[-1]
        for k, (a, b) in enumerate(planes):
            plane = value[k * PIX:(k + 1) * PIX].reshape(SIDE, SIDE, width)
            buf[a, b + 1, 1:ROWS - 1, :, lane:lane + width] = plane

    def row_of(a):
        return [(a, b) for b in range(4)]

    def pool(src, dst, factor, lane, width):
        for a in range(factor):
            for b in range(factor):
                quad = [src[2 * a + p, 2 * b + q + 1, 1:ROWS - 1, :, lane:lane + width] for p in range(2) for q in range(2)]
                dst[a, b + 1, 1:ROWS - 1] = functools.reduce(jnp.maximum, quad)

    LEVEL2 = [(a, b) for a in range(2) for b in range(2)]

    def plane_of(buf, a, b, line, lane, width):
        return buf[a, b, pl.ds(line, SIDE), :, pl.ds(lane, width)].reshape(PIX, width)

    def near(a, buf, weight, lane, width):
        lhs = [plane_of(buf, k, l + 1, 1, lane, width) for k, l in LEVEL2]
        both = [jnp.concatenate([weight[k - a + 1, l - b + 1, lane:lane + width] for k, l in LEVEL2], axis=0) for b in range(2)]
        out = dot(jnp.concatenate(lhs, axis=1), jnp.concatenate(both, axis=1))
        return out[:, :C2], out[:, C2:]

    def far(a, buf, weight, lane, width):
        outs = []
        for b in range(2):
            lhs = [plane_of(buf, 1 - a, b + dx, 2 * a, lane, width) for dx in range(3)]
            lhs += [plane_of(buf, k, 3 * b, 1, lane, width) for k in range(2)]
            rhs = [weight[2 * a, dx, lane:lane + width] for dx in range(3)]
            rhs += [weight[k - a + 1, 2 * b, lane:lane + width] for k in range(2)]
            outs.append(dot(jnp.concatenate(lhs, axis=1), jnp.concatenate(rhs, axis=0)))
        return outs

    def over_level2(terms, put, *operands):
        @pl.loop(0, 2)
        def _(a):
            for b, value in enumerate(terms(a, *operands)):
                put(a, b, value)

    def keep(a, b, value):
        part[2 * a + b] = value

    def add(a, b, value):
        part[2 * a + b] += value

    def done(bias, put):
        return lambda a, b, value: put(a, b, biased_relu(part[2 * a + b] + value, bias))

    def conv_level2(index, src, weight, bias, put, first=None, then=None):
        width = src.shape[-1]
        start(index, src)
        if first is not None:
            first()
        over_level2(near, keep, src, weight, 0, width)
        if then is not None:
            then()
        finish(index, src)
        over_level2(far, done(bias, put), src, weight, 0, width)

    at, to = grid_iota(HALF, HALF)
    split_cols = ones_at(at == lax.rem(to, SIDE) * 4 + to // SIDE)
    at, to = grid_iota(PIX, HALF)
    own_col = lax.rem(at, SIDE) == lax.rem(to, SIDE)
    fold_at, fold_to = grid_iota(HALF, LANE)
    image = []
    for ch in range(3):
        cols = dot(x[ch], split_cols).astype(BF16)
        for a in range(4):
            spread = ones_at(to == (at // SIDE) * 4 + a)
            lines = jnp.where(own_col, dot(spread, cols), 0.0).astype(BF16)
            image.append(dot(lines, ones_at(fold_to == fold_at // SIDE + (ch * SIDE + a * 4))))
    x1[0, 1, 1:ROWS - 1] = sum(image[1:], image[0]).astype(BF16).reshape(SIDE, SIDE, LANE)
    start(IMAGE, x1)

    mapped = ((cat1, 4), (d1a, 4), (p1, 2), (e2a, 2), (cat2, 2), (p2, 1), (ma, 1), (x1, 1))

    @pl.when(row == 0)
    def _():
        for buf, factor in mapped:
            buf[factor - 1, :, 0] = jnp.zeros(buf.shape[1:2] + buf.shape[3:], BF16)
        for buf, (factor, _) in zip(recv_cols, EXCHANGE):
            buf[factor] = jnp.zeros(buf.shape[1:], BF16)

    @pl.when(row == last)
    def _():
        for buf, factor in mapped:
            buf[0, :, ROWS - 1] = jnp.zeros(buf.shape[1:2] + buf.shape[3:], BF16)
        for buf, (factor, _) in zip(recv_cols, EXCHANGE):
            buf[factor + 1] = jnp.zeros(buf.shape[1:], BF16)


    wf[...] = jnp.zeros(wf.shape, F32)
    for t in range(9):
        wf[pl.ds(4 * t, 3), :C1] = we1a[t // 3, t % 3].astype(F32)
    k, m = grid_iota(PATCH, TAPROWS)
    py, px = k // 32, lax.rem(k, 32) // 4
    base = py * 12 + px * 4 + lax.rem(k, 4)

    @pl.loop(0, 4)
    def _(a):
        for b in range(6):
            good = (py >= a) & (py <= a + 2) & (px >= b) & (px <= b + 2)
            place = ones_at(good & (m == base - a * 12 - b * 4))
            vw8[a * 6 + b] = dot(place, wf[...].astype(BF16)).astype(BF16)

    pad = jnp.zeros((1, HALF), F32)
    bpad[0:1, :C1P] = jnp.concatenate([be1a[...].reshape(1, C1), pad], axis=1)
    bpad[1:2, :C1P] = jnp.concatenate([pad, be1b[...].reshape(1, C1)], axis=1)
    bpad[2:3, :C1P] = jnp.concatenate([bd1a[...].reshape(1, C1), pad], axis=1)
    bpad[3:4, :] = bma[...].reshape(1, C3)
    bpad[4:5, :] = bmb[...].reshape(1, C3)
    copies[0].wait()

    @pl.loop(0, 3)
    def _(dy):
        for dx in range(3):
            value = jnp.concatenate([jnp.zeros((C1, HALF), F32), re1b[dy, dx].astype(F32)], axis=1)
            ve1b[dy, dx, :C1] = value.astype(BF16)
            ve1b[dy, dx, C1:] = jnp.zeros((HALF, C1P), BF16)

    finish(IMAGE, x1)

    blank = jnp.zeros((SIDE, LANE), BF16)
    lane, k = grid_iota(LANE, PATCH)
    ch, a, b = lane // SIDE, lax.rem(lane, SIDE) // 4, lax.rem(lane, 4)
    patches = []
    for dx in range(3):
        plane = x1[0, dx].reshape(EXT, LANE)
        blocks = (jnp.concatenate([blank, plane[:-SIDE]], axis=0), plane, jnp.concatenate([plane[SIDE:], blank], axis=0))
        for dy, block in enumerate(blocks):
            py, px = a + (4 * dy - 3), b + (4 * dx - 2)
            good = (ch < 3) & (py >= 0) & (py < 6) & (px >= 0) & (px < 8)
            patches.append(dot(block, ones_at(good & (k == py * 32 + px * 4 + ch))))
    x8[...] = sum(patches[1:], patches[0]).astype(BF16)

    pos = iota((EXT, C1P), 0)
    pos_col = lax.rem(pos, SIDE)
    off = {0: (pos_col == 0) & (col == 0), 5: (pos_col == SIDE - 1) & (col == 1)}

    @pl.loop(0, 4)
    def _(a):
        for b in range(6):
            out = jnp.maximum(dot(x8[...], vw8[a * 6 + b]) + bpad[0:1, :C1P], 0.0)
            if b in off:
                out = jnp.where(off[b], 0.0, out)
            h1[a, b] = out.astype(BF16).reshape(ROWS, SIDE, C1P)

    @pl.when(row == 0)
    def _():
        h1[3, :, 0] = jnp.zeros((6, SIDE, C1P), BF16)

    @pl.when(row == last)
    def _():
        h1[0, :, ROWS - 1] = jnp.zeros((6, SIDE, C1P), BF16)

    @pl.loop(0, 2)
    def _(t):
        for a in (2 * t, 2 * t + 1):
            put_planes(cat1, row_of(a), biased_relu(conv(h1, 4, row_of(a), ve1b), bpad.at[1:2, :C1P]), LANE)

    pool(cat1, p1, 2, LANE, C1P)

    ve2a[:, :, :HALF, :] = jnp.zeros((3, 3, HALF, C2), BF16)

    def fill_constants():
        start(SKIP1, cat1, LANE)
        n, m = grid_iota(2 * PIX, 2 * PIX)
        weave[...] = ones_at(m == lax.rem(n, 4) * LANE + (n // HALF) * SIDE + lax.rem(n, HALF) // 4)
        vd1b[:, :, C1:, :] = jnp.zeros((3, 3, HALF, C1), BF16)
        vd1a[C1:, :] = jnp.zeros((HALF, vd1a.shape[1]), BF16)
        heads[...] = jnp.zeros(heads.shape, F32)

    copies[1].wait()
    conv_level2(POOL1, p1, ve2a, be2a, lambda a, b, value: put_planes(e2a, [(a, b)], value), first=fill_constants)
    copies[2].wait()
    conv_level2(ENC2A, e2a, ve2b, be2b, lambda a, b, value: put_planes(cat2, [(a, b)], value, C2),
                then=lambda: finish(SKIP1, cat1, LANE))
    copies[-1].start()
    pool(cat2, p2, 1, C2, C2)

    start(POOL2, p2)
    start(SKIP2, cat2, C2)
    copies[6].wait()
    over_level2(near, keep, cat2, vd2a, C2, C2)
    copies[3].wait()
    finish(POOL2, p2)

    def conv_level3(src, weight, bias, put):
        @pl.loop(0, 3)
        def _(n):
            lanes = pl.ds(pl.multiple_of(n * PIX, PIX), PIX)
            flat = weight[:, :, :, lanes].reshape(9 * src.shape[-1], PIX)
            put(lanes, biased_relu(dot(gather(src, 1, [(0, 0)]), flat), bpad.at[bias:bias + 1, lanes]))

    def put_ma(lanes, value):
        ma[0, 1, 1:ROWS - 1, :, lanes] = value.reshape(SIDE, SIDE, PIX)

    def put_mid(lanes, value):
        mid[:, lanes] = value

    conv_level3(p2, vma, 3, put_ma)
    start(MIDA, ma)
    finish(SKIP2, cat2, C2)
    over_level2(far, add, cat2, vd2a, C2, C2)
    copies[4].wait()
    finish(MIDA, ma)
    conv_level3(ma, vmb, 4, put_mid)
    copies[5].wait()
    for p in range(2):
        out = dot(mid[...], jnp.concatenate([vu2[p, 0], vu2[p, 1]], axis=1)).astype(BF16)
        for q in range(2):
            put_planes(cat2, [(p, q)], out[:, q * C2:(q + 1) * C2])
    start(UP2, cat2)
    over_level2(near, add, cat2, vd2a, 0, C2)
    finish(UP2, cat2)
    over_level2(far, done(bd2a, lambda a, b, value: put_planes(e2a, [(a, b)], value)), cat2, vd2a, 0, C2)
    copies[-1].wait()

    def put_d2(a, b, value):
        d2[pl.ds((2 * a + b) * PIX, PIX)] = value

    conv_level2(DEC2A, e2a, ve2b, bd2b, put_d2)
    copies[7].wait()

    @pl.loop(0, 2)
    def _(t):
        lhs = d2[pl.ds(2 * t * PIX, 2 * PIX)]
        for p, q in LEVEL2:
            put_planes(cat1, [(2 * t + p, q), (2 * t + p, q + 2)], dot_rows(lhs, vu1[p, q]).astype(BF16))

    for copy in copies[8:17]:
        copy.wait()

    border = 3 * col

    def level1(index, src, layer):
        start(index, src)
        for a in (1, 2):
            layer([(a, 1), (a, 2), (a, border)])
        finish(index, src)
        layer([(1, 3 - border), (2, 3 - border)])
        for a in (0, 3):
            layer(row_of(a))

    def dec1a(planes):
        put_planes(d1a, planes, biased_relu(dot_rows(gather(cat1, 4, planes), vd1a[...]), bpad.at[2:3, :C1P]))

    level1(CAT1, cat1, dec1a)
    copies[17].wait()

    def head(a):
        lines = [h1[a, b + 1, pl.ds(8 * h + 1, 8), :, :C1].reshape(LANE, C1) for h in range(2) for b in range(4)]
        heads[a, :6] = dot_rows(wh[...], jnp.concatenate(lines, axis=0))

    def dec1b(planes):
        put_planes(h1, planes, biased_relu(conv(d1a, 4, planes, vd1b), bd1b))

    level1(DEC1A, d1a, dec1b)
    for a in range(4):
        head(a)
    wide = 2 * PIX
    flat = jnp.concatenate([heads[a, :, h * wide:(h + 1) * wide] for a in range(4) for h in range(2)], axis=0)
    high = flat.astype(BF16)
    rest = flat - high.astype(F32)
    middle = rest.astype(BF16)
    low = (rest - middle.astype(F32)).astype(BF16)
    woven = dot_rows(high, weave[...]) + dot_rows(middle, weave[...]) + dot_rows(low, weave[...])
    for a in range(4):
        for h in range(2):
            for i in range(8):
                y[:, 4 * (8 * h + i) + a, :] = woven[(2 * a + h) * 8:(2 * a + h) * 8 + 6, i * HALF:(i + 1) * HALF]


def solution(mesh):
    tile_spec = P(("data", "row"), "col", None)

    def device_body(image_tile, *params):
        (w_enc1a, b_enc1a, w_enc1b, b_enc1b, w_enc2a, b_enc2a, w_enc2b, b_enc2b,
         w_mid_a, b_mid_a, w_mid_b, b_mid_b, w_up2, w_dec2a, b_dec2a, w_dec2b, b_dec2b,
         w_up1, w_dec1a, b_dec1a, w_dec1b, b_dec1b, w_head, b_head) = params
        anywhere = pl.BlockSpec(memory_space=pl.ANY)
        vmem = pl.BlockSpec(memory_space=pltpu.VMEM)
        operands = [
            jnp.transpose(image_tile, (2, 0, 1)), w_enc1a, w_enc1b, w_enc2a, w_enc2b, w_mid_a, w_mid_b,
            w_up2, w_dec2a, w_dec2b, jnp.swapaxes(w_up1, 2, 3), jnp.swapaxes(w_dec1a, 2, 3), w_dec1b, w_head.T,
            b_enc1a, b_enc1b, b_enc2a, b_enc2b, b_mid_a, b_mid_b, b_dec2a, b_dec2b, b_dec1a, b_dec1b,
        ]
        specs = [vmem] * 2 + [anywhere] * 11 + [vmem] * 11

        def kept(*shape, dtype=BF16):
            return pltpu.VMEM(shape, dtype)

        def level(factor, lanes):
            return kept(factor, factor + 2, ROWS, SIDE, lanes)

        scratch = [
            kept(24, PATCH, C1P), kept(3, 3, C1, C1), kept(3, 3, C1P, C1P), kept(3, 3, C1P, C2), kept(3, 3, C2, C2),
            kept(3, 3, C2, C3), kept(3, 3, C3, C3), kept(2, 2, C3, C2), kept(3, 3, C3, C2),
            kept(2, 2, C1, C2), kept(C1P, 9 * C2), kept(3, 3, C1P, C1),
            level(4, C1P), level(4, C2), level(4, C1P), level(2, C1P), level(2, C2), level(2, C3),
            kept(4 * PIX, C2), level(1, C2), level(1, C3), kept(PIX, C3), level(1, LANE), kept(EXT, PATCH),
            kept(TAPROWS, C1P, dtype=F32), kept(5, C3, dtype=F32), kept(2 * PIX, 2 * PIX),
            kept(4, PIX, C2, dtype=F32), kept(4, 8, 4 * PIX, dtype=F32),
        ]
        scratch += [kept(factor, SIDE, width) for factor, width in EXCHANGE]
        scratch += [kept(factor + 2, SIDE, width) for factor, width in EXCHANGE]
        links = pltpu.SemaphoreType.DMA((len(EXCHANGE), MESSAGES))
        scratch += [pltpu.SemaphoreType.DMA((LOADS,)), links, links]
        out = pl.pallas_call(
            functools.partial(kernel, mesh.shape["row"]),
            name="unet",
            out_shape=jax.ShapeDtypeStruct((6, HALF, HALF), F32),
            in_specs=specs,
            out_specs=vmem,
            scratch_shapes=scratch,
            compiler_params=pltpu.CompilerParams(collective_id=0, has_side_effects=True, vmem_limit_bytes=67043328),
        )(*operands)
        return jnp.transpose(out, (1, 2, 0)) + b_head

    def program(image, *params):
        mapped = jax.shard_map(device_body, mesh=mesh, in_specs=(tile_spec,) + tuple([P()] * len(params)), out_specs=tile_spec, check_vma=False)
        return mapped(image, *params)

    return program
```

```python
import functools

import jax
import jax.numpy as jnp
from jax import lax
from jax.experimental import pallas as pl
from jax.experimental.pallas import tpu as pltpu
from jax.sharding import PartitionSpec as P

MESH = pl.DeviceIdType.MESH
F32 = jnp.float32
BF16 = jnp.bfloat16
ROWS = 18
SIDE = 16
PIX = SIDE * SIDE
EXT = ROWS * SIDE
C1 = 192
C1P = 256
C2 = 384
C3 = 768
HALF = 64
LANE = 128
PATCH = 192
TAPROWS = 40
BY_ROWS = (((1,), (1,)), ((), ()))
POOL1, ENC2A, POOL2, MIDA, UP2, DEC2A, CAT1, DEC1A, IMAGE, SKIP2, SKIP1 = range(11)
EXCHANGE = ((2, C1P), (2, C2), (1, C2), (1, C3), (2, C2), (2, C2), (4, C1P), (4, C1P), (1, LANE), (2, C2), (4, C1P))
MESSAGES = 5
LOADS = 19
SMALL = 13


def iota(shape, dim):
    return lax.broadcasted_iota(jnp.int32, shape, dim)


def grid_iota(*shape):
    return iota(shape, 0), iota(shape, 1)


def ones_at(mask):
    return mask.astype(F32).astype(BF16)


def dot(lhs, rhs):
    return jnp.dot(lhs, rhs, preferred_element_type=F32)


def dot_rows(lhs, rhs):
    return lax.dot_general(lhs, rhs, BY_ROWS, preferred_element_type=F32)


def biased_relu(acc, bias):
    return jnp.maximum(acc + bias[...].reshape(1, bias.shape[-1]), 0.0).astype(BF16)


def kernel(row_count, we1b, we2a, we2b, wma, wmb, wu2, wd2a, wd2b, wu1, wd1a, wd1b, *scratch):
    small, y, scratch = scratch[:SMALL], scratch[SMALL], scratch[SMALL + 1:]
    near_small, scratch = scratch[:SMALL], scratch[SMALL:]
    x, we1a, wh, be1a, be1b, be2a, be2b, bma, bmb, bd2a, bd2b, bd1a, bd1b = near_small
    small_sem, scratch = scratch[-1], scratch[:-1]
    small_copies = [pltpu.make_async_copy(src, dst, small_sem.at[k]) for k, (src, dst) in enumerate(zip(small, near_small))]
    for copy in small_copies:
        copy.start()
    (vw8, re1b, ve1b, ve2a, ve2b, vma, vmb, vu2, vd2a, vu1, vd1a, vd1b,
     h1, cat1, d1a, p1, e2a, cat2, d2, p2, ma, mid, x1, x8, wf, bpad, weave, part, heads) = scratch[:-2 * len(EXCHANGE) - 3]
    send_cols = scratch[-2 * len(EXCHANGE) - 3:-len(EXCHANGE) - 3]
    recv_cols = scratch[-len(EXCHANGE) - 3:-3]
    w_sem, send_sem, recv_sem = scratch[-3:]
    row, col, data = lax.axis_index("row"), lax.axis_index("col"), lax.axis_index("data")
    last = row_count - 1
    has_up, has_down = row > 0, row < last
    up, down = (data, col, row - 1), (data, col, row + 1)
    side, side_up, side_down = (data, 1 - col, row), (data, 1 - col, row - 1), (data, 1 - col, row + 1)
    edge = (1 - col) * (SIDE - 1)

    barrier = pltpu.get_barrier_semaphore()

    def arrive(device):
        pl.semaphore_signal(barrier, inc=1, device_id=device, device_id_type=MESH)

    arrive(side)

    @pl.when(has_up)
    def _():
        arrive(up)
        arrive(side_up)

    @pl.when(has_down)
    def _():
        arrive(down)
        arrive(side_down)

    loads = [(we1b, re1b), (we2a, ve2a.at[:, :, HALF:, :]), (we2b, ve2b), (wma, vma), (wmb, vmb),
             (wu2, vu2), (wd2a, vd2a), (wu1, vu1)]
    loads += [(wd1a.at[t // 3, t % 3], vd1a.at[:C1, pl.ds(t * C2, C2)]) for t in range(9)]
    loads += [(wd1b, vd1b.at[:, :, :C1, :]), (wd2b, ve2b)]
    copies = [pltpu.make_async_copy(src, dst, w_sem.at[k]) for k, (src, dst) in enumerate(loads)]
    for copy in copies[:3]:
        copy.start()
    for copy in copies[3:-1]:
        copy.start()

    def messages(index, buf, lane):
        factor, width = EXCHANGE[index]
        cols, got = send_cols[index], recv_cols[index]
        own = pl.ds(1, factor)
        lanes = pl.ds(lane, width)

        def remote(k, src, dst, device):
            return pltpu.make_async_remote_copy(
                src_ref=src, dst_ref=dst, send_sem=send_sem.at[index, k], recv_sem=recv_sem.at[index, k],
                device_id=device, device_id_type=MESH)

        routes = (
            (cols, got.at[pl.ds(0, factor)], side),
            (buf.at[0, own, 1, :, lanes], buf.at[0, own, ROWS - 1, :, lanes], up),
            (buf.at[factor - 1, own, ROWS - 2, :, lanes], buf.at[factor - 1, own, 0, :, lanes], down),
            (cols.at[0], got.at[factor + 1], side_up),
            (cols.at[factor - 1], got.at[factor], side_down),
        )
        return [remote(k, *route) for k, route in enumerate(routes)]

    def shift(value, right):
        value = value.astype(F32)
        count = value.shape[0]
        at = lax.rem(iota(value.shape, 0), SIDE)
        if right:
            return jnp.where(at == SIDE - 1, 0.0, pltpu.roll(value, count - 1, 0))
        return jnp.where(at == 0, 0.0, pltpu.roll(value, 1, 0))

    def start(index, buf, lane=0):
        factor, width = EXCHANGE[index]
        lanes = pl.ds(lane, width)
        to_side, to_up, to_down, to_side_up, to_side_down = messages(index, buf, lane)
        if index == IMAGE:
            pl.semaphore_wait(barrier, 2 * has_up.astype(jnp.int32) + 2 * has_down.astype(jnp.int32) + 1)

        @pl.when(has_up)
        def _():
            to_up.start()

        @pl.when(has_down)
        def _():
            to_down.start()

        pick_row, pick_at = grid_iota(SIDE, PIX)
        pick = ones_at(pick_at == pick_row * SIDE + edge)
        cols = send_cols[index]
        for a in range(factor):
            plane = buf[a, 1 + (factor - 1) * (1 - col), 1:ROWS - 1, :, lanes].reshape(PIX, width)
            cols[a] = dot(pick, plane).astype(BF16)
        to_side.start()

        @pl.when(has_up)
        def _():
            to_side_up.start()

        @pl.when(has_down)
        def _():
            to_side_down.start()

        def shifted(a):
            for source, target in ((factor, 0), (1, factor + 1)):
                value = shift(buf[a, source, 1:ROWS - 1, :, lanes].reshape(PIX, width), target > 0)
                buf[a, target, 1:ROWS - 1, :, lanes] = value.astype(BF16).reshape(SIDE, SIDE, width)

        if factor == 1:
            shifted(0)
        else:
            pl.loop(0, factor)(shifted)

    def finish(index, buf, lane=0):
        factor, width = EXCHANGE[index]
        lanes = pl.ds(lane, width)
        got = recv_cols[index]
        to_side, to_up, to_down, to_side_up, to_side_down = messages(index, buf, lane)
        to_side.wait()

        @pl.when(has_up)
        def _():
            to_up.wait_send()
            to_side_up.wait_send()
            to_down.wait_recv()
            to_side_down.wait_recv()

        @pl.when(has_down)
        def _():
            to_down.wait_send()
            to_side_down.wait_send()
            to_up.wait_recv()
            to_side_up.wait_recv()

        at, source = grid_iota(EXT, 3 * SIDE)
        place = ones_at((lax.rem(at, SIDE) == edge) & (at // SIDE + SIDE - 1 == source))
        fix = (factor + 1) * (1 - col)
        for a in range(factor):
            put = dot(place, jnp.concatenate([got[factor], got[a], got[factor + 1]], axis=0))
            plane = buf[a, fix, 1:ROWS - 1, :, lanes].reshape(PIX, width).astype(F32) + put[SIDE:EXT - SIDE]
            buf[a, fix, 1:ROWS - 1, :, lanes] = plane.astype(BF16).reshape(SIDE, SIDE, width)
            ends = ([(0, put[:SIDE])] if a == factor - 1 else []) + ([(ROWS - 1, put[EXT - SIDE:])] if a == 0 else [])
            for line, corner in ends:
                left = shift(buf[a, factor, line, :, lanes], False) + jnp.where(col == 1, corner, 0.0)
                right = shift(buf[a, 1, line, :, lanes], True) + jnp.where(col == 0, corner, 0.0)
                buf[a, 0, line, :, lanes] = left.astype(BF16)
                buf[a, factor + 1, line, :, lanes] = right.astype(BF16)

    ALL = [(dy, dx) for dy in range(3) for dx in range(3)]

    def gather(buf, factor, planes):
        rows = []
        for a, b in planes:
            parts = []
            for dy, dx in ALL:
                shifted = a + (dy - 1 + factor)
                piece = buf[lax.rem(shifted, factor), b + dx, pl.ds(shifted // factor, SIDE)]
                parts.append(piece.reshape(PIX, piece.shape[-1]))
            rows.append(jnp.concatenate(parts, axis=1))
        return jnp.concatenate(rows, axis=0)

    def conv(buf, factor, planes, weight):
        return dot(gather(buf, factor, planes), weight[...].reshape(9 * buf.shape[-1], weight.shape[-1]))

    def put_planes(buf, planes, value, lane=0):
        width = value.shape[-1]
        for k, (a, b) in enumerate(planes):
            plane = value[k * PIX:(k + 1) * PIX].reshape(SIDE, SIDE, width)
            buf[a, b + 1, 1:ROWS - 1, :, lane:lane + width] = plane

    def row_of(a):
        return [(a, b) for b in range(4)]

    def pool(src, dst, factor, lane, width):
        for a in range(factor):
            for b in range(factor):
                quad = [src[2 * a + p, 2 * b + q + 1, 1:ROWS - 1, :, lane:lane + width] for p in range(2) for q in range(2)]
                dst[a, b + 1, 1:ROWS - 1] = functools.reduce(jnp.maximum, quad)

    LEVEL2 = [(a, b) for a in range(2) for b in range(2)]

    def plane_of(buf, a, b, line, lane, width):
        return buf[a, b, pl.ds(line, SIDE), :, pl.ds(lane, width)].reshape(PIX, width)

    def near(a, buf, weight, lane, width):
        lhs = [plane_of(buf, k, l + 1, 1, lane, width) for k, l in LEVEL2]
        both = [jnp.concatenate([weight[k - a + 1, l - b + 1, lane:lane + width] for k, l in LEVEL2], axis=0) for b in range(2)]
        out = dot(jnp.concatenate(lhs, axis=1), jnp.concatenate(both, axis=1))
        return out[:, :C2], out[:, C2:]

    def sides(a, b, buf, weight, lane, width):
        lhs = [plane_of(buf, k, 3 * b, 1, lane, width) for k in range(2)]
        rhs = [weight[k - a + 1, 2 * b, lane:lane + width] for k in range(2)]
        return dot(jnp.concatenate(lhs, axis=1), jnp.concatenate(rhs, axis=0))

    def far_rows(a, b, buf, weight, lane, width):
        lhs = [plane_of(buf, 1 - a, b + dx, 2 * a, lane, width) for dx in range(3)]
        rhs = [weight[2 * a, dx, lane:lane + width] for dx in range(3)]
        return dot(jnp.concatenate(lhs, axis=1), jnp.concatenate(rhs, axis=0))

    def near_sums(again, *operands):
        @pl.loop(0, 2)
        def _(a):
            for b, value in enumerate(near(a, *operands)):
                part[2 * a + b] = part[2 * a + b] + value if again else value
            part[2 * a + col] += sides(a, col, *operands)

    def far_sums(put, *operands):
        for a in range(2):
            part[2 * a + 1 - col] += sides(a, 1 - col, *operands)
            for b in range(2):
                put(a, b, far_rows(a, b, *operands))

    def add(a, b, value):
        part[2 * a + b] += value

    def done(bias, put):
        return lambda a, b, value: put(a, b, biased_relu(part[2 * a + b] + value, bias))

    def conv_level2(index, src, weight, bias, put, first=None, then=None):
        width = src.shape[-1]
        start(index, src)
        if first is not None:
            first()
        near_sums(False, src, weight, 0, width)
        if then is not None:
            then()
        finish(index, src)
        far_sums(done(bias, put), src, weight, 0, width)

    at, to = grid_iota(HALF, HALF)
    split_cols = ones_at(at == lax.rem(to, SIDE) * 4 + to // SIDE)
    at, to = grid_iota(PIX, HALF)
    own_col = lax.rem(at, SIDE) == lax.rem(to, SIDE)
    fold_at, fold_to = grid_iota(HALF, LANE)
    small_copies[0].wait()
    image = []
    for ch in range(3):
        cols = dot(x[ch], split_cols).astype(BF16)
        for a in range(4):
            spread = ones_at(to == (at // SIDE) * 4 + a)
            lines = jnp.where(own_col, dot(spread, cols), 0.0).astype(BF16)
            image.append(dot(lines, ones_at(fold_to == fold_at // SIDE + (ch * SIDE + a * 4))))
    x1[0, 1, 1:ROWS - 1] = sum(image[1:], image[0]).astype(BF16).reshape(SIDE, SIDE, LANE)
    start(IMAGE, x1)

    mapped = ((cat1, 4), (d1a, 4), (p1, 2), (e2a, 2), (cat2, 2), (p2, 1), (ma, 1), (x1, 1))

    @pl.when(row == 0)
    def _():
        for buf, factor in mapped:
            buf[factor - 1, :, 0] = jnp.zeros(buf.shape[1:2] + buf.shape[3:], BF16)
        for buf, (factor, _) in zip(recv_cols, EXCHANGE):
            buf[factor] = jnp.zeros(buf.shape[1:], BF16)

    @pl.when(row == last)
    def _():
        for buf, factor in mapped:
            buf[0, :, ROWS - 1] = jnp.zeros(buf.shape[1:2] + buf.shape[3:], BF16)
        for buf, (factor, _) in zip(recv_cols, EXCHANGE):
            buf[factor + 1] = jnp.zeros(buf.shape[1:], BF16)


    for copy in small_copies[1:]:
        copy.wait()

    wf[...] = jnp.zeros(wf.shape, F32)
    for t in range(9):
        wf[pl.ds(4 * t, 3), :C1] = we1a[t // 3, t % 3].astype(F32)
    k, m = grid_iota(PATCH, TAPROWS)
    py, px = k // 32, lax.rem(k, 32) // 4
    base = py * 12 + px * 4 + lax.rem(k, 4)

    @pl.loop(0, 4)
    def _(a):
        for b in range(6):
            good = (py >= a) & (py <= a + 2) & (px >= b) & (px <= b + 2)
            place = ones_at(good & (m == base - a * 12 - b * 4))
            vw8[a * 6 + b] = dot(place, wf[...].astype(BF16)).astype(BF16)

    pad = jnp.zeros((1, HALF), F32)
    bpad[0:1, :C1P] = jnp.concatenate([be1a[...].reshape(1, C1), pad], axis=1)
    bpad[1:2, :C1P] = jnp.concatenate([pad, be1b[...].reshape(1, C1)], axis=1)
    bpad[2:3, :C1P] = jnp.concatenate([bd1a[...].reshape(1, C1), pad], axis=1)
    bpad[3:4, :] = bma[...].reshape(1, C3)
    bpad[4:5, :] = bmb[...].reshape(1, C3)
    copies[0].wait()

    @pl.loop(0, 3)
    def _(dy):
        for dx in range(3):
            value = jnp.concatenate([jnp.zeros((C1, HALF), F32), re1b[dy, dx].astype(F32)], axis=1)
            ve1b[dy, dx, :C1] = value.astype(BF16)
            ve1b[dy, dx, C1:] = jnp.zeros((HALF, C1P), BF16)

    finish(IMAGE, x1)

    blank = jnp.zeros((SIDE, LANE), BF16)
    lane, k = grid_iota(LANE, PATCH)
    ch, a, b = lane // SIDE, lax.rem(lane, SIDE) // 4, lax.rem(lane, 4)
    patches = []
    for dx in range(3):
        plane = x1[0, dx].reshape(EXT, LANE)
        blocks = (jnp.concatenate([blank, plane[:-SIDE]], axis=0), plane, jnp.concatenate([plane[SIDE:], blank], axis=0))
        for dy, block in enumerate(blocks):
            py, px = a + (4 * dy - 3), b + (4 * dx - 2)
            good = (ch < 3) & (py >= 0) & (py < 6) & (px >= 0) & (px < 8)
            patches.append(dot(block, ones_at(good & (k == py * 32 + px * 4 + ch))))
    x8[...] = sum(patches[1:], patches[0]).astype(BF16)

    pos = iota((EXT, C1P), 0)
    pos_col = lax.rem(pos, SIDE)
    off = {0: (pos_col == 0) & (col == 0), 5: (pos_col == SIDE - 1) & (col == 1)}

    @pl.loop(0, 2)
    def _(t):
        for a, b in [(2 * t + k, b) for k in range(2) for b in range(6)]:
            out = jnp.maximum(dot(x8[...], vw8[a * 6 + b]) + bpad[0:1, :C1P], 0.0)
            if b in off:
                out = jnp.where(off[b], 0.0, out)
            h1[a, b] = out.astype(BF16).reshape(ROWS, SIDE, C1P)

    @pl.when(row == 0)
    def _():
        h1[3, :, 0] = jnp.zeros((6, SIDE, C1P), BF16)

    @pl.when(row == last)
    def _():
        h1[0, :, ROWS - 1] = jnp.zeros((6, SIDE, C1P), BF16)

    @pl.loop(0, 2)
    def _(t):
        for a in (2 * t, 2 * t + 1):
            put_planes(cat1, row_of(a), biased_relu(conv(h1, 4, row_of(a), ve1b), bpad.at[1:2, :C1P]), LANE)

    pool(cat1, p1, 2, LANE, C1P)

    ve2a[:, :, :HALF, :] = jnp.zeros((3, 3, HALF, C2), BF16)

    def fill_constants():
        start(SKIP1, cat1, LANE)
        n, m = grid_iota(2 * PIX, 2 * PIX)
        weave[...] = ones_at(m == lax.rem(n, 4) * LANE + (n // HALF) * SIDE + lax.rem(n, HALF) // 4)
        vd1b[:, :, C1:, :] = jnp.zeros((3, 3, HALF, C1), BF16)
        vd1a[C1:, :] = jnp.zeros((HALF, vd1a.shape[1]), BF16)
        heads[...] = jnp.zeros(heads.shape, F32)

    copies[1].wait()
    conv_level2(POOL1, p1, ve2a, be2a, lambda a, b, value: put_planes(e2a, [(a, b)], value), first=fill_constants)
    copies[2].wait()
    conv_level2(ENC2A, e2a, ve2b, be2b, lambda a, b, value: put_planes(cat2, [(a, b)], value, C2),
                then=lambda: finish(SKIP1, cat1, LANE))
    copies[-1].start()
    pool(cat2, p2, 1, C2, C2)

    start(POOL2, p2)
    start(SKIP2, cat2, C2)
    copies[6].wait()
    near_sums(False, cat2, vd2a, C2, C2)
    copies[3].wait()
    finish(POOL2, p2)

    def conv_level3(src, weight, bias, put):
        @pl.loop(0, 3)
        def _(n):
            lanes = pl.ds(pl.multiple_of(n * PIX, PIX), PIX)
            flat = weight[:, :, :, lanes].reshape(9 * src.shape[-1], PIX)
            put(lanes, biased_relu(dot(gather(src, 1, [(0, 0)]), flat), bpad.at[bias:bias + 1, lanes]))

    def put_ma(lanes, value):
        ma[0, 1, 1:ROWS - 1, :, lanes] = value.reshape(SIDE, SIDE, PIX)

    def put_mid(lanes, value):
        mid[:, lanes] = value

    conv_level3(p2, vma, 3, put_ma)
    start(MIDA, ma)
    finish(SKIP2, cat2, C2)
    far_sums(add, cat2, vd2a, C2, C2)
    copies[4].wait()
    finish(MIDA, ma)
    conv_level3(ma, vmb, 4, put_mid)
    copies[5].wait()
    for p in range(2):
        out = dot(mid[...], jnp.concatenate([vu2[p, 0], vu2[p, 1]], axis=1)).astype(BF16)
        for q in range(2):
            put_planes(cat2, [(p, q)], out[:, q * C2:(q + 1) * C2])
    start(UP2, cat2)
    near_sums(True, cat2, vd2a, 0, C2)
    finish(UP2, cat2)
    far_sums(done(bd2a, lambda a, b, value: put_planes(e2a, [(a, b)], value)), cat2, vd2a, 0, C2)
    copies[-1].wait()

    def put_d2(a, b, value):
        d2[pl.ds((2 * a + b) * PIX, PIX)] = value

    conv_level2(DEC2A, e2a, ve2b, bd2b, put_d2)
    copies[7].wait()

    @pl.loop(0, 2)
    def _(t):
        lhs = d2[pl.ds(2 * t * PIX, 2 * PIX)]
        for p, q in LEVEL2:
            put_planes(cat1, [(2 * t + p, q), (2 * t + p, q + 2)], dot_rows(lhs, vu1[p, q]).astype(BF16))

    for copy in copies[8:17]:
        copy.wait()

    border = 3 * col

    def level1(index, src, layer):
        start(index, src)
        for a in (1, 2):
            layer([(a, 1), (a, 2), (a, border)])
        finish(index, src)
        layer([(1, 3 - border), (2, 3 - border)])
        for a in (0, 3):
            layer(row_of(a))

    def dec1a(planes):
        put_planes(d1a, planes, biased_relu(dot_rows(gather(cat1, 4, planes), vd1a[...]), bpad.at[2:3, :C1P]))

    level1(CAT1, cat1, dec1a)
    copies[17].wait()

    def head(a):
        lines = [h1[a, b + 1, pl.ds(8 * h + 1, 8), :, :C1].reshape(LANE, C1) for h in range(2) for b in range(4)]
        heads[a, :6] = dot_rows(wh[...], jnp.concatenate(lines, axis=0))

    def dec1b(planes):
        put_planes(h1, planes, biased_relu(conv(d1a, 4, planes, vd1b), bd1b))

    level1(DEC1A, d1a, dec1b)
    for a in range(4):
        head(a)
    wide = 2 * PIX
    flat = jnp.concatenate([heads[a, :, h * wide:(h + 1) * wide] for a in range(4) for h in range(2)], axis=0)
    high = flat.astype(BF16)
    rest = flat - high.astype(F32)
    middle = rest.astype(BF16)
    low = (rest - middle.astype(F32)).astype(BF16)
    woven = dot_rows(high, weave[...]) + dot_rows(middle, weave[...]) + dot_rows(low, weave[...])
    for a in range(4):
        for h in range(2):
            for i in range(8):
                y[:, 4 * (8 * h + i) + a, :] = woven[(2 * a + h) * 8:(2 * a + h) * 8 + 6, i * HALF:(i + 1) * HALF]


def solution(mesh):
    tile_spec = P(("data", "row"), "col", None)

    def device_body(image_tile, *params):
        (w_enc1a, b_enc1a, w_enc1b, b_enc1b, w_enc2a, b_enc2a, w_enc2b, b_enc2b,
         w_mid_a, b_mid_a, w_mid_b, b_mid_b, w_up2, w_dec2a, b_dec2a, w_dec2b, b_dec2b,
         w_up1, w_dec1a, b_dec1a, w_dec1b, b_dec1b, w_head, b_head) = params
        anywhere = pl.BlockSpec(memory_space=pl.ANY)
        vmem = pl.BlockSpec(memory_space=pltpu.VMEM)
        small = [
            jnp.transpose(image_tile, (2, 0, 1)), w_enc1a, w_head.T, b_enc1a, b_enc1b, b_enc2a, b_enc2b,
            b_mid_a, b_mid_b, b_dec2a, b_dec2b, b_dec1a, b_dec1b,
        ]
        operands = [
            w_enc1b, w_enc2a, w_enc2b, w_mid_a, w_mid_b, w_up2, w_dec2a, w_dec2b,
            jnp.swapaxes(w_up1, 2, 3), jnp.swapaxes(w_dec1a, 2, 3), w_dec1b,
        ]

        def kept(*shape, dtype=BF16):
            return pltpu.VMEM(shape, dtype)

        def level(factor, lanes):
            return kept(factor, factor + 2, ROWS, SIDE, lanes)

        scratch = [
            kept(24, PATCH, C1P), kept(3, 3, C1, C1), kept(3, 3, C1P, C1P), kept(3, 3, C1P, C2), kept(3, 3, C2, C2),
            kept(3, 3, C2, C3), kept(3, 3, C3, C3), kept(2, 2, C3, C2), kept(3, 3, C3, C2),
            kept(2, 2, C1, C2), kept(C1P, 9 * C2), kept(3, 3, C1P, C1),
            level(4, C1P), level(4, C2), level(4, C1P), level(2, C1P), level(2, C2), level(2, C3),
            kept(4 * PIX, C2), level(1, C2), level(1, C3), kept(PIX, C3), level(1, LANE), kept(EXT, PATCH),
            kept(TAPROWS, C1P, dtype=F32), kept(5, C3, dtype=F32), kept(2 * PIX, 2 * PIX),
            kept(4, PIX, C2, dtype=F32), kept(4, 8, 4 * PIX, dtype=F32),
        ]
        scratch += [kept(factor, SIDE, width) for factor, width in EXCHANGE]
        scratch += [kept(factor + 2, SIDE, width) for factor, width in EXCHANGE]
        links = pltpu.SemaphoreType.DMA((len(EXCHANGE), MESSAGES))
        scratch += [pltpu.SemaphoreType.DMA((LOADS,)), links, links, pltpu.SemaphoreType.DMA((SMALL,))]
        scratch = [kept(*array.shape, dtype=array.dtype) for array in small] + scratch
        out = pl.pallas_call(
            functools.partial(kernel, mesh.shape["row"]),
            name="unet",
            out_shape=jax.ShapeDtypeStruct((6, HALF, HALF), F32),
            in_specs=[anywhere] * (len(operands) + SMALL),
            out_specs=vmem,
            scratch_shapes=scratch,
            compiler_params=pltpu.CompilerParams(collective_id=0, has_side_effects=True, vmem_limit_bytes=67043328),
        )(*operands, *small)
        return jnp.transpose(out, (1, 2, 0)) + b_head

    def program(image, *params):
        mapped = jax.shard_map(device_body, mesh=mesh, in_specs=(tile_spec,) + tuple([P()] * len(params)), out_specs=tile_spec, check_vma=False)
        return mapped(image, *params)

    return program
```

```python
import functools

import jax
import jax.numpy as jnp
from jax import lax
from jax.experimental import pallas as pl
from jax.experimental.pallas import tpu as pltpu
from jax.sharding import PartitionSpec as P

MESH = pl.DeviceIdType.MESH
F32 = jnp.float32
BF16 = jnp.bfloat16
ROWS = 18
SIDE = 16
PIX = SIDE * SIDE
EXT = ROWS * SIDE
C1 = 192
C1P = 256
C2 = 384
C3 = 768
HALF = 64
LANE = 128
PATCH = 192
TAPROWS = 40
BY_ROWS = (((1,), (1,)), ((), ()))
POOL1, ENC2A, POOL2, MIDA, UP2, DEC2A, CAT1, DEC1A, IMAGE, SKIP2, SKIP1 = range(11)
EXCHANGE = ((2, C1P), (2, C2), (1, C2), (1, C3), (2, C2), (2, C2), (4, C1P), (4, C1P), (1, LANE), (2, C2), (4, C1P))
MESSAGES = 5
LOADS = 19
SMALL = 13


def iota(shape, dim):
    return lax.broadcasted_iota(jnp.int32, shape, dim)


def grid_iota(*shape):
    return iota(shape, 0), iota(shape, 1)


def ones_at(mask):
    return mask.astype(F32).astype(BF16)


def dot(lhs, rhs):
    return jnp.dot(lhs, rhs, preferred_element_type=F32)


def dot_rows(lhs, rhs):
    return lax.dot_general(lhs, rhs, BY_ROWS, preferred_element_type=F32)


def biased_relu(acc, bias):
    return jnp.maximum(acc + bias[...].reshape(1, bias.shape[-1]), 0.0).astype(BF16)


def kernel(row_count, we1b, we2a, we2b, wma, wmb, wu2, wd2a, wd2b, wu1, wd1a, wd1b, *scratch):
    small, y, scratch = scratch[:SMALL], scratch[SMALL], scratch[SMALL + 1:]
    near_small, scratch = scratch[:SMALL], scratch[SMALL:]
    x, we1a, wh, be1a, be1b, be2a, be2b, bma, bmb, bd2a, bd2b, bd1a, bd1b = near_small
    small_sem, scratch = scratch[-1], scratch[:-1]
    small_copies = [pltpu.make_async_copy(src, dst, small_sem.at[k]) for k, (src, dst) in enumerate(zip(small, near_small))]
    for copy in small_copies:
        copy.start()
    (vw8, re1b, ve1b, ve2a, ve2b, vma, vmb, vu2, vd2a, vu1, vd1a, vd1b,
     h1, cat1, d1a, p1, e2a, cat2, d2, p2, ma, mid, x1, x8, wf, bpad, weave, part, heads) = scratch[:-2 * len(EXCHANGE) - 3]
    send_cols = scratch[-2 * len(EXCHANGE) - 3:-len(EXCHANGE) - 3]
    recv_cols = scratch[-len(EXCHANGE) - 3:-3]
    w_sem, send_sem, recv_sem = scratch[-3:]
    row, col, data = lax.axis_index("row"), lax.axis_index("col"), lax.axis_index("data")
    last = row_count - 1
    has_up, has_down = row > 0, row < last
    up, down = (data, col, row - 1), (data, col, row + 1)
    side, side_up, side_down = (data, 1 - col, row), (data, 1 - col, row - 1), (data, 1 - col, row + 1)
    edge = (1 - col) * (SIDE - 1)

    barrier = pltpu.get_barrier_semaphore()

    def arrive(device):
        pl.semaphore_signal(barrier, inc=1, device_id=device, device_id_type=MESH)

    arrive(side)

    @pl.when(has_up)
    def _():
        arrive(up)
        arrive(side_up)

    @pl.when(has_down)
    def _():
        arrive(down)
        arrive(side_down)

    loads = [(we1b, re1b), (we2a, ve2a.at[:, :, HALF:, :]), (we2b, ve2b), (wma, vma), (wmb, vmb),
             (wu2, vu2), (wd2a, vd2a), (wu1, vu1)]
    loads += [(wd1a.at[t // 3, t % 3], vd1a.at[:C1, pl.ds(t * C2, C2)]) for t in range(9)]
    loads += [(wd1b, vd1b.at[:, :, :C1, :]), (wd2b, ve2b)]
    copies = [pltpu.make_async_copy(src, dst, w_sem.at[k]) for k, (src, dst) in enumerate(loads)]
    for copy in copies[:3]:
        copy.start()
    for copy in copies[3:-1]:
        copy.start()

    def messages(index, buf, lane):
        factor, width = EXCHANGE[index]
        cols, got = send_cols[index], recv_cols[index]
        own = pl.ds(1, factor)
        lanes = pl.ds(lane, width)

        def remote(k, src, dst, device):
            return pltpu.make_async_remote_copy(
                src_ref=src, dst_ref=dst, send_sem=send_sem.at[index, k], recv_sem=recv_sem.at[index, k],
                device_id=device, device_id_type=MESH)

        routes = (
            (cols, got.at[pl.ds(0, factor)], side),
            (buf.at[0, own, 1, :, lanes], buf.at[0, own, ROWS - 1, :, lanes], up),
            (buf.at[factor - 1, own, ROWS - 2, :, lanes], buf.at[factor - 1, own, 0, :, lanes], down),
            (cols.at[0], got.at[factor + 1], side_up),
            (cols.at[factor - 1], got.at[factor], side_down),
        )
        return [remote(k, *route) for k, route in enumerate(routes)]

    def shift(value, right):
        value = value.astype(F32)
        count = value.shape[0]
        at = lax.rem(iota(value.shape, 0), SIDE)
        if right:
            return jnp.where(at == SIDE - 1, 0.0, pltpu.roll(value, count - 1, 0))
        return jnp.where(at == 0, 0.0, pltpu.roll(value, 1, 0))

    def start(index, buf, lane=0):
        factor, width = EXCHANGE[index]
        lanes = pl.ds(lane, width)
        to_side, to_up, to_down, to_side_up, to_side_down = messages(index, buf, lane)
        if index == IMAGE:
            pl.semaphore_wait(barrier, 2 * has_up.astype(jnp.int32) + 2 * has_down.astype(jnp.int32) + 1)

        @pl.when(has_up)
        def _():
            to_up.start()

        @pl.when(has_down)
        def _():
            to_down.start()

        pick_row, pick_at = grid_iota(SIDE, PIX)
        pick = ones_at(pick_at == pick_row * SIDE + edge)
        cols = send_cols[index]
        for a in range(factor):
            plane = buf[a, 1 + (factor - 1) * (1 - col), 1:ROWS - 1, :, lanes].reshape(PIX, width)
            cols[a] = dot(pick, plane).astype(BF16)
        to_side.start()

        @pl.when(has_up)
        def _():
            to_side_up.start()

        @pl.when(has_down)
        def _():
            to_side_down.start()

        def shifted(a):
            for source, target in ((factor, 0), (1, factor + 1)):
                value = shift(buf[a, source, 1:ROWS - 1, :, lanes].reshape(PIX, width), target > 0)
                buf[a, target, 1:ROWS - 1, :, lanes] = value.astype(BF16).reshape(SIDE, SIDE, width)

        if factor == 1:
            shifted(0)
        else:
            pl.loop(0, factor)(shifted)

    def finish(index, buf, lane=0):
        factor, width = EXCHANGE[index]
        lanes = pl.ds(lane, width)
        got = recv_cols[index]
        to_side, to_up, to_down, to_side_up, to_side_down = messages(index, buf, lane)
        to_side.wait()

        @pl.when(has_up)
        def _():
            to_up.wait_send()
            to_side_up.wait_send()
            to_down.wait_recv()
            to_side_down.wait_recv()

        @pl.when(has_down)
        def _():
            to_down.wait_send()
            to_side_down.wait_send()
            to_up.wait_recv()
            to_side_up.wait_recv()

        at, source = grid_iota(EXT, 3 * SIDE)
        place = ones_at((lax.rem(at, SIDE) == edge) & (at // SIDE + SIDE - 1 == source))
        fix = (factor + 1) * (1 - col)
        for a in range(factor):
            put = dot(place, jnp.concatenate([got[factor], got[a], got[factor + 1]], axis=0))
            plane = buf[a, fix, 1:ROWS - 1, :, lanes].reshape(PIX, width).astype(F32) + put[SIDE:EXT - SIDE]
            buf[a, fix, 1:ROWS - 1, :, lanes] = plane.astype(BF16).reshape(SIDE, SIDE, width)
            ends = ([(0, put[:SIDE])] if a == factor - 1 else []) + ([(ROWS - 1, put[EXT - SIDE:])] if a == 0 else [])
            for line, corner in ends:
                left = shift(buf[a, factor, line, :, lanes], False) + jnp.where(col == 1, corner, 0.0)
                right = shift(buf[a, 1, line, :, lanes], True) + jnp.where(col == 0, corner, 0.0)
                buf[a, 0, line, :, lanes] = left.astype(BF16)
                buf[a, factor + 1, line, :, lanes] = right.astype(BF16)

    ALL = [(dy, dx) for dy in range(3) for dx in range(3)]

    def gather(buf, factor, planes):
        rows = []
        for a, b in planes:
            parts = []
            for dy, dx in ALL:
                shifted = a + (dy - 1 + factor)
                piece = buf[lax.rem(shifted, factor), b + dx, pl.ds(shifted // factor, SIDE)]
                parts.append(piece.reshape(PIX, piece.shape[-1]))
            rows.append(jnp.concatenate(parts, axis=1))
        return jnp.concatenate(rows, axis=0)

    def conv(buf, factor, planes, weight):
        return dot(gather(buf, factor, planes), weight[...].reshape(9 * buf.shape[-1], weight.shape[-1]))

    def put_planes(buf, planes, value, lane=0):
        width = value.shape[-1]
        for k, (a, b) in enumerate(planes):
            plane = value[k * PIX:(k + 1) * PIX].reshape(SIDE, SIDE, width)
            buf[a, b + 1, 1:ROWS - 1, :, lane:lane + width] = plane

    def row_of(a):
        return [(a, b) for b in range(4)]

    def pool(src, dst, factor, lane, width):
        for a in range(factor):
            for b in range(factor):
                quad = [src[2 * a + p, 2 * b + q + 1, 1:ROWS - 1, :, lane:lane + width] for p in range(2) for q in range(2)]
                dst[a, b + 1, 1:ROWS - 1] = functools.reduce(jnp.maximum, quad)

    LEVEL2 = [(a, b) for a in range(2) for b in range(2)]

    def plane_of(buf, a, b, line, lane, width):
        return buf[a, b, pl.ds(line, SIDE), :, pl.ds(lane, width)].reshape(PIX, width)

    def near(a, buf, weight, lane, width):
        lhs = [plane_of(buf, k, l + 1, 1, lane, width) for k, l in LEVEL2]
        both = [jnp.concatenate([weight[k - a + 1, l - b + 1, lane:lane + width] for k, l in LEVEL2], axis=0) for b in range(2)]
        out = dot(jnp.concatenate(lhs, axis=1), jnp.concatenate(both, axis=1))
        return out[:, :C2], out[:, C2:]

    def sides(a, b, buf, weight, lane, width):
        lhs = [plane_of(buf, k, 3 * b, 1, lane, width) for k in range(2)]
        rhs = [weight[k - a + 1, 2 * b, lane:lane + width] for k in range(2)]
        return dot(jnp.concatenate(lhs, axis=1), jnp.concatenate(rhs, axis=0))

    def far_rows(a, b, buf, weight, lane, width):
        lhs = [plane_of(buf, 1 - a, b + dx, 2 * a, lane, width) for dx in range(3)]
        rhs = [weight[2 * a, dx, lane:lane + width] for dx in range(3)]
        return dot(jnp.concatenate(lhs, axis=1), jnp.concatenate(rhs, axis=0))

    def near_sums(again, *operands):
        @pl.loop(0, 2)
        def _(a):
            for b, value in enumerate(near(a, *operands)):
                part[2 * a + b] = part[2 * a + b] + value if again else value
            part[2 * a + col] += sides(a, col, *operands)

    def far_sums(put, *operands):
        for a in range(2):
            part[2 * a + 1 - col] += sides(a, 1 - col, *operands)
            for b in range(2):
                put(a, b, far_rows(a, b, *operands))

    def add(a, b, value):
        part[2 * a + b] += value

    def done(bias, put):
        return lambda a, b, value: put(a, b, biased_relu(part[2 * a + b] + value, bias))

    def conv_level2(index, src, weight, bias, put, first=None, then=None):
        width = src.shape[-1]
        start(index, src)
        if first is not None:
            first()
        near_sums(False, src, weight, 0, width)
        if then is not None:
            then()
        finish(index, src)
        far_sums(done(bias, put), src, weight, 0, width)

    at, to = grid_iota(HALF, HALF)
    split_cols = ones_at(at == lax.rem(to, SIDE) * 4 + to // SIDE)
    at, to = grid_iota(PIX, HALF)
    own_col = lax.rem(at, SIDE) == lax.rem(to, SIDE)
    fold_at, fold_to = grid_iota(HALF, LANE)
    small_copies[0].wait()
    image = []
    for ch in range(3):
        cols = dot(x[ch], split_cols).astype(BF16)
        for a in range(4):
            spread = ones_at(to == (at // SIDE) * 4 + a)
            lines = jnp.where(own_col, dot(spread, cols), 0.0).astype(BF16)
            image.append(dot(lines, ones_at(fold_to == fold_at // SIDE + (ch * SIDE + a * 4))))
    x1[0, 1, 1:ROWS - 1] = sum(image[1:], image[0]).astype(BF16).reshape(SIDE, SIDE, LANE)
    start(IMAGE, x1)

    mapped = ((cat1, 4), (d1a, 4), (p1, 2), (e2a, 2), (cat2, 2), (p2, 1), (ma, 1), (x1, 1))

    @pl.when(row == 0)
    def _():
        for buf, factor in mapped:
            buf[factor - 1, :, 0] = jnp.zeros(buf.shape[1:2] + buf.shape[3:], BF16)
        for buf, (factor, _) in zip(recv_cols, EXCHANGE):
            buf[factor] = jnp.zeros(buf.shape[1:], BF16)

    @pl.when(row == last)
    def _():
        for buf, factor in mapped:
            buf[0, :, ROWS - 1] = jnp.zeros(buf.shape[1:2] + buf.shape[3:], BF16)
        for buf, (factor, _) in zip(recv_cols, EXCHANGE):
            buf[factor + 1] = jnp.zeros(buf.shape[1:], BF16)


    for copy in small_copies[1:]:
        copy.wait()

    wf[...] = jnp.zeros(wf.shape, F32)
    for t in range(9):
        wf[pl.ds(4 * t, 3), :C1] = we1a[t // 3, t % 3].astype(F32)
    k, m = grid_iota(PATCH, TAPROWS)
    py, px = k // 32, lax.rem(k, 32) // 4
    base = py * 12 + px * 4 + lax.rem(k, 4)

    @pl.loop(0, 4)
    def _(a):
        for b in range(6):
            good = (py >= a) & (py <= a + 2) & (px >= b) & (px <= b + 2)
            place = ones_at(good & (m == base - a * 12 - b * 4))
            vw8[a * 6 + b] = dot(place, wf[...].astype(BF16)).astype(BF16)

    pad = jnp.zeros((1, HALF), F32)
    bpad[0:1, :C1P] = jnp.concatenate([be1a[...].reshape(1, C1), pad], axis=1)
    bpad[1:2, :C1P] = jnp.concatenate([pad, be1b[...].reshape(1, C1)], axis=1)
    bpad[2:3, :C1P] = jnp.concatenate([bd1a[...].reshape(1, C1), pad], axis=1)
    bpad[3:4, :] = bma[...].reshape(1, C3)
    bpad[4:5, :] = bmb[...].reshape(1, C3)
    copies[0].wait()

    @pl.loop(0, 3)
    def _(dy):
        for dx in range(3):
            value = jnp.concatenate([jnp.zeros((C1, HALF), F32), re1b[dy, dx].astype(F32)], axis=1)
            ve1b[dy, dx, :C1] = value.astype(BF16)
            ve1b[dy, dx, C1:] = jnp.zeros((HALF, C1P), BF16)

    finish(IMAGE, x1)

    blank = jnp.zeros((SIDE, LANE), BF16)
    lane, k = grid_iota(LANE, PATCH)
    ch, a, b = lane // SIDE, lax.rem(lane, SIDE) // 4, lax.rem(lane, 4)
    patches = []
    for dx in range(3):
        plane = x1[0, dx].reshape(EXT, LANE)
        blocks = (jnp.concatenate([blank, plane[:-SIDE]], axis=0), plane, jnp.concatenate([plane[SIDE:], blank], axis=0))
        for dy, block in enumerate(blocks):
            py, px = a + (4 * dy - 3), b + (4 * dx - 2)
            good = (ch < 3) & (py >= 0) & (py < 6) & (px >= 0) & (px < 8)
            patches.append(dot(block, ones_at(good & (k == py * 32 + px * 4 + ch))))
    x8[...] = sum(patches[1:], patches[0]).astype(BF16)

    pos = iota((EXT, C1P), 0)
    pos_col = lax.rem(pos, SIDE)
    off = {0: (pos_col == 0) & (col == 0), 5: (pos_col == SIDE - 1) & (col == 1)}

    @pl.loop(0, 2)
    def _(t):
        for a, b in [(2 * t + k, b) for k in range(2) for b in range(6)]:
            out = jnp.maximum(dot(x8[...], vw8[a * 6 + b]) + bpad[0:1, :C1P], 0.0)
            if b in off:
                out = jnp.where(off[b], 0.0, out)
            h1[a, b] = out.astype(BF16).reshape(ROWS, SIDE, C1P)

    @pl.when(row == 0)
    def _():
        h1[3, :, 0] = jnp.zeros((6, SIDE, C1P), BF16)

    @pl.when(row == last)
    def _():
        h1[0, :, ROWS - 1] = jnp.zeros((6, SIDE, C1P), BF16)

    for a in range(4):
        put_planes(cat1, row_of(a), biased_relu(conv(h1, 4, row_of(a), ve1b), bpad.at[1:2, :C1P]), LANE)

    pool(cat1, p1, 2, LANE, C1P)

    ve2a[:, :, :HALF, :] = jnp.zeros((3, 3, HALF, C2), BF16)

    def fill_constants():
        start(SKIP1, cat1, LANE)
        n, m = grid_iota(2 * PIX, 2 * PIX)
        weave[...] = ones_at(m == lax.rem(n, 4) * LANE + (n // HALF) * SIDE + lax.rem(n, HALF) // 4)
        vd1b[:, :, C1:, :] = jnp.zeros((3, 3, HALF, C1), BF16)
        vd1a[C1:, :] = jnp.zeros((HALF, vd1a.shape[1]), BF16)
        heads[...] = jnp.zeros(heads.shape, F32)

    copies[1].wait()
    conv_level2(POOL1, p1, ve2a, be2a, lambda a, b, value: put_planes(e2a, [(a, b)], value), first=fill_constants)
    copies[2].wait()
    conv_level2(ENC2A, e2a, ve2b, be2b, lambda a, b, value: put_planes(cat2, [(a, b)], value, C2),
                then=lambda: finish(SKIP1, cat1, LANE))
    copies[-1].start()
    pool(cat2, p2, 1, C2, C2)

    start(POOL2, p2)
    start(SKIP2, cat2, C2)
    copies[6].wait()
    near_sums(False, cat2, vd2a, C2, C2)
    copies[3].wait()
    finish(POOL2, p2)

    def conv_level3(src, weight, bias, put):
        @pl.loop(0, 3)
        def _(n):
            lanes = pl.ds(pl.multiple_of(n * PIX, PIX), PIX)
            flat = weight[:, :, :, lanes].reshape(9 * src.shape[-1], PIX)
            put(lanes, biased_relu(dot(gather(src, 1, [(0, 0)]), flat), bpad.at[bias:bias + 1, lanes]))

    def put_ma(lanes, value):
        ma[0, 1, 1:ROWS - 1, :, lanes] = value.reshape(SIDE, SIDE, PIX)

    def put_mid(lanes, value):
        mid[:, lanes] = value

    conv_level3(p2, vma, 3, put_ma)
    start(MIDA, ma)
    finish(SKIP2, cat2, C2)
    far_sums(add, cat2, vd2a, C2, C2)
    copies[4].wait()
    finish(MIDA, ma)
    conv_level3(ma, vmb, 4, put_mid)
    copies[5].wait()
    for p in range(2):
        out = dot(mid[...], jnp.concatenate([vu2[p, 0], vu2[p, 1]], axis=1)).astype(BF16)
        for q in range(2):
            put_planes(cat2, [(p, q)], out[:, q * C2:(q + 1) * C2])
    start(UP2, cat2)
    near_sums(True, cat2, vd2a, 0, C2)
    finish(UP2, cat2)
    far_sums(done(bd2a, lambda a, b, value: put_planes(e2a, [(a, b)], value)), cat2, vd2a, 0, C2)
    copies[-1].wait()

    def put_d2(a, b, value):
        d2[pl.ds((2 * a + b) * PIX, PIX)] = value

    conv_level2(DEC2A, e2a, ve2b, bd2b, put_d2)
    copies[7].wait()

    for t in range(2):
        lhs = d2[pl.ds(2 * t * PIX, 2 * PIX)]
        for p, q in LEVEL2:
            put_planes(cat1, [(2 * t + p, q), (2 * t + p, q + 2)], dot_rows(lhs, vu1[p, q]).astype(BF16))

    for copy in copies[8:17]:
        copy.wait()

    border = 3 * col

    def dec1a(planes):
        put_planes(d1a, planes, biased_relu(dot_rows(gather(cat1, 4, planes), vd1a[...]), bpad.at[2:3, :C1P]))

    inner = (1, 2)
    fixed = [(a, 3 - border) for a in inner]
    start(CAT1, cat1)
    dec1a([(1, b) for b in inner])
    dec1a([(a, border) for a in inner])
    finish(CAT1, cat1)
    dec1a(fixed)
    for a in (0, 3):
        dec1a(row_of(a))
    start(DEC1A, d1a)
    dec1a([(2, b) for b in inner])
    copies[17].wait()

    def head(a):
        lines = [h1[a, b + 1, pl.ds(8 * h + 1, 8), :, :C1].reshape(LANE, C1) for h in range(2) for b in range(4)]
        heads[a, :6] = dot_rows(wh[...], jnp.concatenate(lines, axis=0))

    def dec1b(planes):
        put_planes(h1, planes, biased_relu(conv(d1a, 4, planes, vd1b), bd1b))

    for a in inner:
        dec1b([(a, b) for b in (*inner, border)])
    finish(DEC1A, d1a)
    dec1b(fixed)
    for a in inner:
        head(a)
    for a in (0, 3):
        dec1b(row_of(a))
        head(a)
    wide = 2 * PIX
    flat = jnp.concatenate([heads[a, :, h * wide:(h + 1) * wide] for a in range(4) for h in range(2)], axis=0)
    high = flat.astype(BF16)
    rest = flat - high.astype(F32)
    middle = rest.astype(BF16)
    low = (rest - middle.astype(F32)).astype(BF16)
    woven = dot_rows(high, weave[...]) + dot_rows(middle, weave[...]) + dot_rows(low, weave[...])
    for a in range(4):
        for h in range(2):
            for i in range(8):
                y[:, 4 * (8 * h + i) + a, :] = woven[(2 * a + h) * 8:(2 * a + h) * 8 + 6, i * HALF:(i + 1) * HALF]


def solution(mesh):
    tile_spec = P(("data", "row"), "col", None)

    def device_body(image_tile, *params):
        (w_enc1a, b_enc1a, w_enc1b, b_enc1b, w_enc2a, b_enc2a, w_enc2b, b_enc2b,
         w_mid_a, b_mid_a, w_mid_b, b_mid_b, w_up2, w_dec2a, b_dec2a, w_dec2b, b_dec2b,
         w_up1, w_dec1a, b_dec1a, w_dec1b, b_dec1b, w_head, b_head) = params
        anywhere = pl.BlockSpec(memory_space=pl.ANY)
        vmem = pl.BlockSpec(memory_space=pltpu.VMEM)
        small = [
            jnp.transpose(image_tile, (2, 0, 1)), w_enc1a, w_head.T, b_enc1a, b_enc1b, b_enc2a, b_enc2b,
            b_mid_a, b_mid_b, b_dec2a, b_dec2b, b_dec1a, b_dec1b,
        ]
        operands = [
            w_enc1b, w_enc2a, w_enc2b, w_mid_a, w_mid_b, w_up2, w_dec2a, w_dec2b,
            jnp.swapaxes(w_up1, 2, 3), jnp.swapaxes(w_dec1a, 2, 3), w_dec1b,
        ]

        def kept(*shape, dtype=BF16):
            return pltpu.VMEM(shape, dtype)

        def level(factor, lanes):
            return kept(factor, factor + 2, ROWS, SIDE, lanes)

        scratch = [
            kept(24, PATCH, C1P), kept(3, 3, C1, C1), kept(3, 3, C1P, C1P), kept(3, 3, C1P, C2), kept(3, 3, C2, C2),
            kept(3, 3, C2, C3), kept(3, 3, C3, C3), kept(2, 2, C3, C2), kept(3, 3, C3, C2),
            kept(2, 2, C1, C2), kept(C1P, 9 * C2), kept(3, 3, C1P, C1),
            level(4, C1P), level(4, C2), level(4, C1P), level(2, C1P), level(2, C2), level(2, C3),
            kept(4 * PIX, C2), level(1, C2), level(1, C3), kept(PIX, C3), level(1, LANE), kept(EXT, PATCH),
            kept(TAPROWS, C1P, dtype=F32), kept(5, C3, dtype=F32), kept(2 * PIX, 2 * PIX),
            kept(4, PIX, C2, dtype=F32), kept(4, 8, 4 * PIX, dtype=F32),
        ]
        scratch += [kept(factor, SIDE, width) for factor, width in EXCHANGE]
        scratch += [kept(factor + 2, SIDE, width) for factor, width in EXCHANGE]
        links = pltpu.SemaphoreType.DMA((len(EXCHANGE), MESSAGES))
        scratch += [pltpu.SemaphoreType.DMA((LOADS,)), links, links, pltpu.SemaphoreType.DMA((SMALL,))]
        scratch = [kept(*array.shape, dtype=array.dtype) for array in small] + scratch
        out = pl.pallas_call(
            functools.partial(kernel, mesh.shape["row"]),
            name="unet",
            out_shape=jax.ShapeDtypeStruct((6, HALF, HALF), F32),
            in_specs=[anywhere] * (len(operands) + SMALL),
            out_specs=vmem,
            scratch_shapes=scratch,
            compiler_params=pltpu.CompilerParams(collective_id=0, has_side_effects=True, vmem_limit_bytes=67043328),
        )(*operands, *small)
        return jnp.transpose(out, (1, 2, 0)) + b_head

    def program(image, *params):
        mapped = jax.shard_map(device_body, mesh=mesh, in_specs=(tile_spec,) + tuple([P()] * len(params)), out_specs=tile_spec, check_vma=False)
        return mapped(image, *params)

    return program
```

```python
import functools

import jax
import jax.numpy as jnp
from jax import lax
from jax.experimental import pallas as pl
from jax.experimental.pallas import tpu as pltpu
from jax.sharding import PartitionSpec as P

MESH = pl.DeviceIdType.MESH
F32 = jnp.float32
BF16 = jnp.bfloat16
ROWS = 18
SIDE = 16
PIX = SIDE * SIDE
EXT = ROWS * SIDE
C1 = 192
C1P = 256
C2 = 384
C3 = 768
HALF = 64
LANE = 128
PATCH = 192
TAPROWS = 40
BY_ROWS = (((1,), (1,)), ((), ()))
POOL1, ENC2A, POOL2, MIDA, UP2, DEC2A, CAT1, DEC1A, IMAGE, SKIP2, SKIP1 = range(11)
EXCHANGE = ((2, C1P), (2, C2), (1, C2), (1, C3), (2, C2), (2, C2), (4, C1P), (4, C1P), (1, LANE), (2, C2), (4, C1P))
MESSAGES = 5
LOADS = 19
SMALL = 13


def iota(shape, dim):
    return lax.broadcasted_iota(jnp.int32, shape, dim)


def grid_iota(*shape):
    return iota(shape, 0), iota(shape, 1)


def ones_at(mask):
    return mask.astype(F32).astype(BF16)


def dot(lhs, rhs):
    return jnp.dot(lhs, rhs, preferred_element_type=F32)


def dot_rows(lhs, rhs):
    return lax.dot_general(lhs, rhs, BY_ROWS, preferred_element_type=F32)


def biased_relu(acc, bias):
    return jnp.maximum(acc + bias[...].reshape(1, bias.shape[-1]), 0.0).astype(BF16)


def kernel(row_count, we1b, we2a, we2b, wma, wmb, wu2, wd2a, wd2b, wu1, wd1a, wd1b, *scratch):
    small, y, scratch = scratch[:SMALL], scratch[SMALL], scratch[SMALL + 1:]
    near_small, scratch = scratch[:SMALL], scratch[SMALL:]
    x, we1a, wh, be1a, be1b, be2a, be2b, bma, bmb, bd2a, bd2b, bd1a, bd1b = near_small
    small_sem, scratch = scratch[-1], scratch[:-1]
    small_copies = [pltpu.make_async_copy(src, dst, small_sem.at[k]) for k, (src, dst) in enumerate(zip(small, near_small))]
    for copy in small_copies:
        copy.start()
    (vw8, re1b, ve1b, ve2a, ve2b, vma, vmb, vu2, vd2a, vu1, vd1a, vd1b,
     h1, cat1, d1a, p1, e2a, cat2, d2, p2, ma, mid, x1, x8, wf, bpad, weave, part, heads) = scratch[:-2 * len(EXCHANGE) - 3]
    send_cols = scratch[-2 * len(EXCHANGE) - 3:-len(EXCHANGE) - 3]
    recv_cols = scratch[-len(EXCHANGE) - 3:-3]
    w_sem, send_sem, recv_sem = scratch[-3:]
    row, col, data = lax.axis_index("row"), lax.axis_index("col"), lax.axis_index("data")
    last = row_count - 1
    has_up, has_down = row > 0, row < last
    up, down = (data, col, row - 1), (data, col, row + 1)
    side, side_up, side_down = (data, 1 - col, row), (data, 1 - col, row - 1), (data, 1 - col, row + 1)
    edge = (1 - col) * (SIDE - 1)

    barrier = pltpu.get_barrier_semaphore()

    def arrive(device):
        pl.semaphore_signal(barrier, inc=1, device_id=device, device_id_type=MESH)

    arrive(side)

    @pl.when(has_up)
    def _():
        arrive(up)
        arrive(side_up)

    @pl.when(has_down)
    def _():
        arrive(down)
        arrive(side_down)

    loads = [(we1b, re1b), (we2a, ve2a.at[:, :, HALF:, :]), (we2b, ve2b), (wma, vma), (wmb, vmb),
             (wu2, vu2), (wd2a, vd2a), (wu1, vu1)]
    loads += [(wd1a.at[t // 3, t % 3], vd1a.at[:C1, pl.ds(t * C2, C2)]) for t in range(9)]
    loads += [(wd1b, vd1b.at[:, :, :C1, :]), (wd2b, ve2b)]
    copies = [pltpu.make_async_copy(src, dst, w_sem.at[k]) for k, (src, dst) in enumerate(loads)]
    for copy in copies[:3]:
        copy.start()
    for copy in copies[3:-1]:
        copy.start()

    def messages(index, buf, lane):
        factor, width = EXCHANGE[index]
        cols, got = send_cols[index], recv_cols[index]
        own = pl.ds(1, factor)
        lanes = pl.ds(lane, width)

        def remote(k, src, dst, device):
            return pltpu.make_async_remote_copy(
                src_ref=src, dst_ref=dst, send_sem=send_sem.at[index, k], recv_sem=recv_sem.at[index, k],
                device_id=device, device_id_type=MESH)

        routes = (
            (cols, got.at[pl.ds(0, factor)], side),
            (buf.at[0, own, 1, :, lanes], buf.at[0, own, ROWS - 1, :, lanes], up),
            (buf.at[factor - 1, own, ROWS - 2, :, lanes], buf.at[factor - 1, own, 0, :, lanes], down),
            (cols.at[0], got.at[factor + 1], side_up),
            (cols.at[factor - 1], got.at[factor], side_down),
        )
        return [remote(k, *route) for k, route in enumerate(routes)]

    def shift(value, right):
        value = value.astype(F32)
        count = value.shape[0]
        at = lax.rem(iota(value.shape, 0), SIDE)
        if right:
            return jnp.where(at == SIDE - 1, 0.0, pltpu.roll(value, count - 1, 0))
        return jnp.where(at == 0, 0.0, pltpu.roll(value, 1, 0))

    def start(index, buf, lane=0):
        factor, width = EXCHANGE[index]
        lanes = pl.ds(lane, width)
        to_side, to_up, to_down, to_side_up, to_side_down = messages(index, buf, lane)
        if index == IMAGE:
            pl.semaphore_wait(barrier, 2 * has_up.astype(jnp.int32) + 2 * has_down.astype(jnp.int32) + 1)

        @pl.when(has_up)
        def _():
            to_up.start()

        @pl.when(has_down)
        def _():
            to_down.start()

        pick_row, pick_at = grid_iota(SIDE, PIX)
        pick = ones_at(pick_at == pick_row * SIDE + edge)
        cols = send_cols[index]
        for a in range(factor):
            plane = buf[a, 1 + (factor - 1) * (1 - col), 1:ROWS - 1, :, lanes].reshape(PIX, width)
            cols[a] = dot(pick, plane).astype(BF16)
        to_side.start()

        @pl.when(has_up)
        def _():
            to_side_up.start()

        @pl.when(has_down)
        def _():
            to_side_down.start()

        def shifted(a):
            for source, target in ((factor, 0), (1, factor + 1)):
                value = shift(buf[a, source, 1:ROWS - 1, :, lanes].reshape(PIX, width), target > 0)
                buf[a, target, 1:ROWS - 1, :, lanes] = value.astype(BF16).reshape(SIDE, SIDE, width)

        if factor == 1:
            shifted(0)
        else:
            pl.loop(0, factor)(shifted)

    def finish(index, buf, lane=0):
        factor, width = EXCHANGE[index]
        lanes = pl.ds(lane, width)
        got = recv_cols[index]
        to_side, to_up, to_down, to_side_up, to_side_down = messages(index, buf, lane)
        to_side.wait()

        @pl.when(has_up)
        def _():
            to_up.wait_send()
            to_side_up.wait_send()
            to_down.wait_recv()
            to_side_down.wait_recv()

        @pl.when(has_down)
        def _():
            to_down.wait_send()
            to_side_down.wait_send()
            to_up.wait_recv()
            to_side_up.wait_recv()

        at, source = grid_iota(EXT, 3 * SIDE)
        place = ones_at((lax.rem(at, SIDE) == edge) & (at // SIDE + SIDE - 1 == source))
        fix = (factor + 1) * (1 - col)
        for a in range(factor):
            put = dot(place, jnp.concatenate([got[factor], got[a], got[factor + 1]], axis=0))
            plane = buf[a, fix, 1:ROWS - 1, :, lanes].reshape(PIX, width).astype(F32) + put[SIDE:EXT - SIDE]
            buf[a, fix, 1:ROWS - 1, :, lanes] = plane.astype(BF16).reshape(SIDE, SIDE, width)
            ends = ([(0, put[:SIDE])] if a == factor - 1 else []) + ([(ROWS - 1, put[EXT - SIDE:])] if a == 0 else [])
            for line, corner in ends:
                left = shift(buf[a, factor, line, :, lanes], False) + jnp.where(col == 1, corner, 0.0)
                right = shift(buf[a, 1, line, :, lanes], True) + jnp.where(col == 0, corner, 0.0)
                buf[a, 0, line, :, lanes] = left.astype(BF16)
                buf[a, factor + 1, line, :, lanes] = right.astype(BF16)

    ALL = [(dy, dx) for dy in range(3) for dx in range(3)]

    def gather(buf, factor, planes):
        rows = []
        for a, b in planes:
            parts = []
            for dy, dx in ALL:
                shifted = a + (dy - 1 + factor)
                piece = buf[lax.rem(shifted, factor), b + dx, pl.ds(shifted // factor, SIDE)]
                parts.append(piece.reshape(PIX, piece.shape[-1]))
            rows.append(jnp.concatenate(parts, axis=1))
        return jnp.concatenate(rows, axis=0)

    def conv(buf, factor, planes, weight):
        return dot(gather(buf, factor, planes), weight[...].reshape(9 * buf.shape[-1], weight.shape[-1]))

    def put_planes(buf, planes, value, lane=0):
        width = value.shape[-1]
        for k, (a, b) in enumerate(planes):
            plane = value[k * PIX:(k + 1) * PIX].reshape(SIDE, SIDE, width)
            buf[a, b + 1, 1:ROWS - 1, :, lane:lane + width] = plane

    def row_of(a):
        return [(a, b) for b in range(4)]

    def pool(src, dst, factor, lane, width):
        for a in range(factor):
            for b in range(factor):
                quad = [src[2 * a + p, 2 * b + q + 1, 1:ROWS - 1, :, lane:lane + width] for p in range(2) for q in range(2)]
                dst[a, b + 1, 1:ROWS - 1] = functools.reduce(jnp.maximum, quad)

    LEVEL2 = [(a, b) for a in range(2) for b in range(2)]

    def plane_of(buf, a, b, line, lane, width):
        return buf[a, b, pl.ds(line, SIDE), :, pl.ds(lane, width)].reshape(PIX, width)

    def near(a, buf, weight, lane, width):
        lhs = [plane_of(buf, k, l + 1, 1, lane, width) for k, l in LEVEL2]
        both = [jnp.concatenate([weight[k - a + 1, l - b + 1, lane:lane + width] for k, l in LEVEL2], axis=0) for b in range(2)]
        out = dot(jnp.concatenate(lhs, axis=1), jnp.concatenate(both, axis=1))
        return out[:, :C2], out[:, C2:]

    def sides(a, b, buf, weight, lane, width):
        lhs = [plane_of(buf, k, 3 * b, 1, lane, width) for k in range(2)]
        rhs = [weight[k - a + 1, 2 * b, lane:lane + width] for k in range(2)]
        return dot(jnp.concatenate(lhs, axis=1), jnp.concatenate(rhs, axis=0))

    def far_rows(a, b, buf, weight, lane, width):
        lhs = [plane_of(buf, 1 - a, b + dx, 2 * a, lane, width) for dx in range(3)]
        rhs = [weight[2 * a, dx, lane:lane + width] for dx in range(3)]
        return dot(jnp.concatenate(lhs, axis=1), jnp.concatenate(rhs, axis=0))

    def near_sums(again, *operands):
        @pl.loop(0, 2)
        def _(a):
            for b, value in enumerate(near(a, *operands)):
                part[2 * a + b] = part[2 * a + b] + value if again else value
            part[2 * a + col] += sides(a, col, *operands)

    def far_sums(put, *operands):
        for a in range(2):
            part[2 * a + 1 - col] += sides(a, 1 - col, *operands)
            for b in range(2):
                put(a, b, far_rows(a, b, *operands))

    def add(a, b, value):
        part[2 * a + b] += value

    def done(bias, put):
        return lambda a, b, value: put(a, b, biased_relu(part[2 * a + b] + value, bias))

    def conv_level2(index, src, weight, bias, put, first=None, then=None):
        width = src.shape[-1]
        start(index, src)
        if first is not None:
            first()
        near_sums(False, src, weight, 0, width)
        if then is not None:
            then()
        finish(index, src)
        far_sums(done(bias, put), src, weight, 0, width)

    at, to = grid_iota(HALF, HALF)
    split_cols = ones_at(at == lax.rem(to, SIDE) * 4 + to // SIDE)
    at, to = grid_iota(PIX, HALF)
    own_col = lax.rem(at, SIDE) == lax.rem(to, SIDE)
    fold_at, fold_to = grid_iota(HALF, LANE)
    small_copies[0].wait()
    image = []
    for ch in range(3):
        cols = dot(x[ch], split_cols).astype(BF16)
        for a in range(4):
            spread = ones_at(to == (at // SIDE) * 4 + a)
            lines = jnp.where(own_col, dot(spread, cols), 0.0).astype(BF16)
            image.append(dot(lines, ones_at(fold_to == fold_at // SIDE + (ch * SIDE + a * 4))))
    x1[0, 1, 1:ROWS - 1] = sum(image[1:], image[0]).astype(BF16).reshape(SIDE, SIDE, LANE)
    start(IMAGE, x1)

    mapped = ((cat1, 4), (d1a, 4), (p1, 2), (e2a, 2), (cat2, 2), (p2, 1), (ma, 1), (x1, 1))

    @pl.when(row == 0)
    def _():
        for buf, factor in mapped:
            buf[factor - 1, :, 0] = jnp.zeros(buf.shape[1:2] + buf.shape[3:], BF16)
        for buf, (factor, _) in zip(recv_cols, EXCHANGE):
            buf[factor] = jnp.zeros(buf.shape[1:], BF16)

    @pl.when(row == last)
    def _():
        for buf, factor in mapped:
            buf[0, :, ROWS - 1] = jnp.zeros(buf.shape[1:2] + buf.shape[3:], BF16)
        for buf, (factor, _) in zip(recv_cols, EXCHANGE):
            buf[factor + 1] = jnp.zeros(buf.shape[1:], BF16)


    for copy in small_copies[1:]:
        copy.wait()

    wf[...] = jnp.zeros(wf.shape, F32)
    for t in range(9):
        wf[pl.ds(4 * t, 3), :C1] = we1a[t // 3, t % 3].astype(F32)
    k, m = grid_iota(PATCH, TAPROWS)
    py, px = k // 32, lax.rem(k, 32) // 4
    base = py * 12 + px * 4 + lax.rem(k, 4)

    @pl.loop(0, 4)
    def _(a):
        for b in range(6):
            good = (py >= a) & (py <= a + 2) & (px >= b) & (px <= b + 2)
            place = ones_at(good & (m == base - a * 12 - b * 4))
            vw8[a * 6 + b] = dot(place, wf[...].astype(BF16)).astype(BF16)

    pad = jnp.zeros((1, HALF), F32)
    bpad[0:1, :C1P] = jnp.concatenate([be1a[...].reshape(1, C1), pad], axis=1)
    bpad[1:2, :C1P] = jnp.concatenate([pad, be1b[...].reshape(1, C1)], axis=1)
    bpad[2:3, :C1P] = jnp.concatenate([bd1a[...].reshape(1, C1), pad], axis=1)
    bpad[3:4, :] = bma[...].reshape(1, C3)
    bpad[4:5, :] = bmb[...].reshape(1, C3)
    copies[0].wait()

    @pl.loop(0, 3)
    def _(dy):
        for dx in range(3):
            value = jnp.concatenate([jnp.zeros((C1, HALF), F32), re1b[dy, dx].astype(F32)], axis=1)
            ve1b[dy, dx, :C1] = value.astype(BF16)
            ve1b[dy, dx, C1:] = jnp.zeros((HALF, C1P), BF16)

    finish(IMAGE, x1)

    blank = jnp.zeros((SIDE, LANE), BF16)
    lane, k = grid_iota(LANE, PATCH)
    ch, a, b = lane // SIDE, lax.rem(lane, SIDE) // 4, lax.rem(lane, 4)
    patches = []
    for dx in range(3):
        plane = x1[0, dx].reshape(EXT, LANE)
        blocks = (jnp.concatenate([blank, plane[:-SIDE]], axis=0), plane, jnp.concatenate([plane[SIDE:], blank], axis=0))
        for dy, block in enumerate(blocks):
            py, px = a + (4 * dy - 3), b + (4 * dx - 2)
            good = (ch < 3) & (py >= 0) & (py < 6) & (px >= 0) & (px < 8)
            patches.append(dot(block, ones_at(good & (k == py * 32 + px * 4 + ch))))
    x8[...] = sum(patches[1:], patches[0]).astype(BF16)

    pos = iota((EXT, C1P), 0)
    pos_col = lax.rem(pos, SIDE)
    off = {0: (pos_col == 0) & (col == 0), 5: (pos_col == SIDE - 1) & (col == 1)}

    @pl.loop(0, 2)
    def _(t):
        for a, b in [(2 * t + k, b) for k in range(2) for b in range(6)]:
            out = jnp.maximum(dot(x8[...], vw8[a * 6 + b]) + bpad[0:1, :C1P], 0.0)
            if b in off:
                out = jnp.where(off[b], 0.0, out)
            h1[a, b] = out.astype(BF16).reshape(ROWS, SIDE, C1P)

    @pl.when(row == 0)
    def _():
        h1[3, :, 0] = jnp.zeros((6, SIDE, C1P), BF16)

    @pl.when(row == last)
    def _():
        h1[0, :, ROWS - 1] = jnp.zeros((6, SIDE, C1P), BF16)

    @pl.loop(0, 2)
    def _(t):
        for a in (2 * t, 2 * t + 1):
            put_planes(cat1, row_of(a), biased_relu(conv(h1, 4, row_of(a), ve1b), bpad.at[1:2, :C1P]), LANE)

    pool(cat1, p1, 2, LANE, C1P)

    ve2a[:, :, :HALF, :] = jnp.zeros((3, 3, HALF, C2), BF16)

    def fill_constants():
        start(SKIP1, cat1, LANE)
        n, m = grid_iota(2 * PIX, 2 * PIX)
        weave[...] = ones_at(m == lax.rem(n, 4) * LANE + (n // HALF) * SIDE + lax.rem(n, HALF) // 4)
        vd1b[:, :, C1:, :] = jnp.zeros((3, 3, HALF, C1), BF16)
        vd1a[C1:, :] = jnp.zeros((HALF, vd1a.shape[1]), BF16)
        heads[...] = jnp.zeros(heads.shape, F32)

    copies[1].wait()
    conv_level2(POOL1, p1, ve2a, be2a, lambda a, b, value: put_planes(e2a, [(a, b)], value), first=fill_constants)
    copies[2].wait()
    conv_level2(ENC2A, e2a, ve2b, be2b, lambda a, b, value: put_planes(cat2, [(a, b)], value, C2),
                then=lambda: finish(SKIP1, cat1, LANE))
    copies[-1].start()
    pool(cat2, p2, 1, C2, C2)

    start(POOL2, p2)
    start(SKIP2, cat2, C2)
    copies[6].wait()
    near_sums(False, cat2, vd2a, C2, C2)
    copies[3].wait()
    finish(POOL2, p2)

    def conv_level3(src, weight, bias, put):
        @pl.loop(0, 3)
        def _(n):
            lanes = pl.ds(pl.multiple_of(n * PIX, PIX), PIX)
            flat = weight[:, :, :, lanes].reshape(9 * src.shape[-1], PIX)
            put(lanes, biased_relu(dot(gather(src, 1, [(0, 0)]), flat), bpad.at[bias:bias + 1, lanes]))

    def put_ma(lanes, value):
        ma[0, 1, 1:ROWS - 1, :, lanes] = value.reshape(SIDE, SIDE, PIX)

    def put_mid(lanes, value):
        mid[:, lanes] = value

    conv_level3(p2, vma, 3, put_ma)
    start(MIDA, ma)
    finish(SKIP2, cat2, C2)
    far_sums(add, cat2, vd2a, C2, C2)
    copies[4].wait()
    finish(MIDA, ma)
    conv_level3(ma, vmb, 4, put_mid)
    copies[5].wait()
    for p in range(2):
        out = dot(mid[...], jnp.concatenate([vu2[p, 0], vu2[p, 1]], axis=1)).astype(BF16)
        for q in range(2):
            put_planes(cat2, [(p, q)], out[:, q * C2:(q + 1) * C2])
    start(UP2, cat2)
    near_sums(True, cat2, vd2a, 0, C2)
    finish(UP2, cat2)
    far_sums(done(bd2a, lambda a, b, value: put_planes(e2a, [(a, b)], value)), cat2, vd2a, 0, C2)
    copies[-1].wait()

    def put_d2(a, b, value):
        d2[pl.ds((2 * a + b) * PIX, PIX)] = value

    conv_level2(DEC2A, e2a, ve2b, bd2b, put_d2)
    copies[7].wait()

    @pl.loop(0, 2)
    def _(t):
        lhs = d2[pl.ds(2 * t * PIX, 2 * PIX)]
        for p, q in LEVEL2:
            put_planes(cat1, [(2 * t + p, q), (2 * t + p, q + 2)], dot_rows(lhs, vu1[p, q]).astype(BF16))

    for copy in copies[8:17]:
        copy.wait()

    border = 3 * col

    def dec1a(planes):
        put_planes(d1a, planes, biased_relu(dot_rows(gather(cat1, 4, planes), vd1a[...]), bpad.at[2:3, :C1P]))

    inner = (1, 2)
    fixed = [(a, 3 - border) for a in inner]
    start(CAT1, cat1)
    dec1a([(1, b) for b in inner])
    dec1a([(a, border) for a in inner])
    finish(CAT1, cat1)
    dec1a(fixed)
    for a in (0, 3):
        dec1a(row_of(a))
    start(DEC1A, d1a)
    dec1a([(2, b) for b in inner])
    copies[17].wait()

    def head(a):
        lines = [h1[a, b + 1, pl.ds(8 * h + 1, 8), :, :C1].reshape(LANE, C1) for h in range(2) for b in range(4)]
        heads[a, :6] = dot_rows(wh[...], jnp.concatenate(lines, axis=0))

    def dec1b(planes):
        put_planes(h1, planes, biased_relu(conv(d1a, 4, planes, vd1b), bd1b))

    for a in inner:
        dec1b([(a, b) for b in (*inner, border)])
    finish(DEC1A, d1a)
    dec1b(fixed)
    for a in (0, 3):
        dec1b(row_of(a))
    for a in range(4):
        head(a)
    wide = 2 * PIX
    flat = jnp.concatenate([heads[a, :, h * wide:(h + 1) * wide] for a in range(4) for h in range(2)], axis=0)
    high = flat.astype(BF16)
    rest = flat - high.astype(F32)
    middle = rest.astype(BF16)
    low = (rest - middle.astype(F32)).astype(BF16)
    woven = dot_rows(high, weave[...]) + dot_rows(middle, weave[...]) + dot_rows(low, weave[...])
    for a in range(4):
        for h in range(2):
            for i in range(8):
                y[:, 4 * (8 * h + i) + a, :] = woven[(2 * a + h) * 8:(2 * a + h) * 8 + 6, i * HALF:(i + 1) * HALF]


def solution(mesh):
    tile_spec = P(("data", "row"), "col", None)

    def device_body(image_tile, *params):
        (w_enc1a, b_enc1a, w_enc1b, b_enc1b, w_enc2a, b_enc2a, w_enc2b, b_enc2b,
         w_mid_a, b_mid_a, w_mid_b, b_mid_b, w_up2, w_dec2a, b_dec2a, w_dec2b, b_dec2b,
         w_up1, w_dec1a, b_dec1a, w_dec1b, b_dec1b, w_head, b_head) = params
        anywhere = pl.BlockSpec(memory_space=pl.ANY)
        vmem = pl.BlockSpec(memory_space=pltpu.VMEM)
        small = [
            jnp.transpose(image_tile, (2, 0, 1)), w_enc1a, w_head.T, b_enc1a, b_enc1b, b_enc2a, b_enc2b,
            b_mid_a, b_mid_b, b_dec2a, b_dec2b, b_dec1a, b_dec1b,
        ]
        operands = [
            w_enc1b, w_enc2a, w_enc2b, w_mid_a, w_mid_b, w_up2, w_dec2a, w_dec2b,
            jnp.swapaxes(w_up1, 2, 3), jnp.swapaxes(w_dec1a, 2, 3), w_dec1b,
        ]

        def kept(*shape, dtype=BF16):
            return pltpu.VMEM(shape, dtype)

        def level(factor, lanes):
            return kept(factor, factor + 2, ROWS, SIDE, lanes)

        scratch = [
            kept(24, PATCH, C1P), kept(3, 3, C1, C1), kept(3, 3, C1P, C1P), kept(3, 3, C1P, C2), kept(3, 3, C2, C2),
            kept(3, 3, C2, C3), kept(3, 3, C3, C3), kept(2, 2, C3, C2), kept(3, 3, C3, C2),
            kept(2, 2, C1, C2), kept(C1P, 9 * C2), kept(3, 3, C1P, C1),
            level(4, C1P), level(4, C2), level(4, C1P), level(2, C1P), level(2, C2), level(2, C3),
            kept(4 * PIX, C2), level(1, C2), level(1, C3), kept(PIX, C3), level(1, LANE), kept(EXT, PATCH),
            kept(TAPROWS, C1P, dtype=F32), kept(5, C3, dtype=F32), kept(2 * PIX, 2 * PIX),
            kept(4, PIX, C2, dtype=F32), kept(4, 8, 4 * PIX, dtype=F32),
        ]
        scratch += [kept(factor, SIDE, width) for factor, width in EXCHANGE]
        scratch += [kept(factor + 2, SIDE, width) for factor, width in EXCHANGE]
        links = pltpu.SemaphoreType.DMA((len(EXCHANGE), MESSAGES))
        scratch += [pltpu.SemaphoreType.DMA((LOADS,)), links, links, pltpu.SemaphoreType.DMA((SMALL,))]
        scratch = [kept(*array.shape, dtype=array.dtype) for array in small] + scratch
        out = pl.pallas_call(
            functools.partial(kernel, mesh.shape["row"]),
            name="unet",
            out_shape=jax.ShapeDtypeStruct((6, HALF, HALF), F32),
            in_specs=[anywhere] * (len(operands) + SMALL),
            out_specs=vmem,
            scratch_shapes=scratch,
            compiler_params=pltpu.CompilerParams(collective_id=0, has_side_effects=True, vmem_limit_bytes=67043328),
        )(*operands, *small)
        return jnp.transpose(out, (1, 2, 0)) + b_head

    def program(image, *params):
        mapped = jax.shard_map(device_body, mesh=mesh, in_specs=(tile_spec,) + tuple([P()] * len(params)), out_specs=tile_spec, check_vma=False)
        return mapped(image, *params)

    return program
```

```python
import functools

import jax
import jax.numpy as jnp
from jax import lax
from jax.experimental import pallas as pl
from jax.experimental.pallas import tpu as pltpu
from jax.sharding import PartitionSpec as P

MESH = pl.DeviceIdType.MESH
F32 = jnp.float32
BF16 = jnp.bfloat16
ROWS = 18
SIDE = 16
PIX = SIDE * SIDE
EXT = ROWS * SIDE
C1 = 192
C1P = 256
C2 = 384
C3 = 768
HALF = 64
LANE = 128
PATCH = 192
TAPROWS = 40
BY_ROWS = (((1,), (1,)), ((), ()))
POOL1, ENC2A, POOL2, MIDA, UP2, DEC2A, CAT1, DEC1A, IMAGE, SKIP2, SKIP1 = range(11)
EXCHANGE = ((2, C1P), (2, C2), (1, C2), (1, C3), (2, C2), (2, C2), (4, C1P), (4, C1P), (1, LANE), (2, C2), (4, C1P))
MESSAGES = 5
LOADS = 19
SMALL = 13


def iota(shape, dim):
    return lax.broadcasted_iota(jnp.int32, shape, dim)


def grid_iota(*shape):
    return iota(shape, 0), iota(shape, 1)


def ones_at(mask):
    return mask.astype(F32).astype(BF16)


def dot(lhs, rhs):
    return jnp.dot(lhs, rhs, preferred_element_type=F32)


def dot_rows(lhs, rhs):
    return lax.dot_general(lhs, rhs, BY_ROWS, preferred_element_type=F32)


def biased_relu(acc, bias):
    return jnp.maximum(acc + bias[...].reshape(1, bias.shape[-1]), 0.0).astype(BF16)


def kernel(row_count, we1b, we2a, we2b, wma, wmb, wu2, wd2a, wd2b, wu1, wd1a, wd1b, *scratch):
    small, y, scratch = scratch[:SMALL], scratch[SMALL], scratch[SMALL + 1:]
    near_small, scratch = scratch[:SMALL], scratch[SMALL:]
    x, we1a, wh, be1a, be1b, be2a, be2b, bma, bmb, bd2a, bd2b, bd1a, bd1b = near_small
    small_sem, scratch = scratch[-1], scratch[:-1]
    small_copies = [pltpu.make_async_copy(src, dst, small_sem.at[k]) for k, (src, dst) in enumerate(zip(small, near_small))]
    for copy in small_copies:
        copy.start()
    (vw8, re1b, ve1b, ve2a, ve2b, vma, vmb, vu2, vd2a, vu1, vd1a, vd1b,
     h1, cat1, d1a, p1, e2a, cat2, d2, p2, ma, mid, x1, x8, wf, bpad, weave, part, heads) = scratch[:-2 * len(EXCHANGE) - 3]
    send_cols = scratch[-2 * len(EXCHANGE) - 3:-len(EXCHANGE) - 3]
    recv_cols = scratch[-len(EXCHANGE) - 3:-3]
    w_sem, send_sem, recv_sem = scratch[-3:]
    row, col, data = lax.axis_index("row"), lax.axis_index("col"), lax.axis_index("data")
    last = row_count - 1
    has_up, has_down = row > 0, row < last
    up, down = (data, col, row - 1), (data, col, row + 1)
    side, side_up, side_down = (data, 1 - col, row), (data, 1 - col, row - 1), (data, 1 - col, row + 1)
    edge = (1 - col) * (SIDE - 1)

    barrier = pltpu.get_barrier_semaphore()

    def arrive(device):
        pl.semaphore_signal(barrier, inc=1, device_id=device, device_id_type=MESH)

    arrive(side)

    @pl.when(has_up)
    def _():
        arrive(up)
        arrive(side_up)

    @pl.when(has_down)
    def _():
        arrive(down)
        arrive(side_down)

    loads = [(we1b, re1b), (we2a, ve2a.at[:, :, HALF:, :]), (we2b, ve2b), (wma, vma), (wmb, vmb),
             (wu2, vu2), (wd2a, vd2a), (wu1, vu1)]
    loads += [(wd1a.at[t // 3, t % 3], vd1a.at[:C1, pl.ds(t * C2, C2)]) for t in range(9)]
    loads += [(wd1b, vd1b.at[:, :, :C1, :]), (wd2b, ve2b)]
    copies = [pltpu.make_async_copy(src, dst, w_sem.at[k]) for k, (src, dst) in enumerate(loads)]
    for copy in copies[:3]:
        copy.start()
    for copy in copies[3:-1]:
        copy.start()

    def messages(index, buf, lane):
        factor, width = EXCHANGE[index]
        cols, got = send_cols[index], recv_cols[index]
        own = pl.ds(1, factor)
        lanes = pl.ds(lane, width)

        def remote(k, src, dst, device):
            return pltpu.make_async_remote_copy(
                src_ref=src, dst_ref=dst, send_sem=send_sem.at[index, k], recv_sem=recv_sem.at[index, k],
                device_id=device, device_id_type=MESH)

        routes = (
            (cols, got.at[pl.ds(0, factor)], side),
            (buf.at[0, own, 1, :, lanes], buf.at[0, own, ROWS - 1, :, lanes], up),
            (buf.at[factor - 1, own, ROWS - 2, :, lanes], buf.at[factor - 1, own, 0, :, lanes], down),
            (cols.at[0], got.at[factor + 1], side_up),
            (cols.at[factor - 1], got.at[factor], side_down),
        )
        return [remote(k, *route) for k, route in enumerate(routes)]

    def shift(value, right):
        value = value.astype(F32)
        count = value.shape[0]
        at = lax.rem(iota(value.shape, 0), SIDE)
        if right:
            return jnp.where(at == SIDE - 1, 0.0, pltpu.roll(value, count - 1, 0))
        return jnp.where(at == 0, 0.0, pltpu.roll(value, 1, 0))

    def start(index, buf, lane=0):
        factor, width = EXCHANGE[index]
        lanes = pl.ds(lane, width)
        to_side, to_up, to_down, to_side_up, to_side_down = messages(index, buf, lane)
        if index == IMAGE:
            pl.semaphore_wait(barrier, 2 * has_up.astype(jnp.int32) + 2 * has_down.astype(jnp.int32) + 1)

        @pl.when(has_up)
        def _():
            to_up.start()

        @pl.when(has_down)
        def _():
            to_down.start()

        pick_row, pick_at = grid_iota(SIDE, PIX)
        pick = ones_at(pick_at == pick_row * SIDE + edge)
        cols = send_cols[index]
        for a in range(factor):
            plane = buf[a, 1 + (factor - 1) * (1 - col), 1:ROWS - 1, :, lanes].reshape(PIX, width)
            cols[a] = dot(pick, plane).astype(BF16)
        to_side.start()

        @pl.when(has_up)
        def _():
            to_side_up.start()

        @pl.when(has_down)
        def _():
            to_side_down.start()

        def shifted(a):
            for source, target in ((factor, 0), (1, factor + 1)):
                value = shift(buf[a, source, 1:ROWS - 1, :, lanes].reshape(PIX, width), target > 0)
                buf[a, target, 1:ROWS - 1, :, lanes] = value.astype(BF16).reshape(SIDE, SIDE, width)

        if factor == 1:
            shifted(0)
        else:
            pl.loop(0, factor)(shifted)

    def finish(index, buf, lane=0):
        factor, width = EXCHANGE[index]
        lanes = pl.ds(lane, width)
        got = recv_cols[index]
        to_side, to_up, to_down, to_side_up, to_side_down = messages(index, buf, lane)
        to_side.wait()

        @pl.when(has_up)
        def _():
            to_up.wait_send()
            to_side_up.wait_send()
            to_down.wait_recv()
            to_side_down.wait_recv()

        @pl.when(has_down)
        def _():
            to_down.wait_send()
            to_side_down.wait_send()
            to_up.wait_recv()
            to_side_up.wait_recv()

        at, source = grid_iota(EXT, 3 * SIDE)
        place = ones_at((lax.rem(at, SIDE) == edge) & (at // SIDE + SIDE - 1 == source))
        fix = (factor + 1) * (1 - col)
        for a in range(factor):
            put = dot(place, jnp.concatenate([got[factor], got[a], got[factor + 1]], axis=0))
            plane = buf[a, fix, 1:ROWS - 1, :, lanes].reshape(PIX, width).astype(F32) + put[SIDE:EXT - SIDE]
            buf[a, fix, 1:ROWS - 1, :, lanes] = plane.astype(BF16).reshape(SIDE, SIDE, width)
            ends = ([(0, put[:SIDE])] if a == factor - 1 else []) + ([(ROWS - 1, put[EXT - SIDE:])] if a == 0 else [])
            for line, corner in ends:
                left = shift(buf[a, factor, line, :, lanes], False) + jnp.where(col == 1, corner, 0.0)
                right = shift(buf[a, 1, line, :, lanes], True) + jnp.where(col == 0, corner, 0.0)
                buf[a, 0, line, :, lanes] = left.astype(BF16)
                buf[a, factor + 1, line, :, lanes] = right.astype(BF16)

    ALL = [(dy, dx) for dy in range(3) for dx in range(3)]

    def gather(buf, factor, planes):
        rows = []
        for a, b in planes:
            parts = []
            for dy, dx in ALL:
                shifted = a + (dy - 1 + factor)
                piece = buf[lax.rem(shifted, factor), b + dx, pl.ds(shifted // factor, SIDE)]
                parts.append(piece.reshape(PIX, piece.shape[-1]))
            rows.append(jnp.concatenate(parts, axis=1))
        return jnp.concatenate(rows, axis=0)

    def conv(buf, factor, planes, weight):
        return dot(gather(buf, factor, planes), weight[...].reshape(9 * buf.shape[-1], weight.shape[-1]))

    def put_planes(buf, planes, value, lane=0):
        width = value.shape[-1]
        for k, (a, b) in enumerate(planes):
            plane = value[k * PIX:(k + 1) * PIX].reshape(SIDE, SIDE, width)
            buf[a, b + 1, 1:ROWS - 1, :, lane:lane + width] = plane

    def row_of(a):
        return [(a, b) for b in range(4)]

    def pool(src, dst, factor, lane, width):
        for a in range(factor):
            for b in range(factor):
                quad = [src[2 * a + p, 2 * b + q + 1, 1:ROWS - 1, :, lane:lane + width] for p in range(2) for q in range(2)]
                dst[a, b + 1, 1:ROWS - 1] = functools.reduce(jnp.maximum, quad)

    LEVEL2 = [(a, b) for a in range(2) for b in range(2)]

    def plane_of(buf, a, b, line, lane, width):
        return buf[a, b, pl.ds(line, SIDE), :, pl.ds(lane, width)].reshape(PIX, width)

    def near(a, buf, weight, lane, width):
        lhs = [plane_of(buf, k, l + 1, 1, lane, width) for k, l in LEVEL2]
        both = [jnp.concatenate([weight[k - a + 1, l - b + 1, lane:lane + width] for k, l in LEVEL2], axis=0) for b in range(2)]
        out = dot(jnp.concatenate(lhs, axis=1), jnp.concatenate(both, axis=1))
        return out[:, :C2], out[:, C2:]

    def sides(a, b, buf, weight, lane, width):
        lhs = [plane_of(buf, k, 3 * b, 1, lane, width) for k in range(2)]
        rhs = [weight[k - a + 1, 2 * b, lane:lane + width] for k in range(2)]
        return dot(jnp.concatenate(lhs, axis=1), jnp.concatenate(rhs, axis=0))

    def far_rows(a, b, buf, weight, lane, width):
        lhs = [plane_of(buf, 1 - a, b + dx, 2 * a, lane, width) for dx in range(3)]
        rhs = [weight[2 * a, dx, lane:lane + width] for dx in range(3)]
        return dot(jnp.concatenate(lhs, axis=1), jnp.concatenate(rhs, axis=0))

    def near_sums(again, *operands):
        @pl.loop(0, 2)
        def _(a):
            for b, value in enumerate(near(a, *operands)):
                part[2 * a + b] = part[2 * a + b] + value if again else value
            part[2 * a + col] += sides(a, col, *operands)

    def far_sums(put, *operands):
        for a in range(2):
            part[2 * a + 1 - col] += sides(a, 1 - col, *operands)
            for b in range(2):
                put(a, b, far_rows(a, b, *operands))

    def add(a, b, value):
        part[2 * a + b] += value

    def done(bias, put):
        return lambda a, b, value: put(a, b, biased_relu(part[2 * a + b] + value, bias))

    def conv_level2(index, src, weight, bias, put, first=None, then=None):
        width = src.shape[-1]
        start(index, src)
        if first is not None:
            first()
        near_sums(False, src, weight, 0, width)
        if then is not None:
            then()
        finish(index, src)
        far_sums(done(bias, put), src, weight, 0, width)

    at, to = grid_iota(HALF, HALF)
    split_cols = ones_at(at == lax.rem(to, SIDE) * 4 + to // SIDE)
    at, to = grid_iota(PIX, HALF)
    own_col = lax.rem(at, SIDE) == lax.rem(to, SIDE)
    fold_at, fold_to = grid_iota(HALF, LANE)
    small_copies[0].wait()
    image = []
    for ch in range(3):
        cols = dot(x[ch], split_cols).astype(BF16)
        for a in range(4):
            spread = ones_at(to == (at // SIDE) * 4 + a)
            lines = jnp.where(own_col, dot(spread, cols), 0.0).astype(BF16)
            image.append(dot(lines, ones_at(fold_to == fold_at // SIDE + (ch * SIDE + a * 4))))
    x1[0, 1, 1:ROWS - 1] = sum(image[1:], image[0]).astype(BF16).reshape(SIDE, SIDE, LANE)
    start(IMAGE, x1)

    mapped = ((cat1, 4), (d1a, 4), (p1, 2), (e2a, 2), (cat2, 2), (p2, 1), (ma, 1), (x1, 1))

    @pl.when(row == 0)
    def _():
        for buf, factor in mapped:
            buf[factor - 1, :, 0] = jnp.zeros(buf.shape[1:2] + buf.shape[3:], BF16)
        for buf, (factor, _) in zip(recv_cols, EXCHANGE):
            buf[factor] = jnp.zeros(buf.shape[1:], BF16)

    @pl.when(row == last)
    def _():
        for buf, factor in mapped:
            buf[0, :, ROWS - 1] = jnp.zeros(buf.shape[1:2] + buf.shape[3:], BF16)
        for buf, (factor, _) in zip(recv_cols, EXCHANGE):
            buf[factor + 1] = jnp.zeros(buf.shape[1:], BF16)


    for copy in small_copies[1:]:
        copy.wait()

    wf[...] = jnp.zeros(wf.shape, F32)
    for t in range(9):
        wf[pl.ds(4 * t, 3), :C1] = we1a[t // 3, t % 3].astype(F32)
    k, m = grid_iota(PATCH, TAPROWS)
    py, px = k // 32, lax.rem(k, 32) // 4
    base = py * 12 + px * 4 + lax.rem(k, 4)

    @pl.loop(0, 4)
    def _(a):
        for b in range(6):
            good = (py >= a) & (py <= a + 2) & (px >= b) & (px <= b + 2)
            place = ones_at(good & (m == base - a * 12 - b * 4))
            vw8[a * 6 + b] = dot(place, wf[...].astype(BF16)).astype(BF16)

    pad = jnp.zeros((1, HALF), F32)
    bpad[0:1, :C1P] = jnp.concatenate([be1a[...].reshape(1, C1), pad], axis=1)
    bpad[1:2, :C1P] = jnp.concatenate([pad, be1b[...].reshape(1, C1)], axis=1)
    bpad[2:3, :C1P] = jnp.concatenate([bd1a[...].reshape(1, C1), pad], axis=1)
    bpad[3:4, :] = bma[...].reshape(1, C3)
    bpad[4:5, :] = bmb[...].reshape(1, C3)
    copies[0].wait()

    @pl.loop(0, 3)
    def _(dy):
        for dx in range(3):
            value = jnp.concatenate([jnp.zeros((C1, HALF), F32), re1b[dy, dx].astype(F32)], axis=1)
            ve1b[dy, dx, :C1] = value.astype(BF16)
            ve1b[dy, dx, C1:] = jnp.zeros((HALF, C1P), BF16)

    finish(IMAGE, x1)

    blank = jnp.zeros((SIDE, LANE), BF16)
    lane, k = grid_iota(LANE, PATCH)
    ch, a, b = lane // SIDE, lax.rem(lane, SIDE) // 4, lax.rem(lane, 4)
    patches = []
    for dx in range(3):
        plane = x1[0, dx].reshape(EXT, LANE)
        blocks = (jnp.concatenate([blank, plane[:-SIDE]], axis=0), plane, jnp.concatenate([plane[SIDE:], blank], axis=0))
        for dy, block in enumerate(blocks):
            py, px = a + (4 * dy - 3), b + (4 * dx - 2)
            good = (ch < 3) & (py >= 0) & (py < 6) & (px >= 0) & (px < 8)
            patches.append(dot(block, ones_at(good & (k == py * 32 + px * 4 + ch))))
    x8[...] = sum(patches[1:], patches[0]).astype(BF16)

    pos = iota((EXT, C1P), 0)
    pos_col = lax.rem(pos, SIDE)
    off = {0: (pos_col == 0) & (col == 0), 5: (pos_col == SIDE - 1) & (col == 1)}

    @pl.loop(0, 2)
    def _(t):
        for a, b in [(2 * t + k, b) for k in range(2) for b in range(6)]:
            out = jnp.maximum(dot(x8[...], vw8[a * 6 + b]) + bpad[0:1, :C1P], 0.0)
            if b in off:
                out = jnp.where(off[b], 0.0, out)
            h1[a, b] = out.astype(BF16).reshape(ROWS, SIDE, C1P)

    @pl.when(row == 0)
    def _():
        h1[3, :, 0] = jnp.zeros((6, SIDE, C1P), BF16)

    @pl.when(row == last)
    def _():
        h1[0, :, ROWS - 1] = jnp.zeros((6, SIDE, C1P), BF16)

    @pl.loop(0, 2)
    def _(t):
        for a in (2 * t, 2 * t + 1):
            put_planes(cat1, row_of(a), biased_relu(conv(h1, 4, row_of(a), ve1b), bpad.at[1:2, :C1P]), LANE)

    pool(cat1, p1, 2, LANE, C1P)

    ve2a[:, :, :HALF, :] = jnp.zeros((3, 3, HALF, C2), BF16)

    def fill_constants():
        start(SKIP1, cat1, LANE)
        n, m = grid_iota(2 * PIX, 2 * PIX)
        weave[...] = ones_at(m == lax.rem(n, 4) * LANE + (n // HALF) * SIDE + lax.rem(n, HALF) // 4)
        vd1b[:, :, C1:, :] = jnp.zeros((3, 3, HALF, C1), BF16)
        vd1a[C1:, :] = jnp.zeros((HALF, vd1a.shape[1]), BF16)
        heads[...] = jnp.zeros(heads.shape, F32)

    copies[1].wait()
    conv_level2(POOL1, p1, ve2a, be2a, lambda a, b, value: put_planes(e2a, [(a, b)], value), first=fill_constants)
    copies[2].wait()
    conv_level2(ENC2A, e2a, ve2b, be2b, lambda a, b, value: put_planes(cat2, [(a, b)], value, C2),
                then=lambda: finish(SKIP1, cat1, LANE))
    copies[-1].start()
    pool(cat2, p2, 1, C2, C2)

    start(POOL2, p2)
    start(SKIP2, cat2, C2)
    copies[6].wait()
    near_sums(False, cat2, vd2a, C2, C2)
    copies[3].wait()
    finish(POOL2, p2)

    def conv_level3(src, weight, bias, put):
        for n in range(3):
            lanes = pl.ds(n * PIX, PIX)
            flat = weight[:, :, :, lanes].reshape(9 * src.shape[-1], PIX)
            put(lanes, biased_relu(dot(gather(src, 1, [(0, 0)]), flat), bpad.at[bias:bias + 1, lanes]))

    def put_ma(lanes, value):
        ma[0, 1, 1:ROWS - 1, :, lanes] = value.reshape(SIDE, SIDE, PIX)

    def put_mid(lanes, value):
        mid[:, lanes] = value

    conv_level3(p2, vma, 3, put_ma)
    start(MIDA, ma)
    finish(SKIP2, cat2, C2)
    far_sums(add, cat2, vd2a, C2, C2)
    copies[4].wait()
    finish(MIDA, ma)
    conv_level3(ma, vmb, 4, put_mid)
    copies[5].wait()
    for p in range(2):
        out = dot(mid[...], jnp.concatenate([vu2[p, 0], vu2[p, 1]], axis=1)).astype(BF16)
        for q in range(2):
            put_planes(cat2, [(p, q)], out[:, q * C2:(q + 1) * C2])
    start(UP2, cat2)
    near_sums(True, cat2, vd2a, 0, C2)
    finish(UP2, cat2)
    far_sums(done(bd2a, lambda a, b, value: put_planes(e2a, [(a, b)], value)), cat2, vd2a, 0, C2)
    copies[-1].wait()

    def put_d2(a, b, value):
        d2[pl.ds((2 * a + b) * PIX, PIX)] = value

    conv_level2(DEC2A, e2a, ve2b, bd2b, put_d2)
    copies[7].wait()

    @pl.loop(0, 2)
    def _(t):
        lhs = d2[pl.ds(2 * t * PIX, 2 * PIX)]
        for p, q in LEVEL2:
            put_planes(cat1, [(2 * t + p, q), (2 * t + p, q + 2)], dot_rows(lhs, vu1[p, q]).astype(BF16))

    for copy in copies[8:17]:
        copy.wait()

    border = 3 * col

    def level1(index, src, layer):
        start(index, src)
        for a in (1, 2):
            layer([(a, 1), (a, 2), (a, border)])
        finish(index, src)
        layer([(1, 3 - border), (2, 3 - border)])
        for a in (0, 3):
            layer(row_of(a))

    def dec1a(planes):
        put_planes(d1a, planes, biased_relu(dot_rows(gather(cat1, 4, planes), vd1a[...]), bpad.at[2:3, :C1P]))

    level1(CAT1, cat1, dec1a)
    copies[17].wait()

    def head(a):
        lines = [h1[a, b + 1, pl.ds(8 * h + 1, 8), :, :C1].reshape(LANE, C1) for h in range(2) for b in range(4)]
        heads[a, :6] = dot_rows(wh[...], jnp.concatenate(lines, axis=0))

    def dec1b(planes):
        put_planes(h1, planes, biased_relu(conv(d1a, 4, planes, vd1b), bd1b))

    level1(DEC1A, d1a, dec1b)
    for a in range(4):
        head(a)
    wide = 2 * PIX
    flat = jnp.concatenate([heads[a, :, h * wide:(h + 1) * wide] for a in range(4) for h in range(2)], axis=0)
    high = flat.astype(BF16)
    rest = flat - high.astype(F32)
    middle = rest.astype(BF16)
    low = (rest - middle.astype(F32)).astype(BF16)
    woven = dot_rows(high, weave[...]) + dot_rows(middle, weave[...]) + dot_rows(low, weave[...])
    for a in range(4):
        for h in range(2):
            for i in range(8):
                y[:, 4 * (8 * h + i) + a, :] = woven[(2 * a + h) * 8:(2 * a + h) * 8 + 6, i * HALF:(i + 1) * HALF]


def solution(mesh):
    tile_spec = P(("data", "row"), "col", None)

    def device_body(image_tile, *params):
        (w_enc1a, b_enc1a, w_enc1b, b_enc1b, w_enc2a, b_enc2a, w_enc2b, b_enc2b,
         w_mid_a, b_mid_a, w_mid_b, b_mid_b, w_up2, w_dec2a, b_dec2a, w_dec2b, b_dec2b,
         w_up1, w_dec1a, b_dec1a, w_dec1b, b_dec1b, w_head, b_head) = params
        anywhere = pl.BlockSpec(memory_space=pl.ANY)
        vmem = pl.BlockSpec(memory_space=pltpu.VMEM)
        small = [
            jnp.transpose(image_tile, (2, 0, 1)), w_enc1a, w_head.T, b_enc1a, b_enc1b, b_enc2a, b_enc2b,
            b_mid_a, b_mid_b, b_dec2a, b_dec2b, b_dec1a, b_dec1b,
        ]
        operands = [
            w_enc1b, w_enc2a, w_enc2b, w_mid_a, w_mid_b, w_up2, w_dec2a, w_dec2b,
            jnp.swapaxes(w_up1, 2, 3), jnp.swapaxes(w_dec1a, 2, 3), w_dec1b,
        ]

        def kept(*shape, dtype=BF16):
            return pltpu.VMEM(shape, dtype)

        def level(factor, lanes):
            return kept(factor, factor + 2, ROWS, SIDE, lanes)

        scratch = [
            kept(24, PATCH, C1P), kept(3, 3, C1, C1), kept(3, 3, C1P, C1P), kept(3, 3, C1P, C2), kept(3, 3, C2, C2),
            kept(3, 3, C2, C3), kept(3, 3, C3, C3), kept(2, 2, C3, C2), kept(3, 3, C3, C2),
            kept(2, 2, C1, C2), kept(C1P, 9 * C2), kept(3, 3, C1P, C1),
            level(4, C1P), level(4, C2), level(4, C1P), level(2, C1P), level(2, C2), level(2, C3),
            kept(4 * PIX, C2), level(1, C2), level(1, C3), kept(PIX, C3), level(1, LANE), kept(EXT, PATCH),
            kept(TAPROWS, C1P, dtype=F32), kept(5, C3, dtype=F32), kept(2 * PIX, 2 * PIX),
            kept(4, PIX, C2, dtype=F32), kept(4, 8, 4 * PIX, dtype=F32),
        ]
        scratch += [kept(factor, SIDE, width) for factor, width in EXCHANGE]
        scratch += [kept(factor + 2, SIDE, width) for factor, width in EXCHANGE]
        links = pltpu.SemaphoreType.DMA((len(EXCHANGE), MESSAGES))
        scratch += [pltpu.SemaphoreType.DMA((LOADS,)), links, links, pltpu.SemaphoreType.DMA((SMALL,))]
        scratch = [kept(*array.shape, dtype=array.dtype) for array in small] + scratch
        out = pl.pallas_call(
            functools.partial(kernel, mesh.shape["row"]),
            name="unet",
            out_shape=jax.ShapeDtypeStruct((6, HALF, HALF), F32),
            in_specs=[anywhere] * (len(operands) + SMALL),
            out_specs=vmem,
            scratch_shapes=scratch,
            compiler_params=pltpu.CompilerParams(collective_id=0, has_side_effects=True, vmem_limit_bytes=67043328),
        )(*operands, *small)
        return jnp.transpose(out, (1, 2, 0)) + b_head

    def program(image, *params):
        mapped = jax.shard_map(device_body, mesh=mesh, in_specs=(tile_spec,) + tuple([P()] * len(params)), out_specs=tile_spec, check_vma=False)
        return mapped(image, *params)

    return program
```
